1024 devices in a mesh: gx: 8 (over y), gy: 4 (over x_lo, core), gz: 32 (over z, x_hi).
Axes of the slice: x: 4 (x_hi: 2, x_lo: 2; x = x_hi * 2 + x_lo), y: 8, z: 16, core: 2. Of those that a mesh axis runs over, the one named last changes fastest.
Arguments:
- rhs_velocity: float32 [3, 32, 32, 4096], P(None, 'gx', 'gy', 'gz'), may hold values from -6 to 6
- rhs_pressure: float32 [32, 32, 4096], P('gx', 'gy', 'gz'), may hold values from -6 to 6
- layer_ids: int32 [32, 32, 4096], P('gx', 'gy', 'gz'), may hold values from 0 to 7
- visc_table: float32 [8], replicated, may hold values from 0.5 to 8
- stencil: float32 [27, 3, 3], replicated, as said below
Outputs:
- velocity_out: float32 [3, 32, 32, 4096], P(None, 'gx', 'gy', 'gz')
- pressure_out: float32 [32, 32, 4096], P('gx', 'gy', 'gz')
The draws below stay inside these ranges and needn't reach their ends.
Inputs may be any that keep to these rules, and one draw needn't show every extreme that they name: The block stencil[13] has a positive diagonal that dominates its row together with all other blocks' entries.
All inputs are finite; a program needn't handle non-finite values.
Results may differ from the reference program's by a relative error of at most 0.00015.
Values sent between devices are 32-bit elements; how exact they have to be, the bound alone decides.
A program may use at most 32 MiB of HBM per device.

```python
import math
import jax
import jax.numpy as jnp
from jax import lax

LAYERS = 8
NX = 32
NY = 32
NZ = 4096


def draw_stencil(key, part):
    key_off = jax.random.fold_in(key, 11)
    key_mid = jax.random.fold_in(key, 12)
    key_diag = jax.random.fold_in(key, 13)
    spread = 0.03
    others = jax.random.normal(key_off, (27, 3, 3), jnp.float32) * spread
    center_off = jax.random.normal(key_mid, (3, 3), jnp.float32) * 0.1
    picker = (jnp.arange(27) == 13).astype(jnp.float32)[:, None, None]
    others = others * (1.0 - picker)
    eye = jnp.eye(3, dtype=jnp.float32)
    row_mass = jnp.sum(jnp.abs(others), axis=(0, 2)) + jnp.sum(jnp.abs(center_off * (1.0 - eye)), axis=1)
    extra = jax.random.uniform(key_diag, (3,), jnp.float32, 0.0, 0.5)
    center = center_off * (1.0 - eye) + eye * (1.0 + row_mass + extra)[:, None]
    return others + picker * center[None]


def place_ends(drawn, rng, low, largest):
    shape = drawn.shape
    index_at = [jax.random.randint(jax.random.fold_in(rng, axis), (), 0, shape[axis]) for axis in range(len(shape))]
    drawn = drawn.at[tuple(index_at)].set(low)
    longest = shape.index(max(shape))
    index_at[longest] = (index_at[longest] + 1) % shape[longest]
    return drawn.at[tuple(index_at)].set(largest)


def block_scale(rng, extent, shards, low, largest):
    gain = 1.0
    for dim, shards_of in shards:
        heights = jax.random.uniform(jax.random.fold_in(jax.random.fold_in(rng, 6), dim), (shards_of,), jnp.float32, low / len(shards), largest / len(shards))
        gain = gain * jnp.repeat(jnp.exp(heights), extent[dim] // shards_of).reshape((-1,) + (1,) * (len(extent) - 1 - dim))
    return gain


def normal_values(key, dims, scale, bound, shards=(), held_as=jnp.bfloat16):
    factor_of = block_scale(key, dims, shards, -0.22, 0.18) if shards else 1.0
    values = jax.random.normal(key, dims, jnp.float32) * scale * factor_of
    return jnp.minimum(jnp.maximum(values, -bound), bound).astype(held_as)


def setup_inputs(seed: int = 0) -> dict:
    arg_keys = jax.random.split(jax.random.key(seed), 6)
    return {
        "rhs_velocity": normal_values(arg_keys[0], (3, NX, NY, NZ), 1.0, 6.0, ((1, 8), (2, 4), (3, 32)), jnp.float32),
        "rhs_pressure": normal_values(arg_keys[1], (NX, NY, NZ), 1.0, 6.0, ((0, 8), (1, 4), (2, 32)), jnp.float32),
        "layer_ids": place_ends(jax.random.randint(arg_keys[2], (NX, NY, NZ), 0, LAYERS), jax.random.fold_in(arg_keys[2], 1), 0, LAYERS - 1).astype(jnp.int32),
        "visc_table": jnp.clip(jnp.exp(jax.random.uniform(arg_keys[3], (LAYERS,), jnp.float32, math.log(0.5), math.log(8.0))), 0.5, 8.0),
        "stencil": draw_stencil(jax.random.fold_in(arg_keys[5], 71), 0),
    }


LOW_BOUND = 0.2
HIGH_BOUND = 1.8
OMEGA = 2.0 / 3.0


def cheb_consts():
    theta = (HIGH_BOUND + LOW_BOUND) / 2.0
    delta = (HIGH_BOUND - LOW_BOUND) / 2.0
    sigma = theta / delta
    rho_zero = 1.0 / sigma
    rho_one = 1.0 / (2.0 * sigma - rho_zero)
    return theta, delta, rho_zero, rho_one


def stencil_sum(padded, stencil):
    sizes = (padded.shape[1] - 2, padded.shape[2] - 2, padded.shape[3] - 2)
    total = jnp.zeros((3,) + sizes, jnp.float32)
    for first in range(3):
        for second in range(3):
            for third in range(3):
                slab = padded[:, first:first + sizes[0], second:second + sizes[1], third:third + sizes[2]]
                block = stencil[first * 9 + second * 3 + third]
                total = total + jnp.einsum("ij,jxyz->ixyz", block, slab, precision=lax.Precision.HIGHEST)
    return total


def lookup(layer_ids, visc_table):
    eta = jnp.zeros(layer_ids.shape, jnp.float32)
    for layer in range(visc_table.shape[0]):
        eta = eta + jnp.where(layer_ids == layer, visc_table[layer], 0.0)
    return eta


def apply_field(field, scale, stencil):
    padded = jnp.pad(field, ((0, 0), (1, 1), (1, 1), (1, 1)))
    return scale[None] * stencil_sum(padded, stencil)


def smooth_zero(rhs, scale, dinv, stencil):
    theta, delta, rho_zero, rho_one = cheb_consts()
    first = dinv[None] * rhs / theta
    resid = rhs - apply_field(first, scale, stencil)
    second = rho_one * rho_zero * first + (2.0 * rho_one / delta) * dinv[None] * resid
    return first + second


def coarsen(field):
    shape = field.shape
    blocks = field.reshape(shape[:-3] + (shape[-3] // 2, 2, shape[-2] // 2, 2, shape[-1] // 2, 2))
    count = len(shape)
    return jnp.mean(blocks, axis=(count - 2, count, count + 2))


def refine(field):
    return jnp.repeat(jnp.repeat(jnp.repeat(field, 2, axis=1), 2, axis=2), 2, axis=3)


def reference(rhs_velocity, rhs_pressure, layer_ids, visc_table, stencil):
    theta, delta, rho_zero, rho_one = cheb_consts()
    eta = lookup(layer_ids, visc_table)
    kc = (stencil[13, 0, 0] + stencil[13, 1, 1] + stencil[13, 2, 2]) / 3.0
    dinv = 1.0 / (eta * kc)
    smoothed = smooth_zero(rhs_velocity, eta, dinv, stencil)
    residual = rhs_velocity - apply_field(smoothed, eta, stencil)
    coarse_res = coarsen(residual)
    eta_coarse = coarsen(eta)
    scale_coarse = 0.25 * eta_coarse
    dinv_coarse = 1.0 / (scale_coarse * kc)
    correction = smooth_zero(coarse_res, scale_coarse, dinv_coarse, stencil)
    start = smoothed + refine(correction)
    resid = rhs_velocity - apply_field(start, eta, stencil)
    first = dinv[None] * resid / theta
    middle = start + first
    resid = rhs_velocity - apply_field(middle, eta, stencil)
    second = rho_one * rho_zero * first + (2.0 * rho_one / delta) * dinv[None] * resid
    velocity_out = middle + second
    weight = 1.0 / eta
    pinv = 1.0 / (6.0 * weight)
    pressure = OMEGA * pinv * rhs_pressure
    for sweep in range(2):
        padded = jnp.pad(pressure, 1)
        beside = padded[2:, 1:-1, 1:-1] + padded[:-2, 1:-1, 1:-1]
        beside = beside + padded[1:-1, 2:, 1:-1] + padded[1:-1, :-2, 1:-1]
        beside = beside + padded[1:-1, 1:-1, 2:] + padded[1:-1, 1:-1, :-2]
        applied = weight * (6.0 * pressure - beside)
        pressure = pressure + OMEGA * pinv * (rhs_pressure - applied)
    return velocity_out, pressure
```

```python
import functools

import numpy as np
import jax
import jax.numpy as jnp
from jax import lax
from jax.experimental import pallas as pl
from jax.experimental.pallas import tpu as pltpu
from jax.sharding import PartitionSpec as P

F32 = jnp.float32
BF16 = jnp.bfloat16
MESH = pl.DeviceIdType.MESH

THETA = (1.8 + 0.2) / 2.0
DELTA = (1.8 - 0.2) / 2.0
SIGMA = THETA / DELTA
RHO0 = 1.0 / SIGMA
RHO1 = 1.0 / (2.0 * SIGMA - RHO0)
MOM = RHO1 * RHO0
WEIGHT = 2.0 * RHO1 / DELTA

XLO, XHI, YLO, YHI, ZLO, ZHI, NEVER = 1, 2, 4, 8, 16, 32, 64

ONE, ZERO = 28, 31

CORNER_X = (4, 5, -2, -1)
SIDES = [(dx, dy) for dx in (-1, 0, 1) for dy in (-1, 0, 1) if (dx, dy) != (0, 0)]


def plane_block(x, j):
    return [(x, r, j) for r in range(8)]


def y_block(s, j):
    return [(r // 2, (-2 if s == 0 else 8) + r % 2, j) for r in range(8)]


def c_block(s, j):
    return [(CORNER_X[r // 2], (-2 if s == 0 else 8) + r % 2, j) for r in range(8)]


def yh_block(i, xs=range(4)):
    return [(r // 2, -1 if r % 2 else 8, i) if r // 2 in xs else None for r in range(8)]


def ch_block(i, xs=(-1, 4)):
    return [(CORNER_X[r // 2], -1 if r % 2 else 8, i) if CORNER_X[r // 2] in xs else None for r in range(8)]


def rows_wide(comps):
    rows = []
    for x in (-2, -1, 0, 1, 2):
        for j in range(comps):
            rows += plane_block(x, j)
    for block in (y_block, c_block):
        for s in range(2):
            for j in range(comps):
                rows += block(s, j)
    for x in (3, 4, 5):
        for j in range(comps):
            rows += plane_block(x, j)
    return rows


def rows_ring(comps):
    rows = []
    for x in range(-1, 5):
        for i in range(comps):
            rows += plane_block(x, i)
    for i in range(comps):
        rows += yh_block(i)
    for i in range(comps):
        rows += ch_block(i)
    return rows


def rows_half(planes, y_xs, c_xs):
    rows = []
    for x in planes:
        for i in range(3):
            rows += plane_block(x, i)
    for i in range(3):
        rows += yh_block(i, y_xs)
    for i in range(3):
        rows += ch_block(i, c_xs)
    return rows + [None] * 8


def rows_coarse_in():
    rows = []
    for dx in (-1, 0, 1):
        for dy in (-1, 0, 1):
            for j in range(3):
                rows += [(2 * dx + r // 4, 4 * dy + r % 4, j) for r in range(8)]
    return rows


def rows_coarse_out():
    rows = []
    for q in range(3):
        for i in range(3):
            for r in range(8):
                n = 8 * q + r
                rows.append((n // 6 - 1, n % 6 - 1, i))
    return rows + [None] * 8


def index_stencil(outs, ins):
    table = np.full((len(outs), 256), ZERO, np.int32)
    for m, out in enumerate(outs):
        if out is None:
            continue
        for k, source in enumerate(ins):
            if source is None:
                continue
            a, b = source[0] - out[0] + 1, source[1] - out[1] + 1
            if 0 <= a <= 2 and 0 <= b <= 2:
                table[m, k] = 3 * (3 * a + b) + source[2]
    return table


def index_same(outs, ins, scale):
    table = np.full((len(outs), 256), ZERO, np.int32)
    for m, out in enumerate(outs):
        if out is None:
            continue
        for k, source in enumerate(ins):
            if source is not None and (out[0] // scale, out[1] // scale, out[2]) == source:
                table[m, k] = ONE
    return table


def index_refined(outs, ins):
    table = np.full((len(outs), 256), ZERO, np.int32)
    for m, out in enumerate(outs):
        if out is None:
            continue
        for k, source in enumerate(ins):
            if source is None:
                continue
            a = [v for v in range(3) if (out[0] + v - 1) // 2 == source[0]]
            b = [v for v in range(3) if (out[1] + v - 1) // 2 == source[1]]
            if a and b:
                segment = (len(a) - 1) + 2 * (len(b) - 1)
                table[m, k] = 32 * segment + 3 * (3 * a[0] + b[0]) + source[2]
    return table


def codes(rows, x_end, y_end, lanes, z_bits):
    table = np.full((len(rows), lanes), NEVER, np.int32)
    z_row = np.full((lanes,), NEVER, np.int32)
    for lane, bits in z_bits:
        z_row[lane] = bits
    for m, row in enumerate(rows):
        if row is None:
            continue
        bits = (XLO if row[0] < 0 else 0) | (XHI if row[0] >= x_end else 0)
        bits |= (YLO if row[1] < 0 else 0) | (YHI if row[1] >= y_end else 0)
        table[m] = bits | z_row
    return table


def face_matrix(outs, ins):
    table = np.zeros((len(outs), len(ins)), np.float32)
    for m, out in enumerate(outs):
        if out is None:
            continue
        for k, source in enumerate(ins):
            if source is not None and abs(source[0] - out[0]) + abs(source[1] - out[1]) == 1:
                table[m, k] = 1.0
    return table


FINE_LANES = [(z, 0) for z in range(128)]
WIDE_Z = FINE_LANES + [(128, ZHI), (129, ZHI), (254, ZLO), (255, ZLO)]
RING_Z = FINE_LANES + [(128, ZHI), (255, ZLO)]
COARSE_Z = [(z, 0) for z in range(64)] + [(64, ZHI), (65, ZHI), (126, ZLO), (127, ZLO)]
COARSE_RING_Z = [(z, 0) for z in range(64)] + [(64, ZHI), (127, ZLO)]

WIDE = rows_wide(3)
RING = rows_ring(3)
LOCAL = [row for x in range(4) for i in range(3) for row in plane_block(x, i)]
HALF_A = rows_half((-1, 0, 1), (0, 1), (-1,))
HALF_B = rows_half((2, 3, 4), (2, 3), (4,))
COARSE_IN = rows_coarse_in()
COARSE_OUT = rows_coarse_out()

SECTIONS = [
    ("a", index_stencil(HALF_A, WIDE[0:256]), 3),
    ("b", index_stencil(HALF_B, WIDE[32:288]), 3),
    ("local", index_stencil(LOCAL, RING), 3),
    ("coarse", index_stencil(COARSE_OUT, COARSE_IN), 3),
    ("keep", index_same(COARSE_OUT, COARSE_IN, 1), 1),
    ("fine", index_refined(RING, COARSE_OUT), 3),
    ("spread", index_same(RING, COARSE_OUT, 2), 1),
]
INDEX = np.concatenate([section[1] for section in SECTIONS], axis=0)
PLACE = {}
_at = 0
_row = 0
for _name, _table, _copies in SECTIONS:
    PLACE[_name] = (_at, _row, len(_table), _copies)
    _at += len(_table)
    _row += len(_table) * _copies
W_ROWS = _row

CODE_WIDE = codes(WIDE, 4, 8, 256, WIDE_Z)
CODE_RING = codes(RING, 4, 8, 256, RING_Z)
CODE_COARSE = codes(COARSE_IN, 2, 4, 128, COARSE_Z)
CODE_COARSE_RING = codes(COARSE_OUT, 2, 4, 128, COARSE_RING_Z)
CODE_WIDE_P = codes(rows_wide(1), 4, 8, 256, WIDE_Z)
CODE_RING_P = codes(rows_ring(1), 4, 8, 256, RING_Z)
CODE_256 = np.concatenate([CODE_WIDE, CODE_RING, CODE_WIDE_P, CODE_RING_P], axis=0)
CODE_128 = np.concatenate([CODE_COARSE, CODE_COARSE_RING], axis=0)


def face_pair(outs, ins, width, total):
    single = face_matrix(outs, ins)
    table = np.zeros((len(outs), total), np.float32)
    table[:, : single.shape[1]] = single
    table[:, width : width + single.shape[1]] = single
    return table


FACE_1 = face_pair(rows_ring(1), rows_wide(1), 128, 256)
FACE_2 = face_pair([row for x in range(4) for row in plane_block(x, 0)], rows_ring(1), 64, 128)


def split(value):
    high = value.astype(BF16)
    low = (value - high.astype(F32)).astype(BF16)
    return high, low


def z_shift_sum(product, rows):
    lanes = product.shape[1]
    return (
        product[rows : 2 * rows]
        + pltpu.roll(product[0:rows], 1, 1)
        + pltpu.roll(product[2 * rows : 3 * rows], lanes - 1, 1)
    )


def body(
    rhs_hbm, press_hbm, ids_hbm, visc_hbm, stencil_hbm, index_hbm, code256_hbm, code128_hbm, face1_hbm, face2_hbm,
    out_ref, pout_ref,
    rhs, press, ids, visc, stencil, index, code256, code128, face1, face2,
    eta, main, ypack, zpack, zmerged, rx, ry, rz, rf,
    main2, ypack2, zpack2, zmerged2, rx2, ry2, rz2, rf2,
    cmain, czpack, czmerged, rc, rcz, rcf,
    tables, w, w_fine, wide, wide_p, ring_u, ring_x2, ring_t, resid, ceta,
    in_sem, send_sem, recv_sem,
):
    nx, ny, nz = (lax.axis_size(name) for name in ("gx", "gy", "gz"))
    ix, iy, iz = (lax.axis_index(name) for name in ("gx", "gy", "gz"))

    def device(dx, dy, dz):
        return (
            lax.rem(ix + dx + nx, nx),
            lax.rem(iy + dy + ny, ny),
            lax.rem(iz + dz + nz, nz),
        )

    barrier = pltpu.get_barrier_semaphore()
    for dz in (-1, 1):
        pl.semaphore_signal(barrier, inc=1, device_id=device(0, 0, dz), device_id_type=MESH)
    for dx, dy in SIDES:
        pl.semaphore_signal(barrier, inc=1, device_id=device(dx, dy, 0), device_id_type=MESH)

    loads = [
        pltpu.make_async_copy(source, target, in_sem.at[n])
        for n, (source, target) in enumerate(
            [
                (visc_hbm, visc),
                (ids_hbm, ids),
                (rhs_hbm, rhs),
                (press_hbm, press),
                (stencil_hbm, stencil),
                (index_hbm, index),
                (code256_hbm, code256),
                (code128_hbm, code128),
                (face1_hbm, face1),
                (face2_hbm, face2),
            ]
        )
    ]
    for load in loads:
        load.start()

    counter = [0]
    sent = []

    def send(source, target, where):
        n = counter[0]
        counter[0] += 1
        copy = pltpu.make_async_remote_copy(
            src_ref=source,
            dst_ref=target,
            send_sem=send_sem.at[n],
            recv_sem=recv_sem.at[n],
            device_id=device(*where),
            device_id_type=MESH,
        )
        copy.start()
        sent.append(copy)
        return copy

    bad = (
        NEVER
        + XLO * (ix == 0).astype(jnp.int32)
        + XHI * (ix == nx - 1).astype(jnp.int32)
        + YLO * (iy == 0).astype(jnp.int32)
        + YHI * (iy == ny - 1).astype(jnp.int32)
        + ZLO * (iz == 0).astype(jnp.int32)
        + ZHI * (iz == nz - 1).astype(jnp.int32)
    )

    lane8 = lax.broadcasted_iota(jnp.int32, (8, 128), 1)
    row8 = lax.broadcasted_iota(jnp.int32, (8, 128), 0)

    def inside(code):
        return (code & bad) == 0

    for load in loads[:4]:
        load.wait()
    for p in range(4):
        layer = ids[p]
        value = jnp.zeros((8, 128), F32)
        for k in range(8):
            value = value + jnp.where(layer == k, visc[k], 0.0)
        eta[p] = value
        inverse = 1.0 / value
        for j in range(3):
            main[p, j] = rhs[j, p] * inverse
        main[p, 3] = press[p] * value

    def pack_y(source, target, comps):
        for s in range(2):
            for j in range(comps):
                for p in range(4):
                    target[s, j, 2 * p : 2 * p + 2, :] = source[p, j, 6 * s : 6 * s + 2, :]

    def item_window(k):
        return ((lane8 + (130 - 4 * k)) & 127) < 4

    def pack_z(source, packed, comps):
        total = jnp.zeros((8, 128), F32)
        k = 0
        for p in range(4):
            for j in range(comps):
                total = jnp.where(item_window(k), pltpu.roll(source[p, j], 4 * k, 1), total)
                k += 1
        for s in range(2):
            for j in range(comps):
                total = jnp.where(item_window(k), pltpu.roll(packed[s, j], 4 * k, 1), total)
                k += 1
        return total

    def tile_edge(merged, k):
        moved = pltpu.roll(merged, (128 - 4 * k) % 128, 1)
        return moved

    pack_y(main, ypack, 4)
    zpack[...] = pack_z(main, ypack, 4)

    pl.semaphore_wait(barrier, 10)

    def send_faces(source, packed, x_slots, y_slots):
        copies = []
        for dx in (-1, 1):
            planes = source.at[pl.ds(0 if dx < 0 else 2, 2)]
            copies.append(send(planes, x_slots.at[0 if dx > 0 else 1], (dx, 0, 0)))
        for dy in (-1, 1):
            for dx in (0, -1, 1):
                copies.append(
                    send(packed.at[0 if dy < 0 else 1], y_slots.at[0 if dy > 0 else 1, dx + 1], (dx, dy, 0))
                )
        return copies

    def send_sides(source, slots):
        return [send(source, slots.at[n], (dx, dy, 0)) for n, (dx, dy) in enumerate(SIDES)]

    def send_z(source, slots):
        return [send(source, slots.at[0 if dz > 0 else 1], (0, 0, dz)) for dz in (-1, 1)]

    z_first = send_z(zpack, rz)
    faces_first = send_faces(main, ypack, rx, ry)

    lane16 = lax.broadcasted_iota(jnp.int32, (16, 128), 1)
    loads[4].wait()
    kc = (stencil[0, 0, 13] + stencil[1, 1, 13] + stencil[2, 2, 13]) / 3.0
    loads[5].wait()
    for c in range(3):
        rows = []
        for i in range(3):
            base = jnp.zeros((8, 128), F32)
            for a in range(3):
                for b in range(3):
                    for j in range(3):
                        at = 3 * (3 * a + b) + j
                        base = jnp.where(lane8 == at, stencil[i, j, 9 * a + 3 * b + c], base)
            low = lane8 < 27
            pair_a = base + jnp.where(low, pltpu.roll(base, 128 - 9, 1), 0.0)
            pair_b = base + jnp.where(low, pltpu.roll(base, 128 - 3, 1), 0.0)
            pair_ab = pair_a + jnp.where(low, pltpu.roll(pair_a, 128 - 3, 1), 0.0)
            full = base + pltpu.roll(pair_a, 32, 1) + pltpu.roll(pair_b, 64, 1) + pltpu.roll(pair_ab, 96, 1)
            rows.append(jnp.where(lane8 == ONE, 1.0, full))
        for combo, (one, two) in enumerate(((0, 1), (2, 0), (1, 2))):
            tables[3 * c + combo, 0:8, :] = rows[one]
            tables[3 * c + combo, 8:16, :] = rows[two]

    def build(name, target, base, tiles, width):
        at, _, count, copies = PLACE[name]

        def step(t, carry):
            combo = lax.rem(t, 3)
            start = pl.multiple_of(t * 16, 16)
            for tile in range(tiles):
                picked = index[pl.ds(at + start, 16), 128 * tile : 128 * tile + 128]
                for c in range(copies):
                    value = jnp.take_along_axis(
                        tables[3 * c + combo], picked, axis=1, mode="promise_in_bounds"
                    )
                    high, low = split(value)
                    rows = pl.ds(base + c * count + start, 16)
                    target[rows, 128 * tile : 128 * tile + 128] = high
                    target[rows, width + 128 * tile : width + 128 * tile + 128] = low
                    target[rows, 2 * width + 128 * tile : 2 * width + 128 * tile + 128] = high
            return carry

        lax.fori_loop(0, count // 16, step, 0)

    def w_base(name):
        return PLACE[name][1]

    fine_base = w_base("fine")
    for name in ("a", "b", "local"):
        build(name, w, w_base(name), 2, 256)

    def merge_z(slots):
        return jnp.where((lane8 & 3) < 2, slots[1], slots[0])

    for copy in z_first:
        copy.wait_recv()
    zmerged[...] = merge_z(rz)
    sides_first = send_sides(zmerged, rf)

    for name in ("coarse", "keep"):
        build(name, w, w_base(name), 2, 256)
    for name in ("fine", "spread"):
        build(name, w_fine, w_base(name) - fine_base, 1, 128)

    for load in loads[6:]:
        load.wait()

    for copy in faces_first:
        copy.wait_recv()
    for copy in sides_first:
        copy.wait_recv()

    side = {offset: n for n, offset in enumerate(SIDES)}

    def wide_blocks(comp, comps, source, x_slots, y_slots, merged, forwarded):
        first_y = 4 * comps

        def edge(block, k):
            return tile_edge(block, k)

        def from_side(dx, dy):
            return forwarded[side[(-dx, -dy)]]

        blocks = {}
        for p in range(4):
            blocks[p] = (source[p, comp], edge(merged[...], p * comps + comp))
        for n in range(2):
            blocks[n - 2] = (x_slots[0, n, comp], edge(from_side(-1, 0), (n + 2) * comps + comp))
            blocks[n + 4] = (x_slots[1, n, comp], edge(from_side(1, 0), n * comps + comp))
        low_rows = (row8 & 7) < 4
        for s, dy in enumerate((-1, 1)):
            k = first_y + (1 - s) * comps + comp
            blocks["y", s] = (y_slots[s, 1, comp], edge(from_side(0, dy), k))
            above = (y_slots[s, 0, comp], edge(from_side(1, dy), k))
            below = (y_slots[s, 2, comp], edge(from_side(-1, dy), k))
            blocks["c", s] = tuple(jnp.where(low_rows, one, two) for one, two in zip(above, below))
        return blocks

    def store_wide(target, comps, comp_list, code_at, source, x_slots, y_slots, merged, forwarded):
        count = len(comp_list)
        for place, comp in enumerate(comp_list):
            blocks = wide_blocks(comp, comps, source, x_slots, y_slots, merged, forwarded)
            order = [-2, -1, 0, 1, 2]
            at = {}
            for n, x in enumerate(order):
                at[x] = n * count + place
            for n in range(2):
                at["y", n] = (5 + n) * count + place
                at["c", n] = (7 + n) * count + place
            for n, x in enumerate((3, 4, 5)):
                at[x] = (9 + n) * count + place
            for key, n in at.items():
                one, two = blocks[key]
                rows = slice(8 * n, 8 * n + 8)
                code = slice(code_at + 8 * n, code_at + 8 * n + 8)
                target[rows, 0:128] = jnp.where(inside(code256[code, 0:128]), one, 0.0)
                target[rows, 128:256] = jnp.where(inside(code256[code, 128:256]), two, 0.0)

    def ring_of(source, comps):
        def block(n):
            return source[8 * comps * n : 8 * comps * (n + 1), :]

        rows = 8 * comps
        local_row = lax.broadcasted_iota(jnp.int32, (rows, 256), 0)
        odd = (local_row & 1) == 1
        return jnp.concatenate(
            [
                block(1), block(2), block(3), block(4), block(9), block(10),
                jnp.where(odd, block(5), block(6)),
                jnp.where(odd, block(7), block(8)),
            ],
            axis=0,
        )

    def operator_ring():
        parts = []
        for name, start in (("a", 0), ("b", 32)):
            high, low = split(wide[start : start + 256, :])
            right = jnp.concatenate([high, high, low], axis=0)
            base = w_base(name)
            product = jnp.dot(w[base : base + 384, :], right, preferred_element_type=F32)
            parts.append(z_shift_sum(product, 128))
        one, two = parts
        return jnp.concatenate([one[0:72], two[0:72], one[72:120] + two[72:120]], axis=0)

    def operator_local(value):
        high, low = split(value)
        gap = jnp.zeros((64, 256), BF16)
        right = jnp.concatenate([high, gap, high, gap, low, gap], axis=0)
        base = w_base("local")
        product = jnp.dot(w[base : base + 288, :], right, preferred_element_type=F32)
        return z_shift_sum(product, 96)

    ikc = jnp.full((8, 256), 1.0, F32) / kc
    ikc = ikc[0:1, :]
    gain_u = ((1.0 + MOM + WEIGHT * THETA) / THETA) * ikc
    gain_s = (-WEIGHT / THETA) * ikc * ikc

    ring_code = len(CODE_WIDE)
    wide_p_code = ring_code + len(CODE_RING)
    ring_p_code = wide_p_code + len(CODE_WIDE_P)

    def ring_inside():
        return inside(code256[ring_code : ring_code + 192, :])

    store_wide(wide, 4, (0, 1, 2), 0, main, rx, ry, zmerged, rf)
    u_ring = ring_of(wide, 3)
    ring_u[...] = u_ring
    x2 = jnp.where(ring_inside(), gain_u * u_ring + gain_s * operator_ring(), 0.0)
    ring_x2[...] = x2
    for p in range(4):
        for j in range(3):
            n = 3 + 3 * p + j
            main2[p, j] = x2[8 * n : 8 * n + 8, 0:128]
    pack_y(main2, ypack2, 3)
    zpack2[...] = pack_z(main2, ypack2, 3)
    z_second = send_z(zpack2, rz2)
    faces_second = send_faces(main2, ypack2, rx2, ry2)

    applied = operator_local(x2)
    even = (lane8 * 2) & 127

    def coarse_sum(source, n):
        value = source[n, pl.ds(0, 8, 2), :] + source[n, pl.ds(1, 8, 2), :]
        value = value + pltpu.roll(value, 127, 1)
        return jnp.take_along_axis(value, even, axis=1, mode="promise_in_bounds")

    for big in range(2):
        resid[3, 8 * big : 8 * big + 8, :] = eta[2 * big] + eta[2 * big + 1]
        for j in range(3):
            total = jnp.zeros((8, 128), F32)
            for p in (2 * big, 2 * big + 1):
                n = 3 * p + j
                total = total + eta[p] * (main[p, j] - applied[8 * n : 8 * n + 8, 0:128])
            resid[j, 8 * big : 8 * big + 8, :] = total
    four_over = 4.0 / coarse_sum(resid, 3)
    total = jnp.zeros((8, 128), F32)
    for j in range(3):
        value = coarse_sum(resid, j) * four_over
        cmain[j] = value
        first = (lane8 >= 64 + 4 * j) & (lane8 < 66 + 4 * j)
        last = ((lane8 + (130 - 4 * j)) & 127) < 2
        total = jnp.where(first | last, pltpu.roll(value, 64 + 4 * j, 1), total)
    czpack[...] = total
    z_coarse = send_z(czpack, rcz)
    main_coarse = send_sides(cmain, rc)

    store_wide(wide_p, 4, (3,), wide_p_code, main, rx, ry, zmerged, rf)
    q_ring = ring_of(wide_p, 1)
    high, low = split(wide_p[...])
    gap = jnp.zeros((32, 256), BF16)
    near = jnp.dot(face1[...], jnp.concatenate([high, gap, low, gap], axis=0), preferred_element_type=F32)
    near = near + pltpu.roll(q_ring, 1, 1) + pltpu.roll(q_ring, 255, 1)
    p_ring = (4.0 / 27.0) * q_ring + (1.0 / 81.0) * near
    p_ring = jnp.where(inside(code256[ring_p_code : ring_p_code + 64, :]), p_ring, 0.0)
    high, low = split(p_ring)
    near = jnp.dot(face2[...], jnp.concatenate([high, low], axis=0), preferred_element_type=F32)
    p_in, q_in = p_ring[8:40], q_ring[8:40]
    near = near + pltpu.roll(p_in, 1, 1) + pltpu.roll(p_in, 255, 1)
    p_out = (1.0 / 3.0) * p_in + (1.0 / 9.0) * q_in + (1.0 / 9.0) * near
    for p in range(4):
        pout_ref[p] = p_out[8 * p : 8 * p + 8, 0:128]

    for copy in z_second:
        copy.wait_recv()
    zmerged2[...] = merge_z(rz2)
    sides_second = send_sides(zmerged2, rf2)

    for copy in z_coarse:
        copy.wait_recv()
    czmerged[...] = jnp.where((lane8 >= 64) & (lane8 < 96), rcz[1], rcz[0])
    sides_coarse = send_sides(czmerged, rcf)

    for copy in faces_second:
        copy.wait_recv()
    for copy in sides_second:
        copy.wait_recv()
    store_wide(wide, 3, (0, 1, 2), 0, main2, rx2, ry2, zmerged2, rf2)
    ring_t[...] = operator_ring()

    for copy in main_coarse:
        copy.wait_recv()
    for copy in sides_coarse:
        copy.wait_recv()

    blocks = []
    n = 0
    for dx in (-1, 0, 1):
        for dy in (-1, 0, 1):
            for j in range(3):
                if (dx, dy) == (0, 0):
                    inner, merged = cmain[j], czmerged[...]
                else:
                    slot = side[(-dx, -dy)]
                    inner, merged = rc[slot, j], rcf[slot]
                value = jnp.where(lane8 < 64, inner, tile_edge(merged, j))
                blocks.append(jnp.where(inside(code128[8 * n : 8 * n + 8, :]), value, 0.0))
                n += 1
    blocks.append(jnp.zeros((40, 128), F32))
    high, low = split(jnp.concatenate(blocks, axis=0))
    base = w_base("coarse")
    product = jnp.dot(
        w[base : base + 320, :], jnp.concatenate([high, high, low], axis=0), preferred_element_type=F32
    )
    e = gain_u[:, 0:128] * product[240:320] + gain_s[:, 0:128] * z_shift_sum(product, 80)
    e = jnp.where(inside(code128[216:296, :]), e, 0.0)
    lane80 = lax.broadcasted_iota(jnp.int32, (80, 128), 1)
    near_lane = lane80 >> 1
    far_lane = jnp.where(lane80 < 2, 64, jnp.where(lane80 >= 126, 127, 100))
    e = jnp.concatenate(
        [
            jnp.take_along_axis(e, near_lane, axis=1, mode="promise_in_bounds"),
            jnp.take_along_axis(e, far_lane, axis=1, mode="promise_in_bounds"),
        ],
        axis=1,
    )
    high, low = split(e)
    gap = jnp.zeros((48, 256), BF16)
    right = jnp.concatenate([high, gap, high, gap, low, gap], axis=0)
    product = jnp.dot(w_fine[...], right, preferred_element_type=F32)
    moved = ring_u[...] - (ring_t[...] + z_shift_sum(product, 192))
    step = ((1.0 / THETA) * ikc) * moved
    x = jnp.where(ring_inside(), ring_x2[...] + product[576:768] + step, 0.0)
    applied = operator_local(x)
    final = (
        x[24:120] + MOM * step[24:120] + (WEIGHT * ikc) * (ring_u[24:120, :] - applied)
    )
    for p in range(4):
        for j in range(3):
            n = 3 * p + j
            out_ref[j, p] = final[8 * n : 8 * n + 8, 0:128]

    for copy in sent:
        copy.wait_send()


COPIES = 2 * (2 + 8 + 8) + 2 + 8 + 8


def scratch():
    vmem = pltpu.VMEM
    fine_rows = 4 * 192

    def exchange(comps):
        return [
            vmem((4, comps, 8, 128), F32),
            vmem((2, comps, 8, 128), F32),
            vmem((8, 128), F32),
            vmem((8, 128), F32),
            vmem((2, 2, comps, 8, 128), F32),
            vmem((2, 3, comps, 8, 128), F32),
            vmem((2, 8, 128), F32),
            vmem((8, 8, 128), F32),
        ]

    return [
        vmem((3, 4, 8, 128), F32),
        vmem((4, 8, 128), F32),
        vmem((4, 8, 128), jnp.int32),
        pltpu.SMEM((8,), F32),
        pltpu.SMEM((3, 3, 27), F32),
        vmem(INDEX.shape, jnp.int32),
        vmem(CODE_256.shape, jnp.int32),
        vmem(CODE_128.shape, jnp.int32),
        vmem(FACE_1.shape, BF16),
        vmem(FACE_2.shape, BF16),
        vmem((4, 8, 128), F32),
        *exchange(4),
        *exchange(3),
        vmem((3, 8, 128), F32),
        vmem((8, 128), F32),
        vmem((8, 128), F32),
        vmem((8, 3, 8, 128), F32),
        vmem((2, 8, 128), F32),
        vmem((8, 8, 128), F32),
        vmem((9, 16, 128), F32),
        vmem((W_ROWS - fine_rows, 768), BF16),
        vmem((fine_rows, 384), BF16),
        vmem((288, 256), F32),
        vmem((96, 256), F32),
        vmem((192, 256), F32),
        vmem((192, 256), F32),
        vmem((192, 256), F32),
        vmem((4, 16, 128), F32),
        vmem((8, 128), F32),
        pltpu.SemaphoreType.DMA((10,)),
        pltpu.SemaphoreType.DMA((COPIES,)),
        pltpu.SemaphoreType.DMA((COPIES,)),
    ]


def on_device(rhs_velocity, rhs_pressure, layer_ids, visc_table, stencil):
    anywhere = pl.BlockSpec(memory_space=pltpu.HBM)
    inside = pl.BlockSpec(memory_space=pltpu.VMEM)
    return pl.pallas_call(
        body,
        name="stokes",
        out_shape=(
            jax.ShapeDtypeStruct(rhs_velocity.shape, F32),
            jax.ShapeDtypeStruct(rhs_pressure.shape, F32),
        ),
        in_specs=[anywhere] * 10,
        out_specs=(inside, inside),
        scratch_shapes=scratch(),
        compiler_params=pltpu.CompilerParams(
            collective_id=0, has_side_effects=True, vmem_limit_bytes=60 * 1024 * 1024
        ),
    )(
        rhs_velocity,
        rhs_pressure,
        layer_ids,
        visc_table,
        stencil.transpose(1, 2, 0),
        jnp.asarray(INDEX),
        jnp.asarray(CODE_256),
        jnp.asarray(CODE_128),
        jnp.asarray(FACE_1, BF16),
        jnp.asarray(FACE_2, BF16),
    )


def solution(mesh):
    placed = (P(None, "gx", "gy", "gz"), P("gx", "gy", "gz"), P("gx", "gy", "gz"), P(), P())
    return jax.shard_map(
        on_device,
        mesh=mesh,
        in_specs=placed,
        out_specs=(P(None, "gx", "gy", "gz"), P("gx", "gy", "gz")),
        check_vma=False,
    )
```

```python
import functools

import numpy as np
import jax
import jax.numpy as jnp
from jax import lax
from jax.experimental import pallas as pl
from jax.experimental.pallas import tpu as pltpu
from jax.sharding import PartitionSpec as P

F32 = jnp.float32
BF16 = jnp.bfloat16
MESH = pl.DeviceIdType.MESH

THETA = (1.8 + 0.2) / 2.0
DELTA = (1.8 - 0.2) / 2.0
SIGMA = THETA / DELTA
RHO0 = 1.0 / SIGMA
RHO1 = 1.0 / (2.0 * SIGMA - RHO0)
MOM = RHO1 * RHO0
WEIGHT = 2.0 * RHO1 / DELTA

XLO, XHI, YLO, YHI, ZLO, ZHI, NEVER = 1, 2, 4, 8, 16, 32, 64

ONE, ZERO = 28, 31

CORNER_X = (4, 5, -2, -1)
SIDES = [(dx, dy) for dx in (-1, 0, 1) for dy in (-1, 0, 1) if (dx, dy) != (0, 0)]
AHEAD = [(dy, dz) for dy in (0, -1, 1) for dz in (-1, 1)]


def plane_block(x, j):
    return [(x, r, j) for r in range(8)]


def y_block(s, j):
    return [(r // 2, (-2 if s == 0 else 8) + r % 2, j) for r in range(8)]


def c_block(s, j):
    return [(CORNER_X[r // 2], (-2 if s == 0 else 8) + r % 2, j) for r in range(8)]


def edge_block(i, half):
    rows = []
    for r in range(8):
        y = -1 if r % 2 else 8
        if half == 0:
            x = r // 2 if r < 4 else (-1 if r >= 6 else None)
        else:
            x = r // 2 if r >= 4 else (4 if r < 2 else None)
        rows.append(None if x is None else (x, y, i))
    return rows


def rows_wide(comps):
    rows = []
    for x in (-2, -1, 0, 1, 2):
        for j in range(comps):
            rows += plane_block(x, j)
    for block in (y_block, c_block):
        for s in range(2):
            for j in range(comps):
                rows += block(s, j)
    for x in (3, 4, 5):
        for j in range(comps):
            rows += plane_block(x, j)
    return rows


def rows_half(half, comps):
    rows = []
    for x in ((-1, 0, 1), (2, 3, 4))[half]:
        for i in range(comps):
            rows += plane_block(x, i)
    for i in range(comps):
        rows += edge_block(i, half)
    return rows


def rows_ring(comps):
    return rows_half(0, comps) + rows_half(1, comps)


def rows_coarse_in():
    rows = []
    for dx in (-1, 0, 1):
        for j in range(3):
            rows += [(2 * dx + r // 4, r % 4, j) for r in range(8)]
        for j in range(3):
            rows += [(2 * dx + r // 4, r % 4 + (4 if r % 4 < 2 else -4), j) for r in range(8)]
    return rows


def rows_coarse_out():
    rows = []
    for q in range(3):
        for i in range(3):
            for r in range(8):
                n = 8 * q + r
                rows.append((n // 6 - 1, n % 6 - 1, i))
    return rows + [None] * 8


def index_stencil(outs, ins):
    table = np.full((len(outs), len(ins)), ZERO, np.int32)
    for m, out in enumerate(outs):
        if out is None:
            continue
        for k, source in enumerate(ins):
            if source is None:
                continue
            a, b = source[0] - out[0] + 1, source[1] - out[1] + 1
            if 0 <= a <= 2 and 0 <= b <= 2:
                table[m, k] = 3 * (3 * a + b) + source[2]
    return table


def index_same(outs, ins, scale):
    table = np.full((len(outs), len(ins)), ZERO, np.int32)
    for m, out in enumerate(outs):
        if out is None:
            continue
        for k, source in enumerate(ins):
            if source is not None and (out[0] // scale, out[1] // scale, out[2]) == source:
                table[m, k] = ONE
    return table


def index_refined(outs, ins):
    table = np.full((len(outs), len(ins)), ZERO, np.int32)
    for m, out in enumerate(outs):
        if out is None:
            continue
        for k, source in enumerate(ins):
            if source is None:
                continue
            a = [v for v in range(3) if (out[0] + v - 1) // 2 == source[0]]
            b = [v for v in range(3) if (out[1] + v - 1) // 2 == source[1]]
            if a and b:
                segment = (len(a) - 1) + 2 * (len(b) - 1)
                table[m, k] = 32 * segment + 3 * (3 * a[0] + b[0]) + source[2]
    return table


def codes(rows, x_end, y_end, lanes, z_bits):
    table = np.full((len(rows), lanes), NEVER, np.int32)
    z_row = np.full((lanes,), NEVER, np.int32)
    for lane, bits in z_bits:
        z_row[lane] = bits
    for m, row in enumerate(rows):
        if row is None:
            continue
        bits = (XLO if row[0] < 0 else 0) | (XHI if row[0] >= x_end else 0)
        bits |= (YLO if row[1] < 0 else 0) | (YHI if row[1] >= y_end else 0)
        table[m] = bits | z_row
    return table


def face_matrix(outs, ins):
    table = np.zeros((len(outs), len(ins)), np.float32)
    for m, out in enumerate(outs):
        if out is None:
            continue
        for k, source in enumerate(ins):
            if source is not None and abs(source[0] - out[0]) + abs(source[1] - out[1]) == 1:
                table[m, k] = 1.0
    return table


FINE_LANES = [(z, 0) for z in range(128)]
WIDE_Z = FINE_LANES + [(128, ZHI), (129, ZHI), (254, ZLO), (255, ZLO)]
RING_Z = FINE_LANES + [(128, ZHI), (255, ZLO)]
COARSE_Z = [(z, 0) for z in range(64)] + [(64, ZHI), (65, ZHI), (126, ZLO), (127, ZLO)]
COARSE_RING_Z = [(z, 0) for z in range(64)] + [(64, ZHI), (127, ZLO)]

WIDE = rows_wide(3)
RING = rows_ring(3)
LOCAL = [row for x in range(4) for i in range(3) for row in plane_block(x, i)]
HALF_A = rows_half(0, 3)
HALF_B = rows_half(1, 3)
COARSE_IN = rows_coarse_in()
COARSE_OUT = rows_coarse_out()

def triple(table, width):
    wide = np.full((len(table), width), ZERO, np.int32)
    count = table.shape[1]
    for n in range(3):
        wide[:, n * count : (n + 1) * count] = table
    return wide


def single(table):
    return np.concatenate([table, np.full((len(table), 256 - table.shape[1]), ZERO, np.int32)], axis=1)


def place(sections):
    places, at, row = {}, 0, 0
    for name, table, copies in sections:
        places[name] = (at, len(table), copies, row)
        at += len(table)
        row += len(table) * copies
    return places, np.concatenate([section[1] for section in sections], axis=0), row


WIDE_SECTIONS, WIDE_INDEX, WIDE_ROWS = place(
    [
        ("a", single(index_stencil(HALF_A, WIDE[0:256])), 3),
        ("b", single(index_stencil(HALF_B, WIDE[32:288])), 3),
        ("local", single(index_stencil(LOCAL, RING)), 3),
    ]
)
COARSE_SECTIONS, COARSE_INDEX, COARSE_ROWS = place(
    [
        ("coarse", triple(index_stencil(COARSE_OUT, COARSE_IN), 512), 3),
        ("keep", triple(index_same(COARSE_OUT, COARSE_IN, 1), 512), 1),
    ]
)
FINE_SECTIONS, FINE_INDEX, FINE_ROWS = place(
    [
        ("fine", triple(index_refined(RING, COARSE_OUT), 256), 3),
        ("spread", triple(index_same(RING, COARSE_OUT, 2), 256), 1),
    ]
)

CODE_WIDE = codes(WIDE, 4, 8, 256, WIDE_Z)
CODE_RING = codes(RING, 4, 8, 256, RING_Z)
CODE_COARSE = codes(COARSE_IN, 2, 4, 128, COARSE_Z)
CODE_COARSE_RING = codes(COARSE_OUT, 2, 4, 128, COARSE_RING_Z)
CODE_WIDE_P = codes(rows_wide(1), 4, 8, 256, WIDE_Z)
CODE_RING_P = codes(rows_ring(1), 4, 8, 256, RING_Z)
CODE_256 = np.concatenate([CODE_WIDE, CODE_RING, CODE_WIDE_P, CODE_RING_P], axis=0)
CODE_128 = np.concatenate([CODE_COARSE, CODE_COARSE_RING], axis=0)


def face_pair(outs, ins, width, total):
    single = face_matrix(outs, ins)
    table = np.zeros((len(outs), total), np.float32)
    table[:, : single.shape[1]] = single
    table[:, width : width + single.shape[1]] = single
    return table


FACE_1 = face_pair(rows_ring(1), rows_wide(1), 128, 256)
FACE_2 = face_pair([row for x in range(4) for row in plane_block(x, 0)], rows_ring(1), 64, 128)


def split(value):
    high = value.astype(BF16)
    low = (value - high.astype(F32)).astype(BF16)
    return high, low


def z_shift_sum(product, rows):
    lanes = product.shape[1]
    return (
        product[rows : 2 * rows]
        + pltpu.roll(product[0:rows], 1, 1)
        + pltpu.roll(product[2 * rows : 3 * rows], lanes - 1, 1)
    )


def body(
    rhs_hbm, press_hbm, ids_hbm, visc_hbm, stencil_hbm, windex_hbm, cindex_hbm, findex_hbm,
    code256_hbm, code128_hbm, face1_hbm, face2_hbm,
    out_ref, pout_ref,
    rhs, press, ids, visc, stencil, windex, cindex, findex, code256, code128, face1, face2,
    eta, main, ypack, zpack, zmerged, rx, ry, rz, rf,
    before, coarse, zpack2, zmerged2, rx2, rs2, rz2, rf2,
    tables, w, w_coarse, w_fine, wide, wide_p, ring_x, resid,
    in_sem, send_sem, recv_sem,
):
    nx, ny, nz = (lax.axis_size(name) for name in ("gx", "gy", "gz"))
    ix, iy, iz = (lax.axis_index(name) for name in ("gx", "gy", "gz"))
    ends = {
        ("x", -1): ix > 0, ("x", 1): ix < nx - 1,
        ("y", -1): iy > 0, ("y", 1): iy < ny - 1,
        ("z", -1): iz > 0, ("z", 1): iz < nz - 1,
    }

    def present(dx, dy, dz):
        found = None
        for axis, step in (("x", dx), ("y", dy), ("z", dz)):
            if step:
                one = ends[axis, step]
                found = one if found is None else jnp.logical_and(found, one)
        return found

    def device(dx, dy, dz):
        return (ix + dx, iy + dy, iz + dz)

    partners = [(0, dy, dz) for dy, dz in AHEAD] + [(dx, dy, 0) for dx, dy in SIDES]
    barrier = pltpu.get_barrier_semaphore()
    expected = 0
    for where in partners:
        there = present(*where)
        expected = expected + there.astype(jnp.int32)

        @pl.when(there)
        def _():
            pl.semaphore_signal(barrier, inc=1, device_id=device(*where), device_id_type=MESH)

    loads = [
        pltpu.make_async_copy(source, target, in_sem.at[n])
        for n, (source, target) in enumerate(
            [
                (visc_hbm, visc), (ids_hbm, ids), (rhs_hbm, rhs), (press_hbm, press), (stencil_hbm, stencil),
                (windex_hbm, windex), (code256_hbm, code256), (code128_hbm, code128),
                (cindex_hbm, cindex), (findex_hbm, findex), (face1_hbm, face1), (face2_hbm, face2),
            ]
        )
    ]
    for load in loads:
        load.start()

    counter = [0]
    sent = []

    def send(source, target, where):
        n = counter[0]
        counter[0] += 1
        copy = pltpu.make_async_remote_copy(
            src_ref=source,
            dst_ref=target,
            send_sem=send_sem.at[n],
            recv_sem=recv_sem.at[n],
            device_id=device(*where),
            device_id_type=MESH,
        )
        pl.when(present(*where))(copy.start)
        sent.append((copy, present(*where)))
        return copy, present(*(-step for step in where))

    def receive(copies):
        for copy, there in copies:
            pl.when(there)(copy.wait_recv)

    bad = NEVER
    for bit, end in (
        (XLO, ("x", -1)), (XHI, ("x", 1)), (YLO, ("y", -1)), (YHI, ("y", 1)), (ZLO, ("z", -1)), (ZHI, ("z", 1)),
    ):
        bad = bad + bit * (1 - ends[end].astype(jnp.int32))

    lane8 = lax.broadcasted_iota(jnp.int32, (8, 128), 1)
    row8 = lax.broadcasted_iota(jnp.int32, (8, 128), 0)
    low_rows = row8 < 4
    odd_rows = (row8 & 1) == 1

    def inside(code):
        return (code & bad) == 0

    def roll(value, shift):
        return pltpu.roll(value, shift % 128, 1) if shift % 128 else value

    for load in loads[:4]:
        load.wait()
    for p in range(4):
        layer = ids[p]
        value = jnp.zeros((8, 128), F32)
        for k in range(8):
            value = value + jnp.where(layer == k, visc[k], 0.0)
        eta[p] = value
        inverse = 1.0 / value
        for j in range(3):
            main[p, j] = rhs[j, p] * inverse
        main[p, 3] = press[p] * value

    for s in range(2):
        for j in range(4):
            for p in range(4):
                ypack[s, j, 2 * p : 2 * p + 2, :] = main[p, j, 6 * s : 6 * s + 2, :]
    items = [main[p, j] for p in range(4) for j in range(4)] + [ypack[s, j] for s in range(2) for j in range(4)]
    total = jnp.zeros((8, 128), F32)
    for k, value in enumerate(items):
        total = jnp.where(((lane8 + (130 - 4 * k)) & 127) < 4, roll(value, 4 * k), total)
    zpack[...] = total

    pl.semaphore_wait(barrier, expected)

    def send_ahead(source, slots):
        return [send(source, slots.at[0 if dz > 0 else 1, 1 - dy], (0, dy, dz)) for dy, dz in AHEAD]

    def send_on(source, slots):
        return [send(source, slots.at[0 if dx > 0 else 1], (dx, 0, 0)) for dx in (-1, 1)]

    ahead_first = send_ahead(zpack, rz)
    faces_first = []
    for dx in (-1, 1):
        planes = main.at[pl.ds(0 if dx < 0 else 2, 2)]
        faces_first.append(send(planes, rx.at[0 if dx > 0 else 1], (dx, 0, 0)))
    for dy in (-1, 1):
        for dx in (0, -1, 1):
            faces_first.append(
                send(ypack.at[0 if dy < 0 else 1], ry.at[0 if dy > 0 else 1, 1 - dx], (dx, dy, 0))
            )

    loads[4].wait()
    kc = (stencil[0, 0, 13] + stencil[1, 1, 13] + stencil[2, 2, 13]) / 3.0
    for c in range(3):
        rows = []
        for i in range(3):
            base = jnp.zeros((8, 128), F32)
            for a in range(3):
                for b in range(3):
                    for j in range(3):
                        at = 3 * (3 * a + b) + j
                        base = jnp.where(lane8 == at, stencil[i, j, 9 * a + 3 * b + c], base)
            low = lane8 < 27
            pair_a = base + jnp.where(low, roll(base, -9), 0.0)
            pair_b = base + jnp.where(low, roll(base, -3), 0.0)
            pair_ab = pair_a + jnp.where(low, roll(pair_a, -3), 0.0)
            full = base + roll(pair_a, 32) + roll(pair_b, 64) + roll(pair_ab, 96)
            rows.append(jnp.where(lane8 == ONE, 1.0, full))
        for combo, (one, two) in enumerate(((0, 1), (2, 0), (1, 2))):
            tables[3 * c + combo, 0:8, :] = rows[one]
            tables[3 * c + combo, 8:16, :] = rows[two]

    lane16 = lax.broadcasted_iota(jnp.int32, (16, 128), 1)

    def build(index, section, target, tiles, width, unroll):
        at, count, copies, first = section

        def chunk(t):
            combo = lax.rem(t, 3)
            start = pl.multiple_of(t * 16, 16)
            for tile in range(tiles):
                lanes = slice(128 * tile, 128 * tile + 128)
                picked = index[pl.ds(at + start, 16), lanes]
                for c in range(copies):
                    value = jnp.take_along_axis(
                        tables[3 * c + combo], picked, axis=1, mode="promise_in_bounds"
                    )
                    rows = pl.ds(first + c * count + start, 16)
                    if width is None:
                        high, low = split(value)
                        target[rows, lanes] = high
                        target[rows, 256 + 128 * tile : 384 + 128 * tile] = low
                        target[rows, 512 + 128 * tile : 640 + 128 * tile] = high
                    else:
                        low = value - value.astype(BF16).astype(F32)
                        lane = lane16 + 128 * tile
                        value = jnp.where((lane >= width) & (lane < 2 * width), low, value)
                        target[rows, lanes] = value.astype(BF16)

        def step(t, carry):
            for n in range(unroll):
                chunk(t * unroll + n)
            return carry

        lax.fori_loop(0, count // (16 * unroll), step, 0)

    loads[5].wait()
    for name in ("a", "b", "local"):
        build(windex, WIDE_SECTIONS[name], w, 2, None, 3)
    for load in loads[6:]:
        load.wait()

    receive(ahead_first)
    for n in range(3):
        zmerged[n] = jnp.where((lane8 & 3) < 2, rz[1, n], rz[0, n])
    on_first = send_on(zmerged, rf)

    def along_z(own, passed, ox, oy):
        return own[oy + 1] if ox == 0 else passed[0 if ox < 0 else 1, oy + 1]

    def wide_blocks(comp, tile):
        comps = 4

        def edge(ox, oy, k):
            return roll(along_z(zmerged, rf, ox, oy), -4 * k)

        blocks = {}
        for p in range(4):
            blocks[p] = edge(0, 0, p * comps + comp) if tile else main[p, comp]
        for n in range(2):
            blocks[n - 2] = edge(-1, 0, (n + 2) * comps + comp) if tile else rx[0, n, comp]
            blocks[n + 4] = edge(1, 0, n * comps + comp) if tile else rx[1, n, comp]
        for s, oy in enumerate((-1, 1)):
            k = 4 * comps + (1 - s) * comps + comp
            level, above, below = (edge(ox, oy, k) if tile else ry[s, ox + 1, comp] for ox in (0, 1, -1))
            blocks["y", s] = level
            blocks["c", s] = jnp.where(low_rows, above, below)
        return blocks

    def store_wide(target, comps, code_at, tile):
        lanes = slice(128 * tile, 128 * tile + 128)
        for slot, comp in enumerate(comps):
            blocks = wide_blocks(comp, tile)
            order = [-2, -1, 0, 1, 2, ("y", 0), ("y", 1), ("c", 0), ("c", 1), 3, 4, 5]
            for n, key in enumerate(order):
                at = 8 * (n * len(comps) + slot)
                code = code256[code_at + at : code_at + at + 8, lanes]
                target[at : at + 8, lanes] = jnp.where(inside(code), blocks[key], 0.0)

    def ring_of(source, comps):
        def block(n):
            return source[8 * comps * n : 8 * comps * (n + 1), :]

        row = lax.broadcasted_iota(jnp.int32, (8 * comps, 256), 0)
        odd, low = (row & 1) == 1, (row & 7) < 4
        level = jnp.where(odd, block(5), block(6))
        corner = jnp.where(odd, block(7), block(8))
        return jnp.concatenate(
            [
                block(1), block(2), block(3), jnp.where(low, level, corner),
                block(4), block(9), block(10), jnp.where(low, corner, level),
            ],
            axis=0,
        )

    def local_of(ring, comps):
        return jnp.concatenate([ring[8 * comps : 24 * comps], ring[32 * comps : 48 * comps]], axis=0)

    def operator_ring():
        parts = []
        for name, start in (("a", 0), ("b", 32)):
            high, low = split(wide[start : start + 256, :])
            right = jnp.concatenate([high, high, low], axis=0)
            base = WIDE_SECTIONS[name][3]
            product = jnp.dot(w[base : base + 288, :], right, preferred_element_type=F32)
            parts.append(z_shift_sum(product, 96))
        return jnp.concatenate(parts, axis=0)

    def operator_local(value):
        high, low = split(value)
        gap = jnp.zeros((64, 256), BF16)
        right = jnp.concatenate([high, gap, high, gap, low, gap], axis=0)
        base = WIDE_SECTIONS["local"][3]
        product = jnp.dot(w[base : base + 288, :], right, preferred_element_type=F32)
        return z_shift_sum(product, 96)

    ikc = (jnp.full((8, 256), 1.0, F32) / kc)[0:1, :]
    gain_u = ((1.0 + MOM + WEIGHT * THETA) / THETA) * ikc
    gain_s = (-WEIGHT / THETA) * ikc * ikc

    ring_code = len(CODE_WIDE)
    wide_p_code = ring_code + len(CODE_RING)
    ring_p_code = wide_p_code + len(CODE_WIDE_P)

    def ring_inside():
        return inside(code256[ring_code : ring_code + 192, :])

    receive(faces_first)
    store_wide(wide, (0, 1, 2), 0, 0)
    receive(on_first)

    store_wide(wide, (0, 1, 2), 0, 1)
    x2 = jnp.where(ring_inside(), gain_u * ring_of(wide, 3) + gain_s * operator_ring(), 0.0)
    ring_x[...] = x2

    applied = operator_local(x2)
    even = (lane8 * 2) & 127

    def coarse_sum(source, n):
        value = source[n, pl.ds(0, 8, 2), :] + source[n, pl.ds(1, 8, 2), :]
        value = value + roll(value, -1)
        return jnp.take_along_axis(value, even, axis=1, mode="promise_in_bounds")

    def local_row(p):
        return 8 * (3 + 3 * p if p < 2 else 6 + 3 * p)

    for big in range(2):
        resid[3, 8 * big : 8 * big + 8, :] = eta[2 * big] + eta[2 * big + 1]
        for j in range(3):
            total = jnp.zeros((8, 128), F32)
            for p in (2 * big, 2 * big + 1):
                n = 8 * (3 * p + j)
                left = main[p, j] - applied[n : n + 8, 0:128]
                resid[4 + j, 8 * p : 8 * p + 8, :] = left
                at = local_row(p) + 8 * j
                value = ring_x[at : at + 8, 0:128] + ((1.0 / THETA) * ikc[:, 0:128]) * left
                before[p, j] = value
                total = total + eta[p] * left
            resid[j, 8 * big : 8 * big + 8, :] = total
    four_over = 4.0 / coarse_sum(resid, 3)
    total = jnp.zeros((8, 128), F32)
    for j in range(3):
        value = coarse_sum(resid, j) * four_over
        coarse[j] = value
        first = (lane8 >= 98 + 4 * j) & (lane8 < 100 + 4 * j)
        last = (lane8 >= 32 + 4 * j) & (lane8 < 34 + 4 * j)
        total = jnp.where(first | last, roll(value, 98 + 4 * j), total)
        for p in range(4):
            coarse[3 + j, 2 * p : 2 * p + 1, :] = before[p, j, 0:1, :]
            coarse[3 + j, 2 * p + 1 : 2 * p + 2, :] = before[p, j, 7:8, :]
    items = [before[p, j] for p in range(4) for j in range(3)] + [coarse[3 + j] for j in range(3)]
    for k, value in enumerate(items):
        total = jnp.where(((lane8 + (129 - 2 * k)) & 127) < 2, roll(value, 2 * k), total)
    zpack2[...] = total
    ahead_second = send_ahead(zpack2, rz2)
    side = {offset: n for n, offset in enumerate(SIDES)}
    sides_second = [
        send(coarse, rs2.at[side[(-dx, -dy)]], (dx, dy, 0)) for dx, dy in SIDES
    ]
    for dx in (-1, 1):
        sides_second.append(send(before.at[0 if dx < 0 else 3], rx2.at[0 if dx > 0 else 1], (dx, 0, 0)))

    store_wide(wide_p, (3,), wide_p_code, 0)
    store_wide(wide_p, (3,), wide_p_code, 1)
    q_ring = ring_of(wide_p, 1)
    high, low = split(wide_p[...])
    gap = jnp.zeros((32, 256), BF16)
    near = jnp.dot(face1[...], jnp.concatenate([high, gap, low, gap], axis=0), preferred_element_type=F32)
    near = near + pltpu.roll(q_ring, 1, 1) + pltpu.roll(q_ring, 255, 1)
    p_ring = (4.0 / 27.0) * q_ring + (1.0 / 81.0) * near
    p_ring = jnp.where(inside(code256[ring_p_code : ring_p_code + 64, :]), p_ring, 0.0)
    high, low = split(p_ring)
    near = jnp.dot(face2[...], jnp.concatenate([high, low], axis=0), preferred_element_type=F32)
    p_in, q_in = local_of(p_ring, 1), local_of(q_ring, 1)
    near = near + pltpu.roll(p_in, 1, 1) + pltpu.roll(p_in, 255, 1)
    p_out = (1.0 / 3.0) * p_in + (1.0 / 9.0) * q_in + (1.0 / 9.0) * near
    for p in range(4):
        pout_ref[p] = p_out[8 * p : 8 * p + 8, 0:128]
    for name in ("coarse", "keep"):
        build(cindex, COARSE_SECTIONS[name], w_coarse, 4, 144, 1)

    receive(ahead_second)
    from_high = ((lane8 < 32) & ((lane8 & 1) == 0)) | ((lane8 >= 64) & (lane8 < 127))
    for n in range(3):
        zmerged2[n] = jnp.where(from_high, rz2[1, n], rz2[0, n])
    on_second = send_on(zmerged2, rf2)

    for name in ("fine", "spread"):
        build(findex, FINE_SECTIONS[name], w_fine, 2, 80, 3)

    receive(sides_second)
    receive(on_second)

    def coarse_block(ox, oy, j):
        inner = coarse[j] if (ox, oy) == (0, 0) else rs2[side[(ox, oy)], j]
        return jnp.where(lane8 < 64, inner, roll(along_z(zmerged2, rf2, ox, oy), -(34 + 4 * j)))

    blocks = []
    near_high = (row8 & 3) < 2
    for ox in (-1, 0, 1):
        blocks += [coarse_block(ox, 0, j) for j in range(3)]
        blocks += [jnp.where(near_high, coarse_block(ox, 1, j), coarse_block(ox, -1, j)) for j in range(3)]
    value = jnp.where(inside(code128[0:144, :]), jnp.concatenate(blocks, axis=0), 0.0)
    high, low = split(value)
    right = jnp.concatenate([high, high, low, jnp.zeros((80, 128), BF16)], axis=0)
    product = jnp.dot(w_coarse[...], right, preferred_element_type=F32)
    e = gain_u[:, 0:128] * product[240:320] + gain_s[:, 0:128] * z_shift_sum(product, 80)
    e = jnp.where(inside(code128[144:224, :]), e, 0.0)
    lane80 = lax.broadcasted_iota(jnp.int32, (80, 128), 1)
    near_lane = lane80 >> 1
    far_lane = jnp.where(lane80 < 2, 64, jnp.where(lane80 >= 126, 127, 100))
    e = jnp.concatenate(
        [
            jnp.take_along_axis(e, near_lane, axis=1, mode="promise_in_bounds"),
            jnp.take_along_axis(e, far_lane, axis=1, mode="promise_in_bounds"),
        ],
        axis=1,
    )
    high, low = split(e)
    right = jnp.concatenate([high, high, low, jnp.zeros((16, 256), BF16)], axis=0)
    product = jnp.dot(w_fine[...], right, preferred_element_type=F32)

    def ring_block(ox, oy, inner, k):
        return jnp.concatenate([inner, roll(along_z(zmerged2, rf2, ox, oy), -2 * k)], axis=1)

    def layer(ox, oy, j):
        return ring_block(ox, oy, rs2[side[(ox, oy)], 3 + j], 12 + j)

    low_wide = lax.broadcasted_iota(jnp.int32, (8, 256), 0) < 4
    odd_wide = (lax.broadcasted_iota(jnp.int32, (8, 256), 0) & 1) == 1
    halves = [[], []]
    for half in range(2):
        for x in ((-1, 0, 1), (2, 3, 4))[half]:
            for j in range(3):
                if x == -1:
                    halves[half].append(ring_block(-1, 0, rx2[0, j], 9 + j))
                elif x == 4:
                    halves[half].append(ring_block(1, 0, rx2[1, j], j))
                else:
                    halves[half].append(ring_block(0, 0, before[x, j], 3 * x + j))
    for j in range(3):
        level = jnp.where(odd_wide, layer(0, -1, j), layer(0, 1, j))
        low_x = jnp.where(odd_wide, layer(-1, -1, j), layer(-1, 1, j))
        high_x = jnp.where(odd_wide, layer(1, -1, j), layer(1, 1, j))
        halves[0].append(jnp.where(low_wide, level, low_x))
        halves[1].append(jnp.where(low_wide, high_x, level))
    start = jnp.concatenate(halves[0] + halves[1], axis=0)

    down = ((1.0 / THETA) * ikc) * z_shift_sum(product, 192)
    x = jnp.where(ring_inside(), start + product[576:768] - down, 0.0)
    applied = operator_local(x)
    x_in, down_in = local_of(x, 3), local_of(down, 3)
    for p in range(4):
        for j in range(3):
            n = 8 * (3 * p + j)
            step = ((1.0 / THETA) * ikc[:, 0:128]) * resid[4 + j, 8 * p : 8 * p + 8, :] - down_in[n : n + 8, 0:128]
            out_ref[j, p] = (
                x_in[n : n + 8, 0:128]
                + MOM * step
                + (WEIGHT * ikc[:, 0:128]) * (main[p, j] - applied[n : n + 8, 0:128])
            )

    for copy, there in sent:
        pl.when(there)(copy.wait_send)


COPIES = 6 + 8 + 2 + 6 + 10 + 2


def scratch():
    vmem = pltpu.VMEM
    return [
        vmem((3, 4, 8, 128), F32),
        vmem((4, 8, 128), F32),
        vmem((4, 8, 128), jnp.int32),
        pltpu.SMEM((8,), F32),
        pltpu.SMEM((3, 3, 27), F32),
        vmem(WIDE_INDEX.shape, jnp.int32),
        vmem(COARSE_INDEX.shape, jnp.int32),
        vmem(FINE_INDEX.shape, jnp.int32),
        vmem(CODE_256.shape, jnp.int32),
        vmem(CODE_128.shape, jnp.int32),
        vmem(FACE_1.shape, BF16),
        vmem(FACE_2.shape, BF16),
        vmem((4, 8, 128), F32),
        vmem((4, 4, 8, 128), F32),
        vmem((2, 4, 8, 128), F32),
        vmem((8, 128), F32),
        vmem((3, 8, 128), F32),
        vmem((2, 2, 4, 8, 128), F32),
        vmem((2, 3, 4, 8, 128), F32),
        vmem((2, 3, 8, 128), F32),
        vmem((2, 3, 8, 128), F32),
        vmem((4, 3, 8, 128), F32),
        vmem((6, 8, 128), F32),
        vmem((8, 128), F32),
        vmem((3, 8, 128), F32),
        vmem((2, 3, 8, 128), F32),
        vmem((8, 6, 8, 128), F32),
        vmem((2, 3, 8, 128), F32),
        vmem((2, 3, 8, 128), F32),
        vmem((9, 16, 128), F32),
        vmem((WIDE_ROWS, 768), BF16),
        vmem((COARSE_ROWS, 512), BF16),
        vmem((FINE_ROWS, 256), BF16),
        vmem((288, 256), F32),
        vmem((96, 256), F32),
        vmem((192, 256), F32),
        vmem((7, 32, 128), F32),
        pltpu.SemaphoreType.DMA((12,)),
        pltpu.SemaphoreType.DMA((COPIES,)),
        pltpu.SemaphoreType.DMA((COPIES,)),
    ]


def on_device(rhs_velocity, rhs_pressure, layer_ids, visc_table, stencil):
    anywhere = pl.BlockSpec(memory_space=pltpu.HBM)
    inside = pl.BlockSpec(memory_space=pltpu.VMEM)
    return pl.pallas_call(
        body,
        name="stokes",
        out_shape=(
            pltpu.VMEM(rhs_velocity.shape, F32),
            pltpu.VMEM(rhs_pressure.shape, F32),
        ),
        in_specs=[anywhere] * 12,
        out_specs=(inside, inside),
        scratch_shapes=scratch(),
        compiler_params=pltpu.CompilerParams(
            collective_id=0, has_side_effects=True, vmem_limit_bytes=60 * 1024 * 1024
        ),
    )(
        *(
            pltpu.with_memory_space_constraint(value, pltpu.HBM)
            for value in (
                rhs_velocity,
                rhs_pressure,
                layer_ids,
                visc_table,
                stencil.transpose(1, 2, 0),
                jnp.asarray(WIDE_INDEX),
                jnp.asarray(COARSE_INDEX),
                jnp.asarray(FINE_INDEX),
                jnp.asarray(CODE_256),
                jnp.asarray(CODE_128),
                jnp.asarray(FACE_1, BF16),
                jnp.asarray(FACE_2, BF16),
            )
        )
    )


def solution(mesh):
    placed = (P(None, "gx", "gy", "gz"), P("gx", "gy", "gz"), P("gx", "gy", "gz"), P(), P())
    return jax.shard_map(
        on_device,
        mesh=mesh,
        in_specs=placed,
        out_specs=(P(None, "gx", "gy", "gz"), P("gx", "gy", "gz")),
        check_vma=False,
    )
```

```python
import functools

import numpy as np
import jax
import jax.numpy as jnp
from jax import lax
from jax.experimental import pallas as pl
from jax.experimental.pallas import tpu as pltpu
from jax.sharding import PartitionSpec as P

F32 = jnp.float32
BF16 = jnp.bfloat16
MESH = pl.DeviceIdType.MESH

THETA = (1.8 + 0.2) / 2.0
DELTA = (1.8 - 0.2) / 2.0
SIGMA = THETA / DELTA
RHO0 = 1.0 / SIGMA
RHO1 = 1.0 / (2.0 * SIGMA - RHO0)
MOM = RHO1 * RHO0
WEIGHT = 2.0 * RHO1 / DELTA

XLO, XHI, YLO, YHI, ZLO, ZHI, NEVER = 1, 2, 4, 8, 16, 32, 64

ONE, ZERO = 28, 31

CORNER_X = (4, 5, -2, -1)
SIDES = [(dx, dy) for dx in (-1, 0, 1) for dy in (-1, 0, 1) if (dx, dy) != (0, 0)]
AHEAD = [(dx, dy, dz) for dx in (-1, 1, 0) for dy in (0, -1, 1) for dz in (-1, 1)]


def plane_block(x, j):
    return [(x, r, j) for r in range(8)]


def y_block(s, j):
    return [(r // 2, (-2 if s == 0 else 8) + r % 2, j) for r in range(8)]


def c_block(s, j):
    return [(CORNER_X[r // 2], (-2 if s == 0 else 8) + r % 2, j) for r in range(8)]


def edge_block(i, half):
    rows = []
    for r in range(8):
        y = -1 if r % 2 else 8
        if half == 0:
            x = r // 2 if r < 4 else (-1 if r >= 6 else None)
        else:
            x = r // 2 if r >= 4 else (4 if r < 2 else None)
        rows.append(None if x is None else (x, y, i))
    return rows


def rows_wide(comps):
    rows = []
    for x in (-2, -1, 0, 1, 2):
        for j in range(comps):
            rows += plane_block(x, j)
    for block in (y_block, c_block):
        for s in range(2):
            for j in range(comps):
                rows += block(s, j)
    for x in (3, 4, 5):
        for j in range(comps):
            rows += plane_block(x, j)
    return rows


def rows_half(half, comps):
    rows = []
    for x in ((-1, 0, 1), (2, 3, 4))[half]:
        for i in range(comps):
            rows += plane_block(x, i)
    for i in range(comps):
        rows += edge_block(i, half)
    return rows


def rows_ring(comps):
    return rows_half(0, comps) + rows_half(1, comps)


def rows_coarse_in():
    rows = []
    for dx in (-1, 0, 1):
        for j in range(3):
            rows += [(2 * dx + r // 4, r % 4, j) for r in range(8)]
        for j in range(3):
            rows += [(2 * dx + r // 4, r % 4 + (4 if r % 4 < 2 else -4), j) for r in range(8)]
    return rows


def rows_coarse_out():
    rows = []
    for q in range(3):
        for i in range(3):
            for r in range(8):
                n = 8 * q + r
                rows.append((n // 6 - 1, n % 6 - 1, i))
    return rows + [None] * 8


def index_stencil(outs, ins):
    table = np.full((len(outs), len(ins)), ZERO, np.int32)
    for m, out in enumerate(outs):
        if out is None:
            continue
        for k, source in enumerate(ins):
            if source is None:
                continue
            a, b = source[0] - out[0] + 1, source[1] - out[1] + 1
            if 0 <= a <= 2 and 0 <= b <= 2:
                table[m, k] = 3 * (3 * a + b) + source[2]
    return table


def index_same(outs, ins, scale):
    table = np.full((len(outs), len(ins)), ZERO, np.int32)
    for m, out in enumerate(outs):
        if out is None:
            continue
        for k, source in enumerate(ins):
            if source is not None and (out[0] // scale, out[1] // scale, out[2]) == source:
                table[m, k] = ONE
    return table


def index_refined(outs, ins):
    table = np.full((len(outs), len(ins)), ZERO, np.int32)
    for m, out in enumerate(outs):
        if out is None:
            continue
        for k, source in enumerate(ins):
            if source is None:
                continue
            a = [v for v in range(3) if (out[0] + v - 1) // 2 == source[0]]
            b = [v for v in range(3) if (out[1] + v - 1) // 2 == source[1]]
            if a and b:
                segment = (len(a) - 1) + 2 * (len(b) - 1)
                table[m, k] = 32 * segment + 3 * (3 * a[0] + b[0]) + source[2]
    return table


def codes(rows, x_end, y_end, lanes, z_bits):
    table = np.full((len(rows), lanes), NEVER, np.int32)
    z_row = np.full((lanes,), NEVER, np.int32)
    for lane, bits in z_bits:
        z_row[lane] = bits
    for m, row in enumerate(rows):
        if row is None:
            continue
        bits = (XLO if row[0] < 0 else 0) | (XHI if row[0] >= x_end else 0)
        bits |= (YLO if row[1] < 0 else 0) | (YHI if row[1] >= y_end else 0)
        table[m] = bits | z_row
    return table


def face_matrix(outs, ins):
    table = np.zeros((len(outs), len(ins)), np.float32)
    for m, out in enumerate(outs):
        if out is None:
            continue
        for k, source in enumerate(ins):
            if source is not None and abs(source[0] - out[0]) + abs(source[1] - out[1]) == 1:
                table[m, k] = 1.0
    return table


FINE_LANES = [(z, 0) for z in range(128)]
WIDE_Z = FINE_LANES + [(128, ZHI), (129, ZHI), (254, ZLO), (255, ZLO)]
RING_Z = FINE_LANES + [(128, ZHI), (255, ZLO)]
COARSE_Z = [(z, 0) for z in range(64)] + [(64, ZHI), (65, ZHI), (126, ZLO), (127, ZLO)]
COARSE_RING_Z = [(z, 0) for z in range(64)] + [(64, ZHI), (127, ZLO)]

WIDE = rows_wide(3)
RING = rows_ring(3)
LOCAL = [row for x in range(4) for i in range(3) for row in plane_block(x, i)]
HALF_A = rows_half(0, 3)
HALF_B = rows_half(1, 3)
COARSE_IN = rows_coarse_in()
COARSE_OUT = rows_coarse_out()

def triple(table, width):
    wide = np.full((len(table), width), ZERO, np.int32)
    count = table.shape[1]
    for n in range(3):
        wide[:, n * count : (n + 1) * count] = table
    return wide


def single(table):
    return np.concatenate([table, np.full((len(table), 256 - table.shape[1]), ZERO, np.int32)], axis=1)


def place(sections):
    places, at, row = {}, 0, 0
    for name, table, copies in sections:
        places[name] = (at, len(table), copies, row)
        at += len(table)
        row += len(table) * copies
    return places, np.concatenate([section[1] for section in sections], axis=0), row


WIDE_SECTIONS, WIDE_INDEX, WIDE_ROWS = place(
    [
        ("a", single(index_stencil(HALF_A, WIDE[0:256])), 3),
        ("b", single(index_stencil(HALF_B, WIDE[32:288])), 3),
        ("local", single(index_stencil(LOCAL, RING)), 3),
    ]
)
COARSE_SECTIONS, COARSE_INDEX, COARSE_ROWS = place(
    [
        ("coarse", triple(index_stencil(COARSE_OUT, COARSE_IN), 512), 3),
        ("keep", triple(index_same(COARSE_OUT, COARSE_IN, 1), 512), 1),
    ]
)
FINE_SECTIONS, FINE_INDEX, FINE_ROWS = place(
    [
        ("fine", triple(index_refined(RING, COARSE_OUT), 256), 3),
        ("spread", triple(index_same(RING, COARSE_OUT, 2), 256), 1),
    ]
)

CODE_WIDE = codes(WIDE, 4, 8, 256, WIDE_Z)
CODE_RING = codes(RING, 4, 8, 256, RING_Z)
CODE_COARSE = codes(COARSE_IN, 2, 4, 128, COARSE_Z)
CODE_COARSE_RING = codes(COARSE_OUT, 2, 4, 128, COARSE_RING_Z)
CODE_WIDE_P = codes(rows_wide(1), 4, 8, 256, WIDE_Z)
CODE_RING_P = codes(rows_ring(1), 4, 8, 256, RING_Z)
CODE_256 = np.concatenate([CODE_WIDE, CODE_RING, CODE_WIDE_P, CODE_RING_P], axis=0)
CODE_128 = np.concatenate([CODE_COARSE, CODE_COARSE_RING], axis=0)


def face_pair(outs, ins, width, total):
    single = face_matrix(outs, ins)
    table = np.zeros((len(outs), total), np.float32)
    table[:, : single.shape[1]] = single
    table[:, width : width + single.shape[1]] = single
    return table


FACE_1 = face_pair(rows_ring(1), rows_wide(1), 128, 256)
FACE_2 = face_pair([row for x in range(4) for row in plane_block(x, 0)], rows_ring(1), 64, 128)


def split(value):
    high = value.astype(BF16)
    low = (value - high.astype(F32)).astype(BF16)
    return high, low


def z_shift_sum(product, rows):
    lanes = product.shape[1]
    return (
        product[rows : 2 * rows]
        + pltpu.roll(product[0:rows], 1, 1)
        + pltpu.roll(product[2 * rows : 3 * rows], lanes - 1, 1)
    )


def body(
    rhs_hbm, press_hbm, ids_hbm, visc_hbm, stencil_hbm, windex_hbm, cindex_hbm, findex_hbm,
    code256_hbm, code128_hbm, face1_hbm, face2_hbm,
    out_ref, pout_ref,
    rhs, press, ids, visc, stencil, windex, cindex, findex, code256, code128, face1, face2,
    eta, main, qmain, ypack, qpack, cpack, zpack, rx, ry, rc, rqx, rqy, rz,
    before, coarse, zpack2, xsend, ysend, csend, rx2, ry2, rc2, rz2,
    tables, w, w_coarse, w_fine, wide, wide_p, ring_x, resid, blank,
    in_sem, send_sem, recv_sem,
):
    nx, ny, nz = (lax.axis_size(name) for name in ("gx", "gy", "gz"))
    ix, iy, iz = (lax.axis_index(name) for name in ("gx", "gy", "gz"))
    ends = {
        ("x", -1): ix > 0, ("x", 1): ix < nx - 1,
        ("y", -1): iy > 0, ("y", 1): iy < ny - 1,
        ("z", -1): iz > 0, ("z", 1): iz < nz - 1,
    }

    def present(dx, dy, dz):
        found = None
        for axis, step in (("x", dx), ("y", dy), ("z", dz)):
            if step:
                one = ends[axis, step]
                found = one if found is None else jnp.logical_and(found, one)
        return found

    def device(dx, dy, dz):
        return (ix + dx, iy + dy, iz + dz)

    partners = AHEAD + [(dx, dy, 0) for dx, dy in SIDES]
    barrier = pltpu.get_barrier_semaphore()
    expected = 0
    for where in partners:
        there = present(*where)
        expected = expected + there.astype(jnp.int32)

        @pl.when(there)
        def _():
            pl.semaphore_signal(barrier, inc=1, device_id=device(*where), device_id_type=MESH)

    def load(n, pairs):
        for source, target in pairs:
            pltpu.make_async_copy(source, target, in_sem.at[n]).start()

    def tiles(count):
        return blank.at[pl.ds(0, count)]

    def loaded(n, count):
        pltpu.make_async_copy(tiles(count), tiles(count), in_sem.at[n]).wait()

    visc_load = pltpu.make_async_copy(visc_hbm, visc, in_sem.at[0])
    visc_load.start()
    load(1, [(ids_hbm, ids), (rhs_hbm, rhs), (press_hbm, press)])
    stencil_load = pltpu.make_async_copy(stencil_hbm, stencil, in_sem.at[2])
    stencil_load.start()
    windex_load = pltpu.make_async_copy(windex_hbm, windex, in_sem.at[3])
    windex_load.start()
    rest = [
        pltpu.make_async_copy(source, target, in_sem.at[4 + n])
        for n, (source, target) in enumerate(
            [
                (code256_hbm, code256), (code128_hbm, code128), (cindex_hbm, cindex), (findex_hbm, findex),
                (face1_hbm, face1), (face2_hbm, face2),
            ]
        )
    ]
    for copy in rest:
        copy.start()

    groups = []

    def send(group, source, target, where):
        copy = pltpu.make_async_remote_copy(
            src_ref=source,
            dst_ref=target,
            send_sem=send_sem.at[group],
            recv_sem=recv_sem.at[group],
            device_id=device(*where),
            device_id_type=MESH,
        )
        pl.when(present(*where))(copy.start)

    count_x, count_y, count_z = (
        ends[axis, -1].astype(jnp.int32) + ends[axis, 1].astype(jnp.int32) for axis in "xyz"
    )

    def wait_group(semaphore, choices):
        for there, count in choices:

            @pl.when(there)
            def _():
                pltpu.make_async_copy(tiles(count), tiles(count), semaphore).wait()

    def plane_choices(corner, along_x, along_y):
        return [
            (
                jnp.logical_and(count_x == nx, count_y == ny),
                corner * nx * ny + along_x * nx + along_y * ny,
            )
            for nx in (1, 2)
            for ny in (1, 2)
        ]

    def ahead_choices():
        return [
            (
                jnp.logical_and(jnp.logical_and(count_x == nx, count_y == ny), count_z == nz),
                (nx + 1) * (ny + 1) * nz,
            )
            for nx in (1, 2)
            for ny in (1, 2)
            for nz in (1, 2)
        ]

    def receive(group, choices):
        wait_group(recv_sem.at[group], choices)
        groups.append((group, choices))

    bad = NEVER
    for bit, end in (
        (XLO, ("x", -1)), (XHI, ("x", 1)), (YLO, ("y", -1)), (YHI, ("y", 1)), (ZLO, ("z", -1)), (ZHI, ("z", 1)),
    ):
        bad = bad + bit * (1 - ends[end].astype(jnp.int32))

    lane8 = lax.broadcasted_iota(jnp.int32, (8, 128), 1)
    row8 = lax.broadcasted_iota(jnp.int32, (8, 128), 0)
    low_rows = row8 < 4
    odd_rows = (row8 & 1) == 1

    def inside(code):
        return (code & bad) == 0

    def roll(value, shift):
        return pltpu.roll(value, shift % 128, 1) if shift % 128 else value

    visc_load.wait()
    loaded(1, 20)
    for p in range(4):
        layer = ids[p]
        value = jnp.zeros((8, 128), F32)
        for k in range(8):
            value = value + jnp.where(layer == k, visc[k], 0.0)
        eta[p] = value
        inverse = 1.0 / value
        for j in range(3):
            main[p, j] = rhs[j, p] * inverse
        qmain[p] = press[p] * value

    for s in range(2):
        for p in range(4):
            for j in range(3):
                ypack[s, j, 2 * p : 2 * p + 2, :] = main[p, j, 6 * s : 6 * s + 2, :]
            qpack[s, 2 * p : 2 * p + 2, :] = qmain[p, 6 * s : 6 * s + 2, :]
    for s in range(2):
        for v, (one, two) in enumerate(((ypack[s, 0], ypack[s, 1]), (ypack[s, 2], qpack[s]))):
            two = pltpu.roll(two, 4, 0)
            cpack[0, s, v] = jnp.where(low_rows, one, two)
            cpack[1, s, v] = jnp.where(low_rows, two, one)
    items = []
    for p in range(4):
        items += [main[p, j] for j in range(3)] + [qmain[p]]
    for s in range(2):
        items += [ypack[s, j] for j in range(3)] + [qpack[s]]
    total = jnp.zeros((8, 128), F32)
    for k, value in enumerate(items):
        total = jnp.where(((lane8 + (130 - 4 * k)) & 127) < 4, roll(value, 4 * k), total)
    zpack[...] = total

    pl.semaphore_wait(barrier, expected)

    def send_ahead(group, source, slots):
        for dx, dy, dz in AHEAD:
            send(group, source, slots.at[0 if dz > 0 else 1, 1 - dx, 1 - dy], (dx, dy, dz))

    send_ahead(0, zpack, rz)
    for dx in (-1, 1):
        for dy in (-1, 1):
            send(
                1,
                cpack.at[0 if dx < 0 else 1, 0 if dy < 0 else 1],
                rc.at[0 if dx > 0 else 1, 0 if dy > 0 else 1],
                (dx, dy, 0),
            )
        planes = pl.ds(0 if dx < 0 else 2, 2)
        send(1, main.at[planes], rx.at[0 if dx > 0 else 1], (dx, 0, 0))
    for dy in (-1, 1):
        send(1, ypack.at[0 if dy < 0 else 1], ry.at[0 if dy > 0 else 1], (0, dy, 0))
    for dx in (-1, 1):
        planes = pl.ds(0 if dx < 0 else 2, 2)
        send(2, qmain.at[planes], rqx.at[0 if dx > 0 else 1], (dx, 0, 0))
    for dy in (-1, 1):
        send(2, qpack.at[0 if dy < 0 else 1], rqy.at[0 if dy > 0 else 1], (0, dy, 0))

    stencil_load.wait()
    kc = (stencil[0, 0, 13] + stencil[1, 1, 13] + stencil[2, 2, 13]) / 3.0
    for c in range(3):
        rows = []
        for i in range(3):
            base = jnp.zeros((8, 128), F32)
            for a in range(3):
                for b in range(3):
                    for j in range(3):
                        at = 3 * (3 * a + b) + j
                        base = jnp.where(lane8 == at, stencil[i, j, 9 * a + 3 * b + c], base)
            low = lane8 < 27
            pair_a = base + jnp.where(low, roll(base, -9), 0.0)
            pair_b = base + jnp.where(low, roll(base, -3), 0.0)
            pair_ab = pair_a + jnp.where(low, roll(pair_a, -3), 0.0)
            full = base + roll(pair_a, 32) + roll(pair_b, 64) + roll(pair_ab, 96)
            rows.append(jnp.where(lane8 == ONE, 1.0, full))
        for combo, (one, two) in enumerate(((0, 1), (2, 0), (1, 2))):
            tables[3 * c + combo, 0:8, :] = rows[one]
            tables[3 * c + combo, 8:16, :] = rows[two]

    lane16 = lax.broadcasted_iota(jnp.int32, (16, 128), 1)

    def build(index, section, target, tiles, width, unroll):
        at, count, copies, first = section

        def chunk(t):
            combo = lax.rem(t, 3)
            start = pl.multiple_of(t * 16, 16)
            for tile in range(tiles):
                lanes = slice(128 * tile, 128 * tile + 128)
                picked = index[pl.ds(at + start, 16), lanes]
                for c in range(copies):
                    value = jnp.take_along_axis(
                        tables[3 * c + combo], picked, axis=1, mode="promise_in_bounds"
                    )
                    rows = pl.ds(first + c * count + start, 16)
                    if width is None:
                        high, low = split(value)
                        target[rows, lanes] = high
                        target[rows, 256 + 128 * tile : 384 + 128 * tile] = low
                        target[rows, 512 + 128 * tile : 640 + 128 * tile] = high
                    else:
                        low = value - value.astype(BF16).astype(F32)
                        lane = lane16 + 128 * tile
                        value = jnp.where((lane >= width) & (lane < 2 * width), low, value)
                        target[rows, lanes] = value.astype(BF16)

        def step(t, carry):
            for n in range(unroll):
                chunk(t * unroll + n)
            return carry

        lax.fori_loop(0, count // (16 * unroll), step, 0)

    windex_load.wait()
    for name in ("a", "b", "local"):
        build(windex, WIDE_SECTIONS[name], w, 2, None, 3)
    for copy in rest:
        copy.wait()
    for name in ("coarse", "keep"):
        build(cindex, COARSE_SECTIONS[name], w_coarse, 4, 144, 1)
    for name in ("fine", "spread"):
        build(findex, FINE_SECTIONS[name], w_fine, 2, 80, 3)

    def along_z(slots, select, ox, oy):
        return jnp.where(select, slots[1, ox + 1, oy + 1], slots[0, ox + 1, oy + 1])

    from_high_1 = (lane8 & 3) < 2
    from_high_2 = ((lane8 < 32) & ((lane8 & 1) == 0)) | ((lane8 >= 64) & (lane8 < 127))

    def wide_blocks(comp, tile):
        comps = 4

        def edge(ox, oy, k):
            return roll(along_z(rz, from_high_1, ox, oy), -4 * k)

        blocks = {}
        for p in range(4):
            own = main[p, comp] if comp < 3 else qmain[p]
            blocks[p] = edge(0, 0, p * comps + comp) if tile else own
        for n in range(2):
            for side, ox, first in ((0, -1, -2), (1, 1, 4)):
                near = rx[side, n, comp] if comp < 3 else rqx[side, n]
                plane = n if ox > 0 else n + 2
                blocks[first + n] = edge(ox, 0, plane * comps + comp) if tile else near
        for s, oy in enumerate((-1, 1)):
            k = 4 * comps + (1 - s) * comps + comp
            if tile:
                blocks["y", s] = edge(0, oy, k)
                blocks["c", s] = jnp.where(low_rows, edge(1, oy, k), edge(-1, oy, k))
                continue
            blocks["y", s] = ry[s, comp] if comp < 3 else rqy[s]
            below, above = rc[0, s, comp // 2], rc[1, s, comp // 2]
            if comp % 2 == 0:
                blocks["c", s] = jnp.where(low_rows, above, below)
            else:
                blocks["c", s] = pltpu.roll(jnp.where(low_rows, below, above), 4, 0)
        return blocks

    def store_wide(target, comps, code_at, tile):
        lanes = slice(128 * tile, 128 * tile + 128)
        for slot, comp in enumerate(comps):
            blocks = wide_blocks(comp, tile)
            order = [-2, -1, 0, 1, 2, ("y", 0), ("y", 1), ("c", 0), ("c", 1), 3, 4, 5]
            for n, key in enumerate(order):
                at = 8 * (n * len(comps) + slot)
                code = code256[code_at + at : code_at + at + 8, lanes]
                target[at : at + 8, lanes] = jnp.where(inside(code), blocks[key], 0.0)

    def ring_of(source, comps):
        def block(n):
            return source[8 * comps * n : 8 * comps * (n + 1), :]

        row = lax.broadcasted_iota(jnp.int32, (8 * comps, 256), 0)
        odd, low = (row & 1) == 1, (row & 7) < 4
        level = jnp.where(odd, block(5), block(6))
        corner = jnp.where(odd, block(7), block(8))
        return jnp.concatenate(
            [
                block(1), block(2), block(3), jnp.where(low, level, corner),
                block(4), block(9), block(10), jnp.where(low, corner, level),
            ],
            axis=0,
        )

    def local_of(ring, comps):
        return jnp.concatenate([ring[8 * comps : 24 * comps], ring[32 * comps : 48 * comps]], axis=0)

    def operator_ring():
        parts = []
        for name, start in (("a", 0), ("b", 32)):
            high, low = split(wide[start : start + 256, :])
            right = jnp.concatenate([high, high, low], axis=0)
            base = WIDE_SECTIONS[name][3]
            product = jnp.dot(w[base : base + 288, :], right, preferred_element_type=F32)
            parts.append(z_shift_sum(product, 96))
        return jnp.concatenate(parts, axis=0)

    def operator_local(value):
        high, low = split(value)
        gap = jnp.zeros((64, 256), BF16)
        right = jnp.concatenate([high, gap, high, gap, low, gap], axis=0)
        base = WIDE_SECTIONS["local"][3]
        product = jnp.dot(w[base : base + 288, :], right, preferred_element_type=F32)
        return z_shift_sum(product, 96)

    ikc = (jnp.full((8, 256), 1.0, F32) / kc)[0:1, :]
    gain_u = ((1.0 + MOM + WEIGHT * THETA) / THETA) * ikc
    gain_s = (-WEIGHT / THETA) * ikc * ikc

    ring_code = len(CODE_WIDE)
    wide_p_code = ring_code + len(CODE_RING)
    ring_p_code = wide_p_code + len(CODE_WIDE_P)

    def ring_inside():
        return inside(code256[ring_code : ring_code + 192, :])

    receive(1, plane_choices(2, 6, 3))
    store_wide(wide, (0, 1, 2), 0, 0)
    receive(0, ahead_choices())

    store_wide(wide, (0, 1, 2), 0, 1)
    x2 = jnp.where(ring_inside(), gain_u * ring_of(wide, 3) + gain_s * operator_ring(), 0.0)
    ring_x[...] = x2

    applied = operator_local(x2)
    even = (lane8 * 2) & 127

    def coarse_sum(source, n):
        value = source[n, pl.ds(0, 8, 2), :] + source[n, pl.ds(1, 8, 2), :]
        value = value + roll(value, -1)
        return jnp.take_along_axis(value, even, axis=1, mode="promise_in_bounds")

    def local_row(p):
        return 8 * (3 + 3 * p if p < 2 else 6 + 3 * p)

    for big in range(2):
        resid[3, 8 * big : 8 * big + 8, :] = eta[2 * big] + eta[2 * big + 1]
        for j in range(3):
            total = jnp.zeros((8, 128), F32)
            for p in (2 * big, 2 * big + 1):
                n = 8 * (3 * p + j)
                left = main[p, j] - applied[n : n + 8, 0:128]
                resid[4 + j, 8 * p : 8 * p + 8, :] = left
                at = local_row(p) + 8 * j
                value = ring_x[at : at + 8, 0:128] + ((1.0 / THETA) * ikc[:, 0:128]) * left
                before[p, j] = value
                total = total + eta[p] * left
            resid[j, 8 * big : 8 * big + 8, :] = total
    four_over = 4.0 / coarse_sum(resid, 3)
    total = jnp.zeros((8, 128), F32)
    for j in range(3):
        value = coarse_sum(resid, j) * four_over
        coarse[j] = value
        first = (lane8 >= 98 + 4 * j) & (lane8 < 100 + 4 * j)
        last = (lane8 >= 32 + 4 * j) & (lane8 < 34 + 4 * j)
        total = jnp.where(first | last, roll(value, 98 + 4 * j), total)
        for p in range(4):
            ysend[2 + j, 2 * p : 2 * p + 1, :] = before[p, j, 0:1, :]
            ysend[2 + j, 2 * p + 1 : 2 * p + 2, :] = before[p, j, 7:8, :]
            if p in (0, 3):
                n = 0 if p == 0 else 1
                xsend[n, 2 + j] = before[p, j]
                csend[n, 2, 2 * j : 2 * j + 1, :] = before[p, j, 0:1, :]
                csend[n, 2, 2 * j + 1 : 2 * j + 2, :] = before[p, j, 7:8, :]
    items = [before[p, j] for p in range(4) for j in range(3)] + [ysend[2 + j] for j in range(3)]
    for k, value in enumerate(items):
        total = jnp.where(((lane8 + (129 - 2 * k)) & 127) < 2, roll(value, 2 * k), total)
    zpack2[...] = total
    for n, value in enumerate((jnp.where(lane8 < 64, coarse[0], roll(coarse[1], 64)), coarse[2])):
        ysend[n] = value
        for m in range(2):
            xsend[m, n] = value
            csend[m, n] = value
    send_ahead(3, zpack2, rz2)
    for dx in (-1, 1):
        for dy in (-1, 1):
            send(
                4,
                csend.at[0 if dx < 0 else 1],
                rc2.at[0 if dx > 0 else 1, 0 if dy > 0 else 1],
                (dx, dy, 0),
            )
        send(4, xsend.at[0 if dx < 0 else 1], rx2.at[0 if dx > 0 else 1], (dx, 0, 0))
    for dy in (-1, 1):
        send(4, ysend, ry2.at[0 if dy > 0 else 1], (0, dy, 0))

    receive(2, plane_choices(0, 2, 1))
    store_wide(wide_p, (3,), wide_p_code, 0)
    store_wide(wide_p, (3,), wide_p_code, 1)
    q_ring = ring_of(wide_p, 1)
    high, low = split(wide_p[...])
    gap = jnp.zeros((32, 256), BF16)
    near = jnp.dot(face1[...], jnp.concatenate([high, gap, low, gap], axis=0), preferred_element_type=F32)
    near = near + pltpu.roll(q_ring, 1, 1) + pltpu.roll(q_ring, 255, 1)
    p_ring = (4.0 / 27.0) * q_ring + (1.0 / 81.0) * near
    p_ring = jnp.where(inside(code256[ring_p_code : ring_p_code + 64, :]), p_ring, 0.0)
    high, low = split(p_ring)
    near = jnp.dot(face2[...], jnp.concatenate([high, low], axis=0), preferred_element_type=F32)
    p_in, q_in = local_of(p_ring, 1), local_of(q_ring, 1)
    near = near + pltpu.roll(p_in, 1, 1) + pltpu.roll(p_in, 255, 1)
    p_out = (1.0 / 3.0) * p_in + (1.0 / 9.0) * q_in + (1.0 / 9.0) * near
    for p in range(4):
        pout_ref[p] = p_out[8 * p : 8 * p + 8, 0:128]
    receive(4, plane_choices(3, 5, 5))
    receive(3, ahead_choices())

    def from_side(ox, oy, n):
        if ox and oy:
            return rc2[0 if ox < 0 else 1, 0 if oy < 0 else 1, n]
        return rx2[0 if ox < 0 else 1, n] if ox else ry2[0 if oy < 0 else 1, n]

    def coarse_block(ox, oy, j):
        if (ox, oy) == (0, 0):
            inner = coarse[j]
        else:
            inner = from_side(ox, oy, j // 2)
            inner = roll(inner, 64) if j == 1 else inner
        return jnp.where(lane8 < 64, inner, roll(along_z(rz2, from_high_2, ox, oy), -(34 + 4 * j)))

    blocks = []
    near_high = (row8 & 3) < 2
    for ox in (-1, 0, 1):
        blocks += [coarse_block(ox, 0, j) for j in range(3)]
        blocks += [jnp.where(near_high, coarse_block(ox, 1, j), coarse_block(ox, -1, j)) for j in range(3)]
    value = jnp.where(inside(code128[0:144, :]), jnp.concatenate(blocks, axis=0), 0.0)
    high, low = split(value)
    right = jnp.concatenate([high, high, low, jnp.zeros((80, 128), BF16)], axis=0)
    product = jnp.dot(w_coarse[...], right, preferred_element_type=F32)
    e = gain_u[:, 0:128] * product[240:320] + gain_s[:, 0:128] * z_shift_sum(product, 80)
    e = jnp.where(inside(code128[144:224, :]), e, 0.0)
    lane80 = lax.broadcasted_iota(jnp.int32, (80, 128), 1)
    near_lane = lane80 >> 1
    far_lane = jnp.where(lane80 < 2, 64, jnp.where(lane80 >= 126, 127, 100))
    e = jnp.concatenate(
        [
            jnp.take_along_axis(e, near_lane, axis=1, mode="promise_in_bounds"),
            jnp.take_along_axis(e, far_lane, axis=1, mode="promise_in_bounds"),
        ],
        axis=1,
    )
    high, low = split(e)
    right = jnp.concatenate([high, high, low, jnp.zeros((16, 256), BF16)], axis=0)
    product = jnp.dot(w_fine[...], right, preferred_element_type=F32)

    def ring_block(ox, oy, inner, k):
        return jnp.concatenate([inner, roll(along_z(rz2, from_high_2, ox, oy), -2 * k)], axis=1)

    def layer(ox, j):
        if ox == 0:
            inner = jnp.where(odd_rows, from_side(0, -1, 2 + j), from_side(0, 1, 2 + j))
        else:
            inner = jnp.where(odd_rows, from_side(ox, -1, 2), from_side(ox, 1, 2))
            shift = (-2 * j if ox > 0 else 6 - 2 * j) % 8
            inner = pltpu.roll(inner, shift, 0) if shift else inner
        outer = jnp.where(odd_rows, along_z(rz2, from_high_2, ox, -1), along_z(rz2, from_high_2, ox, 1))
        return jnp.concatenate([inner, roll(outer, -2 * (12 + j))], axis=1)

    low_wide = lax.broadcasted_iota(jnp.int32, (8, 256), 0) < 4
    halves = [[], []]
    for half in range(2):
        for x in ((-1, 0, 1), (2, 3, 4))[half]:
            for j in range(3):
                if x == -1:
                    halves[half].append(ring_block(-1, 0, rx2[0, 2 + j], 9 + j))
                elif x == 4:
                    halves[half].append(ring_block(1, 0, rx2[1, 2 + j], j))
                else:
                    halves[half].append(ring_block(0, 0, before[x, j], 3 * x + j))
    for j in range(3):
        level = layer(0, j)
        halves[0].append(jnp.where(low_wide, level, layer(-1, j)))
        halves[1].append(jnp.where(low_wide, layer(1, j), level))
    start = jnp.concatenate(halves[0] + halves[1], axis=0)

    down = ((1.0 / THETA) * ikc) * z_shift_sum(product, 192)
    x = jnp.where(ring_inside(), start + product[576:768] - down, 0.0)
    applied = operator_local(x)
    x_in, down_in = local_of(x, 3), local_of(down, 3)
    for p in range(4):
        for j in range(3):
            n = 8 * (3 * p + j)
            step = ((1.0 / THETA) * ikc[:, 0:128]) * resid[4 + j, 8 * p : 8 * p + 8, :] - down_in[n : n + 8, 0:128]
            out_ref[j, p] = (
                x_in[n : n + 8, 0:128]
                + MOM * step
                + (WEIGHT * ikc[:, 0:128]) * (main[p, j] - applied[n : n + 8, 0:128])
            )

    for group, choices in groups:
        wait_group(send_sem.at[group], choices)


GROUPS = 5


def scratch():
    vmem = pltpu.VMEM
    return [
        vmem((3, 4, 8, 128), F32),
        vmem((4, 8, 128), F32),
        vmem((4, 8, 128), jnp.int32),
        pltpu.SMEM((8,), F32),
        pltpu.SMEM((3, 3, 27), F32),
        vmem(WIDE_INDEX.shape, jnp.int32),
        vmem(COARSE_INDEX.shape, jnp.int32),
        vmem(FINE_INDEX.shape, jnp.int32),
        vmem(CODE_256.shape, jnp.int32),
        vmem(CODE_128.shape, jnp.int32),
        vmem(FACE_1.shape, BF16),
        vmem(FACE_2.shape, BF16),
        vmem((4, 8, 128), F32),
        vmem((4, 3, 8, 128), F32),
        vmem((4, 8, 128), F32),
        vmem((2, 3, 8, 128), F32),
        vmem((2, 8, 128), F32),
        vmem((2, 2, 2, 8, 128), F32),
        vmem((8, 128), F32),
        vmem((2, 2, 3, 8, 128), F32),
        vmem((2, 3, 8, 128), F32),
        vmem((2, 2, 2, 8, 128), F32),
        vmem((2, 2, 8, 128), F32),
        vmem((2, 8, 128), F32),
        vmem((2, 3, 3, 8, 128), F32),
        vmem((4, 3, 8, 128), F32),
        vmem((3, 8, 128), F32),
        vmem((8, 128), F32),
        vmem((2, 5, 8, 128), F32),
        vmem((5, 8, 128), F32),
        vmem((2, 3, 8, 128), F32),
        vmem((2, 5, 8, 128), F32),
        vmem((2, 5, 8, 128), F32),
        vmem((2, 2, 3, 8, 128), F32),
        vmem((2, 3, 3, 8, 128), F32),
        vmem((9, 16, 128), F32),
        vmem((WIDE_ROWS, 768), BF16),
        vmem((COARSE_ROWS, 512), BF16),
        vmem((FINE_ROWS, 256), BF16),
        vmem((288, 256), F32),
        vmem((96, 256), F32),
        vmem((192, 256), F32),
        vmem((7, 32, 128), F32),
        vmem((32, 8, 128), F32),
        pltpu.SemaphoreType.DMA((10,)),
        pltpu.SemaphoreType.DMA((GROUPS,)),
        pltpu.SemaphoreType.DMA((GROUPS,)),
    ]


def on_device(rhs_velocity, rhs_pressure, layer_ids, visc_table, stencil):
    anywhere = pl.BlockSpec(memory_space=pltpu.HBM)
    inside = pl.BlockSpec(memory_space=pltpu.VMEM)
    return pl.pallas_call(
        body,
        name="stokes",
        out_shape=(
            pltpu.VMEM(rhs_velocity.shape, F32),
            pltpu.VMEM(rhs_pressure.shape, F32),
        ),
        in_specs=[anywhere] * 12,
        out_specs=(inside, inside),
        scratch_shapes=scratch(),
        compiler_params=pltpu.CompilerParams(
            collective_id=0, has_side_effects=True, vmem_limit_bytes=60 * 1024 * 1024
        ),
    )(
        *(
            pltpu.with_memory_space_constraint(value, pltpu.HBM)
            for value in (
                rhs_velocity,
                rhs_pressure,
                layer_ids,
                visc_table,
                stencil.transpose(1, 2, 0),
                jnp.asarray(WIDE_INDEX),
                jnp.asarray(COARSE_INDEX),
                jnp.asarray(FINE_INDEX),
                jnp.asarray(CODE_256),
                jnp.asarray(CODE_128),
                jnp.asarray(FACE_1, BF16),
                jnp.asarray(FACE_2, BF16),
            )
        )
    )


def solution(mesh):
    placed = (P(None, "gx", "gy", "gz"), P("gx", "gy", "gz"), P("gx", "gy", "gz"), P(), P())
    return jax.shard_map(
        on_device,
        mesh=mesh,
        in_specs=placed,
        out_specs=(P(None, "gx", "gy", "gz"), P("gx", "gy", "gz")),
        check_vma=False,
    )
```

```python
import functools

import numpy as np
import jax
import jax.numpy as jnp
from jax import lax
from jax.experimental import pallas as pl
from jax.experimental.pallas import tpu as pltpu
from jax.sharding import PartitionSpec as P

F32 = jnp.float32
BF16 = jnp.bfloat16
MESH = pl.DeviceIdType.MESH

THETA = (1.8 + 0.2) / 2.0
DELTA = (1.8 - 0.2) / 2.0
SIGMA = THETA / DELTA
RHO0 = 1.0 / SIGMA
RHO1 = 1.0 / (2.0 * SIGMA - RHO0)
MOM = RHO1 * RHO0
WEIGHT = 2.0 * RHO1 / DELTA

XLO, XHI, YLO, YHI, ZLO, ZHI, NEVER = 1, 2, 4, 8, 16, 32, 64

ONE, ZERO = 28, 31

CORNER_X = (4, 5, -2, -1)
SIDES = [(dx, dy) for dx in (-1, 0, 1) for dy in (-1, 0, 1) if (dx, dy) != (0, 0)]
AHEAD = [(dx, dy, dz) for dx in (-1, 1, 0) for dy in (0, -1, 1) for dz in (-1, 1)]


def plane_block(x, j):
    return [(x, r, j) for r in range(8)]


def y_block(s, j):
    return [(r // 2, (-2 if s == 0 else 8) + r % 2, j) for r in range(8)]


def c_block(s, j):
    return [(CORNER_X[r // 2], (-2 if s == 0 else 8) + r % 2, j) for r in range(8)]


def edge_block(i, half):
    rows = []
    for r in range(8):
        y = -1 if r % 2 else 8
        if half == 0:
            x = r // 2 if r < 4 else (-1 if r >= 6 else None)
        else:
            x = r // 2 if r >= 4 else (4 if r < 2 else None)
        rows.append(None if x is None else (x, y, i))
    return rows


def rows_wide(comps):
    rows = []
    for x in (-2, -1, 0, 1, 2):
        for j in range(comps):
            rows += plane_block(x, j)
    for block in (y_block, c_block):
        for s in range(2):
            for j in range(comps):
                rows += block(s, j)
    for x in (3, 4, 5):
        for j in range(comps):
            rows += plane_block(x, j)
    return rows


def rows_half(half, comps):
    rows = []
    for x in ((-1, 0, 1), (2, 3, 4))[half]:
        for i in range(comps):
            rows += plane_block(x, i)
    for i in range(comps):
        rows += edge_block(i, half)
    return rows


def rows_ring(comps):
    return rows_half(0, comps) + rows_half(1, comps)


def rows_coarse_in():
    rows = []
    for dx in (-1, 0, 1):
        for j in range(3):
            rows += [(2 * dx + r // 4, r % 4, j) for r in range(8)]
        for j in range(3):
            rows += [(2 * dx + r // 4, r % 4 + (4 if r % 4 < 2 else -4), j) for r in range(8)]
    return rows


def rows_coarse_out():
    rows = []
    for q in range(3):
        for i in range(3):
            for r in range(8):
                n = 8 * q + r
                rows.append((n // 6 - 1, n % 6 - 1, i))
    return rows + [None] * 8


def index_stencil(outs, ins):
    table = np.full((len(outs), len(ins)), ZERO, np.int32)
    for m, out in enumerate(outs):
        if out is None:
            continue
        for k, source in enumerate(ins):
            if source is None:
                continue
            a, b = source[0] - out[0] + 1, source[1] - out[1] + 1
            if 0 <= a <= 2 and 0 <= b <= 2:
                table[m, k] = 3 * (3 * a + b) + source[2]
    return table


def index_same(outs, ins, scale):
    table = np.full((len(outs), len(ins)), ZERO, np.int32)
    for m, out in enumerate(outs):
        if out is None:
            continue
        for k, source in enumerate(ins):
            if source is not None and (out[0] // scale, out[1] // scale, out[2]) == source:
                table[m, k] = ONE
    return table


def index_refined(outs, ins):
    table = np.full((len(outs), len(ins)), ZERO, np.int32)
    for m, out in enumerate(outs):
        if out is None:
            continue
        for k, source in enumerate(ins):
            if source is None:
                continue
            a = [v for v in range(3) if (out[0] + v - 1) // 2 == source[0]]
            b = [v for v in range(3) if (out[1] + v - 1) // 2 == source[1]]
            if a and b:
                segment = (len(a) - 1) + 2 * (len(b) - 1)
                table[m, k] = 32 * segment + 3 * (3 * a[0] + b[0]) + source[2]
    return table


def codes(rows, x_end, y_end, lanes, z_bits):
    table = np.full((len(rows), lanes), NEVER, np.int32)
    z_row = np.full((lanes,), NEVER, np.int32)
    for lane, bits in z_bits:
        z_row[lane] = bits
    for m, row in enumerate(rows):
        if row is None:
            continue
        bits = (XLO if row[0] < 0 else 0) | (XHI if row[0] >= x_end else 0)
        bits |= (YLO if row[1] < 0 else 0) | (YHI if row[1] >= y_end else 0)
        table[m] = bits | z_row
    return table


def face_matrix(outs, ins):
    table = np.zeros((len(outs), len(ins)), np.float32)
    for m, out in enumerate(outs):
        if out is None:
            continue
        for k, source in enumerate(ins):
            if source is not None and abs(source[0] - out[0]) + abs(source[1] - out[1]) == 1:
                table[m, k] = 1.0
    return table


FINE_LANES = [(z, 0) for z in range(128)]
WIDE_Z = FINE_LANES + [(128, ZHI), (129, ZHI), (254, ZLO), (255, ZLO)]
RING_Z = FINE_LANES + [(128, ZHI), (255, ZLO)]
COARSE_Z = [(z, 0) for z in range(64)] + [(64, ZHI), (65, ZHI), (126, ZLO), (127, ZLO)]
COARSE_RING_Z = [(z, 0) for z in range(64)] + [(64, ZHI), (127, ZLO)]

WIDE = rows_wide(3)
RING = rows_ring(3)
LOCAL = [row for x in range(4) for i in range(3) for row in plane_block(x, i)]
HALF_A = rows_half(0, 3)
HALF_B = rows_half(1, 3)
COARSE_IN = rows_coarse_in()
COARSE_OUT = rows_coarse_out()

def triple(table, width):
    wide = np.full((len(table), width), ZERO, np.int32)
    count = table.shape[1]
    for n in range(3):
        wide[:, n * count : (n + 1) * count] = table
    return wide


def single(table):
    return np.concatenate([table, np.full((len(table), 256 - table.shape[1]), ZERO, np.int32)], axis=1)


def place(sections):
    places, at, row = {}, 0, 0
    for name, table, copies in sections:
        places[name] = (at, len(table), copies, row)
        at += len(table)
        row += len(table) * copies
    return places, np.concatenate([section[1] for section in sections], axis=0), row


WIDE_SECTIONS, WIDE_INDEX, WIDE_ROWS = place(
    [
        ("a", single(index_stencil(HALF_A, WIDE[0:256])), 3),
        ("b", single(index_stencil(HALF_B, WIDE[32:288])), 3),
        ("local", single(index_stencil(LOCAL, RING)), 3),
    ]
)
COARSE_SECTIONS, COARSE_INDEX, COARSE_ROWS = place(
    [
        ("coarse", triple(index_stencil(COARSE_OUT, COARSE_IN), 512), 3),
        ("keep", triple(index_same(COARSE_OUT, COARSE_IN, 1), 512), 1),
    ]
)
FINE_SECTIONS, FINE_INDEX, FINE_ROWS = place(
    [
        ("fine", triple(index_refined(RING, COARSE_OUT), 256), 3),
        ("spread", triple(index_same(RING, COARSE_OUT, 2), 256), 1),
    ]
)

CODE_WIDE = codes(WIDE, 4, 8, 256, WIDE_Z)
CODE_RING = codes(RING, 4, 8, 256, RING_Z)
CODE_COARSE = codes(COARSE_IN, 2, 4, 128, COARSE_Z)
CODE_COARSE_RING = codes(COARSE_OUT, 2, 4, 128, COARSE_RING_Z)
CODE_WIDE_P = codes(rows_wide(1), 4, 8, 256, WIDE_Z)
CODE_RING_P = codes(rows_ring(1), 4, 8, 256, RING_Z)
CODE_256 = np.concatenate([CODE_WIDE, CODE_RING, CODE_WIDE_P, CODE_RING_P], axis=0)
CODE_128 = np.concatenate([CODE_COARSE, CODE_COARSE_RING], axis=0)


def face_pair(outs, ins, width, total):
    single = face_matrix(outs, ins)
    table = np.zeros((len(outs), total), np.float32)
    table[:, : single.shape[1]] = single
    table[:, width : width + single.shape[1]] = single
    return table


FACE_1 = face_pair(rows_ring(1), rows_wide(1), 128, 256)
FACE_2 = face_pair([row for x in range(4) for row in plane_block(x, 0)], rows_ring(1), 64, 128)


def split(value):
    high = value.astype(BF16)
    low = (value - high.astype(F32)).astype(BF16)
    return high, low


def z_shift_sum(product, rows):
    lanes = product.shape[1]
    return (
        product[rows : 2 * rows]
        + pltpu.roll(product[0:rows], 1, 1)
        + pltpu.roll(product[2 * rows : 3 * rows], lanes - 1, 1)
    )


def body(
    rhs_hbm, press_hbm, ids_hbm, visc_hbm, stencil_hbm, windex_hbm, cindex_hbm, findex_hbm,
    code256_hbm, code128_hbm, face1_hbm, face2_hbm,
    out_ref, pout_ref,
    rhs, press, ids, visc, stencil, windex, cindex, findex, code256, code128, face1, face2,
    eta, main, qmain, ypack, qpack, cpack, zpack, rx, ry, rc, rqx, rqy, rz,
    before, coarse, zpack2, xsend, ysend, csend, rx2, ry2, rc2, rz2,
    tables, w, w_coarse, w_fine, wide, wide_p, ring_x, resid, blank,
    in_sem, send_sem, recv_sem,
):
    nx, ny, nz = (lax.axis_size(name) for name in ("gx", "gy", "gz"))
    ix, iy, iz = (lax.axis_index(name) for name in ("gx", "gy", "gz"))
    ends = {
        ("x", -1): ix > 0, ("x", 1): ix < nx - 1,
        ("y", -1): iy > 0, ("y", 1): iy < ny - 1,
        ("z", -1): iz > 0, ("z", 1): iz < nz - 1,
    }

    def present(dx, dy, dz):
        found = None
        for axis, step in (("x", dx), ("y", dy), ("z", dz)):
            if step:
                one = ends[axis, step]
                found = one if found is None else jnp.logical_and(found, one)
        return found

    def device(dx, dy, dz):
        return (ix + dx, iy + dy, iz + dz)

    partners = AHEAD + [(dx, dy, 0) for dx, dy in SIDES]
    barrier = pltpu.get_barrier_semaphore()
    expected = 0
    for where in partners:
        there = present(*where)
        expected = expected + there.astype(jnp.int32)

        @pl.when(there)
        def _():
            pl.semaphore_signal(barrier, inc=1, device_id=device(*where), device_id_type=MESH)

    def load(n, pairs):
        for source, target in pairs:
            pltpu.make_async_copy(source, target, in_sem.at[n]).start()

    def tiles(count):
        return blank.at[pl.ds(0, count)]

    def loaded(n, count):
        pltpu.make_async_copy(tiles(count), tiles(count), in_sem.at[n]).wait()

    visc_load = pltpu.make_async_copy(visc_hbm, visc, in_sem.at[0])
    visc_load.start()
    load(1, [(ids_hbm, ids), (rhs_hbm, rhs), (press_hbm, press)])
    stencil_load = pltpu.make_async_copy(stencil_hbm, stencil, in_sem.at[2])
    stencil_load.start()
    windex_load = pltpu.make_async_copy(windex_hbm, windex, in_sem.at[3])
    windex_load.start()
    rest = [
        pltpu.make_async_copy(source, target, in_sem.at[4 + n])
        for n, (source, target) in enumerate(
            [
                (code256_hbm, code256), (code128_hbm, code128), (cindex_hbm, cindex), (findex_hbm, findex),
                (face1_hbm, face1), (face2_hbm, face2),
            ]
        )
    ]
    for copy in rest:
        copy.start()

    groups = []

    def send(group, source, target, where):
        copy = pltpu.make_async_remote_copy(
            src_ref=source,
            dst_ref=target,
            send_sem=send_sem.at[group],
            recv_sem=recv_sem.at[group],
            device_id=device(*where),
            device_id_type=MESH,
        )
        pl.when(present(*where))(copy.start)

    count_x, count_y, count_z = (
        ends[axis, -1].astype(jnp.int32) + ends[axis, 1].astype(jnp.int32) for axis in "xyz"
    )

    def wait_group(semaphore, choices):
        for there, count in choices:

            @pl.when(there)
            def _():
                pltpu.make_async_copy(tiles(count), tiles(count), semaphore).wait()

    def plane_choices(corner, along_x, along_y):
        return [
            (
                jnp.logical_and(count_x == nx, count_y == ny),
                corner * nx * ny + along_x * nx + along_y * ny,
            )
            for nx in (1, 2)
            for ny in (1, 2)
        ]

    def ahead_choices():
        return [
            (
                jnp.logical_and(jnp.logical_and(count_x == nx, count_y == ny), count_z == nz),
                (nx + 1) * (ny + 1) * nz,
            )
            for nx in (1, 2)
            for ny in (1, 2)
            for nz in (1, 2)
        ]

    def receive(group, choices):
        wait_group(recv_sem.at[group], choices)
        groups.append((group, choices))

    bad = NEVER
    for bit, end in (
        (XLO, ("x", -1)), (XHI, ("x", 1)), (YLO, ("y", -1)), (YHI, ("y", 1)), (ZLO, ("z", -1)), (ZHI, ("z", 1)),
    ):
        bad = bad + bit * (1 - ends[end].astype(jnp.int32))

    lane8 = lax.broadcasted_iota(jnp.int32, (8, 128), 1)
    row8 = lax.broadcasted_iota(jnp.int32, (8, 128), 0)
    low_rows = row8 < 4
    odd_rows = (row8 & 1) == 1

    def inside(code):
        return (code & bad) == 0

    def roll(value, shift):
        return pltpu.roll(value, shift % 128, 1) if shift % 128 else value

    visc_load.wait()
    loaded(1, 20)
    for p in range(4):
        layer = ids[p]
        value = jnp.zeros((8, 128), F32)
        for k in range(8):
            value = value + jnp.where(layer == k, visc[k], 0.0)
        eta[p] = value
        inverse = 1.0 / value
        for j in range(3):
            main[p, j] = rhs[j, p] * inverse
        qmain[p] = press[p] * value

    for s in range(2):
        for p in range(4):
            for j in range(3):
                ypack[s, j, 2 * p : 2 * p + 2, :] = main[p, j, 6 * s : 6 * s + 2, :]
            qpack[s, 2 * p : 2 * p + 2, :] = qmain[p, 6 * s : 6 * s + 2, :]
    for s in range(2):
        for v, (one, two) in enumerate(((ypack[s, 0], ypack[s, 1]), (ypack[s, 2], qpack[s]))):
            two = pltpu.roll(two, 4, 0)
            cpack[0, s, v] = jnp.where(low_rows, one, two)
            cpack[1, s, v] = jnp.where(low_rows, two, one)
    items = []
    for p in range(4):
        items += [main[p, j] for j in range(3)] + [qmain[p]]
    for s in range(2):
        items += [ypack[s, j] for j in range(3)] + [qpack[s]]
    total = jnp.zeros((8, 128), F32)
    for k, value in enumerate(items):
        total = jnp.where(((lane8 + (130 - 4 * k)) & 127) < 4, roll(value, 4 * k), total)
    zpack[...] = total

    pl.semaphore_wait(barrier, expected)

    def send_ahead(group, source, slots):
        for dx, dy, dz in AHEAD:
            send(group, source, slots.at[0 if dz > 0 else 1, 1 - dx, 1 - dy], (dx, dy, dz))

    send_ahead(0, zpack, rz)
    for dx in (-1, 1):
        for dy in (-1, 1):
            send(
                1,
                cpack.at[0 if dx < 0 else 1, 0 if dy < 0 else 1],
                rc.at[0 if dx > 0 else 1, 0 if dy > 0 else 1],
                (dx, dy, 0),
            )
        planes = pl.ds(0 if dx < 0 else 2, 2)
        send(1, main.at[planes], rx.at[0 if dx > 0 else 1], (dx, 0, 0))
    for dy in (-1, 1):
        send(1, ypack.at[0 if dy < 0 else 1], ry.at[0 if dy > 0 else 1], (0, dy, 0))
    for dx in (-1, 1):
        planes = pl.ds(0 if dx < 0 else 2, 2)
        send(2, qmain.at[planes], rqx.at[0 if dx > 0 else 1], (dx, 0, 0))
    for dy in (-1, 1):
        send(2, qpack.at[0 if dy < 0 else 1], rqy.at[0 if dy > 0 else 1], (0, dy, 0))

    stencil_load.wait()
    kc = (stencil[0, 0, 13] + stencil[1, 1, 13] + stencil[2, 2, 13]) / 3.0
    for c in range(3):
        rows = []
        for i in range(3):
            base = jnp.zeros((8, 128), F32)
            for a in range(3):
                for b in range(3):
                    for j in range(3):
                        at = 3 * (3 * a + b) + j
                        base = jnp.where(lane8 == at, stencil[i, j, 9 * a + 3 * b + c], base)
            low = lane8 < 27
            pair_a = base + jnp.where(low, roll(base, -9), 0.0)
            pair_b = base + jnp.where(low, roll(base, -3), 0.0)
            pair_ab = pair_a + jnp.where(low, roll(pair_a, -3), 0.0)
            full = base + roll(pair_a, 32) + roll(pair_b, 64) + roll(pair_ab, 96)
            rows.append(jnp.where(lane8 == ONE, 1.0, full))
        for combo, (one, two) in enumerate(((0, 1), (2, 0), (1, 2))):
            tables[3 * c + combo, 0:8, :] = rows[one]
            tables[3 * c + combo, 8:16, :] = rows[two]

    lane16 = lax.broadcasted_iota(jnp.int32, (16, 128), 1)

    def build(index, section, target, tiles, width, unroll):
        at, count, copies, first = section

        def chunk(t):
            combo = lax.rem(t, 3)
            start = pl.multiple_of(t * 16, 16)
            for tile in range(tiles):
                lanes = slice(128 * tile, 128 * tile + 128)
                picked = index[pl.ds(at + start, 16), lanes]
                for c in range(copies):
                    value = jnp.take_along_axis(
                        tables[3 * c + combo], picked, axis=1, mode="promise_in_bounds"
                    )
                    rows = pl.ds(first + c * count + start, 16)
                    if width is None:
                        high, low = split(value)
                        target[rows, lanes] = high
                        target[rows, 256 + 128 * tile : 384 + 128 * tile] = low
                        target[rows, 512 + 128 * tile : 640 + 128 * tile] = high
                    else:
                        low = value - value.astype(BF16).astype(F32)
                        lane = lane16 + 128 * tile
                        value = jnp.where((lane >= width) & (lane < 2 * width), low, value)
                        target[rows, lanes] = value.astype(BF16)

        def step(t, carry):
            for n in range(unroll):
                chunk(t * unroll + n)
            return carry

        lax.fori_loop(0, count // (16 * unroll), step, 0)

    windex_load.wait()
    for name in ("a", "b", "local"):
        build(windex, WIDE_SECTIONS[name], w, 2, None, 3)
    for copy in rest:
        copy.wait()
    for name in ("coarse", "keep"):
        build(cindex, COARSE_SECTIONS[name], w_coarse, 4, 144, 1)
    for name in ("fine", "spread"):
        build(findex, FINE_SECTIONS[name], w_fine, 2, 80, 3)

    def along_z(slots, select, ox, oy):
        return jnp.where(select, slots[1, ox + 1, oy + 1], slots[0, ox + 1, oy + 1])

    from_high_1 = (lane8 & 3) < 2
    from_high_2 = ((lane8 < 32) & ((lane8 & 1) == 0)) | ((lane8 >= 64) & (lane8 < 127))

    def wide_blocks(comp, tile):
        comps = 4

        def edge(ox, oy, k):
            return roll(along_z(rz, from_high_1, ox, oy), -4 * k)

        blocks = {}
        for p in range(4):
            own = main[p, comp] if comp < 3 else qmain[p]
            blocks[p] = edge(0, 0, p * comps + comp) if tile else own
        for n in range(2):
            for side, ox, first in ((0, -1, -2), (1, 1, 4)):
                near = rx[side, n, comp] if comp < 3 else rqx[side, n]
                plane = n if ox > 0 else n + 2
                blocks[first + n] = edge(ox, 0, plane * comps + comp) if tile else near
        for s, oy in enumerate((-1, 1)):
            k = 4 * comps + (1 - s) * comps + comp
            if tile:
                blocks["y", s] = edge(0, oy, k)
                blocks["c", s] = jnp.where(low_rows, edge(1, oy, k), edge(-1, oy, k))
                continue
            blocks["y", s] = ry[s, comp] if comp < 3 else rqy[s]
            below, above = rc[0, s, comp // 2], rc[1, s, comp // 2]
            if comp % 2 == 0:
                blocks["c", s] = jnp.where(low_rows, above, below)
            else:
                blocks["c", s] = pltpu.roll(jnp.where(low_rows, below, above), 4, 0)
        return blocks

    def store_wide(target, comps, code_at, tile):
        lanes = slice(128 * tile, 128 * tile + 128)
        for slot, comp in enumerate(comps):
            blocks = wide_blocks(comp, tile)
            order = [-2, -1, 0, 1, 2, ("y", 0), ("y", 1), ("c", 0), ("c", 1), 3, 4, 5]
            for n, key in enumerate(order):
                at = 8 * (n * len(comps) + slot)
                code = code256[code_at + at : code_at + at + 8, lanes]
                target[at : at + 8, lanes] = jnp.where(inside(code), blocks[key], 0.0)

    def ring_of(source, comps):
        def block(n):
            return source[8 * comps * n : 8 * comps * (n + 1), :]

        row = lax.broadcasted_iota(jnp.int32, (8 * comps, 256), 0)
        odd, low = (row & 1) == 1, (row & 7) < 4
        level = jnp.where(odd, block(5), block(6))
        corner = jnp.where(odd, block(7), block(8))
        return jnp.concatenate(
            [
                block(1), block(2), block(3), jnp.where(low, level, corner),
                block(4), block(9), block(10), jnp.where(low, corner, level),
            ],
            axis=0,
        )

    def local_of(ring, comps):
        return jnp.concatenate([ring[8 * comps : 24 * comps], ring[32 * comps : 48 * comps]], axis=0)

    def operator_ring():
        parts = []
        for name, start in (("a", 0), ("b", 32)):
            high, low = split(wide[start : start + 256, :])
            right = jnp.concatenate([high, high, low], axis=0)
            base = WIDE_SECTIONS[name][3]
            product = jnp.dot(w[base : base + 288, :], right, preferred_element_type=F32)
            parts.append(z_shift_sum(product, 96))
        return jnp.concatenate(parts, axis=0)

    def operator_local(value):
        high, low = split(value)
        gap = jnp.zeros((64, 256), BF16)
        right = jnp.concatenate([high, gap, high, gap, low, gap], axis=0)
        base = WIDE_SECTIONS["local"][3]
        product = jnp.dot(w[base : base + 288, :], right, preferred_element_type=F32)
        return z_shift_sum(product, 96)

    ikc = (jnp.full((8, 256), 1.0, F32) / kc)[0:1, :]
    gain_u = ((1.0 + MOM + WEIGHT * THETA) / THETA) * ikc
    gain_s = (-WEIGHT / THETA) * ikc * ikc

    ring_code = len(CODE_WIDE)
    wide_p_code = ring_code + len(CODE_RING)
    ring_p_code = wide_p_code + len(CODE_WIDE_P)

    def ring_inside():
        return inside(code256[ring_code : ring_code + 192, :])

    receive(1, plane_choices(2, 6, 3))
    store_wide(wide, (0, 1, 2), 0, 0)
    receive(0, ahead_choices())

    store_wide(wide, (0, 1, 2), 0, 1)
    x2 = jnp.where(ring_inside(), gain_u * ring_of(wide, 3) + gain_s * operator_ring(), 0.0)
    ring_x[...] = x2

    applied = operator_local(x2)
    even = (lane8 * 2) & 127

    def coarse_sum(source, n):
        value = source[n, pl.ds(0, 8, 2), :] + source[n, pl.ds(1, 8, 2), :]
        value = value + roll(value, -1)
        return jnp.take_along_axis(value, even, axis=1, mode="promise_in_bounds")

    def local_row(p):
        return 8 * (3 + 3 * p if p < 2 else 6 + 3 * p)

    for big in range(2):
        resid[3, 8 * big : 8 * big + 8, :] = eta[2 * big] + eta[2 * big + 1]
        for j in range(3):
            total = jnp.zeros((8, 128), F32)
            for p in (2 * big, 2 * big + 1):
                n = 8 * (3 * p + j)
                left = main[p, j] - applied[n : n + 8, 0:128]
                resid[4 + j, 8 * p : 8 * p + 8, :] = left
                at = local_row(p) + 8 * j
                value = ring_x[at : at + 8, 0:128] + ((1.0 / THETA) * ikc[:, 0:128]) * left
                before[p, j] = value
                total = total + eta[p] * left
            resid[j, 8 * big : 8 * big + 8, :] = total
    four_over = 4.0 / coarse_sum(resid, 3)
    total = jnp.zeros((8, 128), F32)
    for j in range(3):
        value = coarse_sum(resid, j) * four_over
        coarse[j] = value
        first = (lane8 >= 98 + 4 * j) & (lane8 < 100 + 4 * j)
        last = (lane8 >= 32 + 4 * j) & (lane8 < 34 + 4 * j)
        total = jnp.where(first | last, roll(value, 98 + 4 * j), total)
        for p in range(4):
            ysend[2 + j, 2 * p : 2 * p + 1, :] = before[p, j, 0:1, :]
            ysend[2 + j, 2 * p + 1 : 2 * p + 2, :] = before[p, j, 7:8, :]
            if p in (0, 3):
                n = 0 if p == 0 else 1
                xsend[n, 2 + j] = before[p, j]
                csend[n, 2, 2 * j : 2 * j + 1, :] = before[p, j, 0:1, :]
                csend[n, 2, 2 * j + 1 : 2 * j + 2, :] = before[p, j, 7:8, :]
    items = [before[p, j] for p in range(4) for j in range(3)] + [ysend[2 + j] for j in range(3)]
    for k, value in enumerate(items):
        total = jnp.where(((lane8 + (129 - 2 * k)) & 127) < 2, roll(value, 2 * k), total)
    zpack2[...] = total
    for n, value in enumerate((jnp.where(lane8 < 64, coarse[0], roll(coarse[1], 64)), coarse[2])):
        ysend[n] = value
        for m in range(2):
            xsend[m, n] = value
            csend[m, n] = value
    send_ahead(3, zpack2, rz2)
    for dx in (-1, 1):
        for dy in (-1, 1):
            send(
                4,
                csend.at[0 if dx < 0 else 1],
                rc2.at[0 if dx > 0 else 1, 0 if dy > 0 else 1],
                (dx, dy, 0),
            )
        send(4, xsend.at[0 if dx < 0 else 1], rx2.at[0 if dx > 0 else 1], (dx, 0, 0))
    for dy in (-1, 1):
        send(4, ysend, ry2.at[0 if dy > 0 else 1], (0, dy, 0))

    receive(2, plane_choices(0, 2, 1))
    store_wide(wide_p, (3,), wide_p_code, 0)
    store_wide(wide_p, (3,), wide_p_code, 1)
    q_ring = ring_of(wide_p, 1)
    high, low = split(wide_p[...])
    gap = jnp.zeros((32, 256), BF16)
    near = jnp.dot(face1[...], jnp.concatenate([high, gap, low, gap], axis=0), preferred_element_type=F32)
    near = near + pltpu.roll(q_ring, 1, 1) + pltpu.roll(q_ring, 255, 1)
    p_ring = (4.0 / 27.0) * q_ring + (1.0 / 81.0) * near
    p_ring = jnp.where(inside(code256[ring_p_code : ring_p_code + 64, :]), p_ring, 0.0)
    high, low = split(p_ring)
    near = jnp.dot(face2[...], jnp.concatenate([high, low], axis=0), preferred_element_type=F32)
    p_in, q_in = local_of(p_ring, 1), local_of(q_ring, 1)
    near = near + pltpu.roll(p_in, 1, 1) + pltpu.roll(p_in, 255, 1)
    p_out = (1.0 / 3.0) * p_in + (1.0 / 9.0) * q_in + (1.0 / 9.0) * near
    for p in range(4):
        pout_ref[p] = p_out[8 * p : 8 * p + 8, 0:128]
    receive(4, plane_choices(3, 5, 5))
    receive(3, ahead_choices())

    def from_side(ox, oy, n):
        if ox and oy:
            return rc2[0 if ox < 0 else 1, 0 if oy < 0 else 1, n]
        return rx2[0 if ox < 0 else 1, n] if ox else ry2[0 if oy < 0 else 1, n]

    def coarse_block(ox, oy, j):
        if (ox, oy) == (0, 0):
            inner = coarse[j]
        else:
            inner = from_side(ox, oy, j // 2)
            inner = roll(inner, 64) if j == 1 else inner
        return jnp.where(lane8 < 64, inner, roll(along_z(rz2, from_high_2, ox, oy), -(34 + 4 * j)))

    blocks = []
    near_high = (row8 & 3) < 2
    for ox in (-1, 0, 1):
        blocks += [coarse_block(ox, 0, j) for j in range(3)]
        blocks += [jnp.where(near_high, coarse_block(ox, 1, j), coarse_block(ox, -1, j)) for j in range(3)]
    value = jnp.where(inside(code128[0:144, :]), jnp.concatenate(blocks, axis=0), 0.0)
    high, low = split(value)
    right = jnp.concatenate([high, high, low, jnp.zeros((80, 128), BF16)], axis=0)
    product = jnp.dot(w_coarse[...], right, preferred_element_type=F32)
    e = gain_u[:, 0:128] * product[240:320] + gain_s[:, 0:128] * z_shift_sum(product, 80)
    e = jnp.where(inside(code128[144:224, :]), e, 0.0)
    lane80 = lax.broadcasted_iota(jnp.int32, (80, 128), 1)
    near_lane = lane80 >> 1
    far_lane = jnp.where(lane80 < 2, 64, jnp.where(lane80 >= 126, 127, 100))
    e = jnp.concatenate(
        [
            jnp.take_along_axis(e, near_lane, axis=1, mode="promise_in_bounds"),
            jnp.take_along_axis(e, far_lane, axis=1, mode="promise_in_bounds"),
        ],
        axis=1,
    )
    high, low = split(e)
    right = jnp.concatenate([high, high, low, jnp.zeros((16, 256), BF16)], axis=0)
    product = jnp.dot(w_fine[...], right, preferred_element_type=F32)

    def ring_block(ox, oy, inner, k):
        return jnp.concatenate([inner, roll(along_z(rz2, from_high_2, ox, oy), -2 * k)], axis=1)

    def layer(ox, j):
        if ox == 0:
            inner = jnp.where(odd_rows, from_side(0, -1, 2 + j), from_side(0, 1, 2 + j))
        else:
            inner = jnp.where(odd_rows, from_side(ox, -1, 2), from_side(ox, 1, 2))
            shift = (-2 * j if ox > 0 else 6 - 2 * j) % 8
            inner = pltpu.roll(inner, shift, 0) if shift else inner
        outer = jnp.where(odd_rows, along_z(rz2, from_high_2, ox, -1), along_z(rz2, from_high_2, ox, 1))
        return jnp.concatenate([inner, roll(outer, -2 * (12 + j))], axis=1)

    low_wide = lax.broadcasted_iota(jnp.int32, (8, 256), 0) < 4
    halves = [[], []]
    for half in range(2):
        for x in ((-1, 0, 1), (2, 3, 4))[half]:
            for j in range(3):
                if x == -1:
                    halves[half].append(ring_block(-1, 0, rx2[0, 2 + j], 9 + j))
                elif x == 4:
                    halves[half].append(ring_block(1, 0, rx2[1, 2 + j], j))
                else:
                    halves[half].append(ring_block(0, 0, before[x, j], 3 * x + j))
    for j in range(3):
        level = layer(0, j)
        halves[0].append(jnp.where(low_wide, level, layer(-1, j)))
        halves[1].append(jnp.where(low_wide, layer(1, j), level))
    start = jnp.concatenate(halves[0] + halves[1], axis=0)

    down = ((1.0 / THETA) * ikc) * z_shift_sum(product, 192)
    x = jnp.where(ring_inside(), start + product[576:768] - down, 0.0)
    applied = operator_local(x)
    x_in, down_in = local_of(x, 3), local_of(down, 3)
    for p in range(4):
        for j in range(3):
            n = 8 * (3 * p + j)
            step = ((1.0 / THETA) * ikc[:, 0:128]) * resid[4 + j, 8 * p : 8 * p + 8, :] - down_in[n : n + 8, 0:128]
            out_ref[j, p] = (
                x_in[n : n + 8, 0:128]
                + MOM * step
                + (WEIGHT * ikc[:, 0:128]) * (main[p, j] - applied[n : n + 8, 0:128])
            )

    for group, choices in groups:
        wait_group(send_sem.at[group], choices)


GROUPS = 5


def scratch():
    vmem = pltpu.VMEM
    return [
        vmem((3, 4, 8, 128), F32),
        vmem((4, 8, 128), F32),
        vmem((4, 8, 128), jnp.int32),
        pltpu.SMEM((8,), F32),
        pltpu.SMEM((3, 3, 27), F32),
        vmem(WIDE_INDEX.shape, jnp.int32),
        vmem(COARSE_INDEX.shape, jnp.int32),
        vmem(FINE_INDEX.shape, jnp.int32),
        vmem(CODE_256.shape, jnp.int32),
        vmem(CODE_128.shape, jnp.int32),
        vmem(FACE_1.shape, BF16),
        vmem(FACE_2.shape, BF16),
        vmem((4, 8, 128), F32),
        vmem((4, 3, 8, 128), F32),
        vmem((4, 8, 128), F32),
        vmem((2, 3, 8, 128), F32),
        vmem((2, 8, 128), F32),
        vmem((2, 2, 2, 8, 128), F32),
        vmem((8, 128), F32),
        vmem((2, 2, 3, 8, 128), F32),
        vmem((2, 3, 8, 128), F32),
        vmem((2, 2, 2, 8, 128), F32),
        vmem((2, 2, 8, 128), F32),
        vmem((2, 8, 128), F32),
        vmem((2, 3, 3, 8, 128), F32),
        vmem((4, 3, 8, 128), F32),
        vmem((3, 8, 128), F32),
        vmem((8, 128), F32),
        vmem((2, 5, 8, 128), F32),
        vmem((5, 8, 128), F32),
        vmem((2, 3, 8, 128), F32),
        vmem((2, 5, 8, 128), F32),
        vmem((2, 5, 8, 128), F32),
        vmem((2, 2, 3, 8, 128), F32),
        vmem((2, 3, 3, 8, 128), F32),
        vmem((9, 16, 128), F32),
        vmem((WIDE_ROWS, 768), BF16),
        vmem((COARSE_ROWS, 512), BF16),
        vmem((FINE_ROWS, 256), BF16),
        vmem((288, 256), F32),
        vmem((96, 256), F32),
        vmem((192, 256), F32),
        vmem((7, 32, 128), F32),
        vmem((32, 8, 128), F32),
        pltpu.SemaphoreType.DMA((10,)),
        pltpu.SemaphoreType.DMA((GROUPS,)),
        pltpu.SemaphoreType.DMA((GROUPS,)),
    ]


def store_results(velocity, pressure, velocity_out, pressure_out, sem):
    one = pltpu.make_async_copy(velocity, velocity_out, sem.at[0])
    two = pltpu.make_async_copy(pressure, pressure_out, sem.at[1])
    one.start()
    two.start()
    one.wait()
    two.wait()


def on_device(rhs_velocity, rhs_pressure, layer_ids, visc_table, stencil):
    anywhere = pl.BlockSpec(memory_space=pltpu.HBM)
    inside = pl.BlockSpec(memory_space=pltpu.VMEM)
    results = pl.pallas_call(
        body,
        name="stokes",
        out_shape=(
            pltpu.VMEM(rhs_velocity.shape, F32),
            pltpu.VMEM(rhs_pressure.shape, F32),
        ),
        in_specs=[anywhere] * 12,
        out_specs=(inside, inside),
        scratch_shapes=scratch(),
        compiler_params=pltpu.CompilerParams(
            collective_id=0, has_side_effects=True, vmem_limit_bytes=60 * 1024 * 1024
        ),
    )(
        *(
            pltpu.with_memory_space_constraint(value, pltpu.HBM)
            for value in (
                rhs_velocity,
                rhs_pressure,
                layer_ids,
                visc_table,
                stencil.transpose(1, 2, 0),
                jnp.asarray(WIDE_INDEX),
                jnp.asarray(COARSE_INDEX),
                jnp.asarray(FINE_INDEX),
                jnp.asarray(CODE_256),
                jnp.asarray(CODE_128),
                jnp.asarray(FACE_1, BF16),
                jnp.asarray(FACE_2, BF16),
            )
        )
    )
    return pl.pallas_call(
        store_results,
        name="store",
        out_shape=(
            jax.ShapeDtypeStruct(rhs_velocity.shape, F32),
            jax.ShapeDtypeStruct(rhs_pressure.shape, F32),
        ),
        in_specs=[inside] * 2,
        out_specs=(anywhere,) * 2,
        scratch_shapes=[pltpu.SemaphoreType.DMA((2,))],
    )(*(pltpu.with_memory_space_constraint(value, pltpu.VMEM) for value in results))


def solution(mesh):
    placed = (P(None, "gx", "gy", "gz"), P("gx", "gy", "gz"), P("gx", "gy", "gz"), P(), P())
    return jax.shard_map(
        on_device,
        mesh=mesh,
        in_specs=placed,
        out_specs=(P(None, "gx", "gy", "gz"), P("gx", "gy", "gz")),
        check_vma=False,
    )
```

```python
import functools

import numpy as np
import jax
import jax.numpy as jnp
from jax import lax
from jax.experimental import pallas as pl
from jax.experimental.pallas import tpu as pltpu
from jax.sharding import PartitionSpec as P

F32 = jnp.float32
BF16 = jnp.bfloat16
MESH = pl.DeviceIdType.MESH

THETA = (1.8 + 0.2) / 2.0
DELTA = (1.8 - 0.2) / 2.0
SIGMA = THETA / DELTA
RHO0 = 1.0 / SIGMA
RHO1 = 1.0 / (2.0 * SIGMA - RHO0)
MOM = RHO1 * RHO0
WEIGHT = 2.0 * RHO1 / DELTA

XLO, XHI, YLO, YHI, ZLO, ZHI, NEVER = 1, 2, 4, 8, 16, 32, 64

ONE, ZERO = 28, 31

CORNER_X = (4, 5, -2, -1)
SIDES = [(dx, dy) for dx in (-1, 0, 1) for dy in (-1, 0, 1) if (dx, dy) != (0, 0)]
AHEAD = [(dx, dy, dz) for dx in (-1, 1, 0) for dy in (0, -1, 1) for dz in (-1, 1)]


def plane_block(x, j):
    return [(x, r, j) for r in range(8)]


def y_block(s, j):
    return [(r // 2, (-2 if s == 0 else 8) + r % 2, j) for r in range(8)]


def c_block(s, j):
    return [(CORNER_X[r // 2], (-2 if s == 0 else 8) + r % 2, j) for r in range(8)]


def edge_block(i, half):
    rows = []
    for r in range(8):
        y = -1 if r % 2 else 8
        if half == 0:
            x = r // 2 if r < 4 else (-1 if r >= 6 else None)
        else:
            x = r // 2 if r >= 4 else (4 if r < 2 else None)
        rows.append(None if x is None else (x, y, i))
    return rows


def rows_wide(comps):
    rows = []
    for x in (-2, -1, 0, 1, 2):
        for j in range(comps):
            rows += plane_block(x, j)
    for block in (y_block, c_block):
        for s in range(2):
            for j in range(comps):
                rows += block(s, j)
    for x in (3, 4, 5):
        for j in range(comps):
            rows += plane_block(x, j)
    return rows


def rows_half(half, comps):
    rows = []
    for x in ((-1, 0, 1), (2, 3, 4))[half]:
        for i in range(comps):
            rows += plane_block(x, i)
    for i in range(comps):
        rows += edge_block(i, half)
    return rows


def rows_ring(comps):
    return rows_half(0, comps) + rows_half(1, comps)


def rows_coarse_in():
    rows = []
    for dx in (-1, 0, 1):
        for j in range(3):
            rows += [(2 * dx + r // 4, r % 4, j) for r in range(8)]
        for j in range(3):
            rows += [(2 * dx + r // 4, r % 4 + (4 if r % 4 < 2 else -4), j) for r in range(8)]
    return rows


def rows_coarse_out():
    rows = []
    for q in range(3):
        for i in range(3):
            for r in range(8):
                n = 8 * q + r
                rows.append((n // 6 - 1, n % 6 - 1, i))
    return rows + [None] * 8


def index_stencil(outs, ins):
    table = np.full((len(outs), len(ins)), ZERO, np.int32)
    for m, out in enumerate(outs):
        if out is None:
            continue
        for k, source in enumerate(ins):
            if source is None:
                continue
            a, b = source[0] - out[0] + 1, source[1] - out[1] + 1
            if 0 <= a <= 2 and 0 <= b <= 2:
                table[m, k] = 3 * (3 * a + b) + source[2]
    return table


def index_same(outs, ins, scale):
    table = np.full((len(outs), len(ins)), ZERO, np.int32)
    for m, out in enumerate(outs):
        if out is None:
            continue
        for k, source in enumerate(ins):
            if source is not None and (out[0] // scale, out[1] // scale, out[2]) == source:
                table[m, k] = ONE
    return table


def index_refined(outs, ins):
    table = np.full((len(outs), len(ins)), ZERO, np.int32)
    for m, out in enumerate(outs):
        if out is None:
            continue
        for k, source in enumerate(ins):
            if source is None:
                continue
            a = [v for v in range(3) if (out[0] + v - 1) // 2 == source[0]]
            b = [v for v in range(3) if (out[1] + v - 1) // 2 == source[1]]
            if a and b:
                segment = (len(a) - 1) + 2 * (len(b) - 1)
                table[m, k] = 32 * segment + 3 * (3 * a[0] + b[0]) + source[2]
    return table


def codes(rows, x_end, y_end, lanes, z_bits):
    table = np.full((len(rows), lanes), NEVER, np.int32)
    z_row = np.full((lanes,), NEVER, np.int32)
    for lane, bits in z_bits:
        z_row[lane] = bits
    for m, row in enumerate(rows):
        if row is None:
            continue
        bits = (XLO if row[0] < 0 else 0) | (XHI if row[0] >= x_end else 0)
        bits |= (YLO if row[1] < 0 else 0) | (YHI if row[1] >= y_end else 0)
        table[m] = bits | z_row
    return table


def face_matrix(outs, ins):
    table = np.zeros((len(outs), len(ins)), np.float32)
    for m, out in enumerate(outs):
        if out is None:
            continue
        for k, source in enumerate(ins):
            if source is not None and abs(source[0] - out[0]) + abs(source[1] - out[1]) == 1:
                table[m, k] = 1.0
    return table


FINE_LANES = [(z, 0) for z in range(128)]
WIDE_Z = FINE_LANES + [(128, ZHI), (129, ZHI), (254, ZLO), (255, ZLO)]
RING_Z = FINE_LANES + [(128, ZHI), (255, ZLO)]
COARSE_Z = [(z, 0) for z in range(64)] + [(64, ZHI), (65, ZHI), (126, ZLO), (127, ZLO)]
COARSE_RING_Z = [(z, 0) for z in range(64)] + [(64, ZHI), (127, ZLO)]

WIDE = rows_wide(3)
RING = rows_ring(3)
LOCAL = [row for x in range(4) for i in range(3) for row in plane_block(x, i)]
HALF_A = rows_half(0, 3)
HALF_B = rows_half(1, 3)
COARSE_IN = rows_coarse_in()
COARSE_OUT = rows_coarse_out()

def triple(table, width):
    wide = np.full((len(table), width), ZERO, np.int32)
    count = table.shape[1]
    for n in range(3):
        wide[:, n * count : (n + 1) * count] = table
    return wide


def single(table):
    return np.concatenate([table, np.full((len(table), 256 - table.shape[1]), ZERO, np.int32)], axis=1)


def place(sections):
    places, at, row = {}, 0, 0
    for name, table, copies in sections:
        places[name] = (at, len(table), copies, row)
        at += len(table)
        row += len(table) * copies
    return places, np.concatenate([section[1] for section in sections], axis=0), row


WIDE_SECTIONS, WIDE_INDEX, WIDE_ROWS = place(
    [
        ("a", single(index_stencil(HALF_A, WIDE[0:256])), 3),
        ("b", single(index_stencil(HALF_B, WIDE[32:288])), 3),
        ("local", single(index_stencil(LOCAL, RING)), 3),
    ]
)
COARSE_SECTIONS, COARSE_INDEX, COARSE_ROWS = place(
    [
        ("coarse", triple(index_stencil(COARSE_OUT, COARSE_IN), 512), 3),
        ("keep", triple(index_same(COARSE_OUT, COARSE_IN, 1), 512), 1),
    ]
)
FINE_SECTIONS, FINE_INDEX, FINE_ROWS = place(
    [
        ("fine", triple(index_refined(RING, COARSE_OUT), 256), 3),
        ("spread", triple(index_same(RING, COARSE_OUT, 2), 256), 1),
    ]
)

CODE_WIDE = codes(WIDE, 4, 8, 256, WIDE_Z)
CODE_RING = codes(RING, 4, 8, 256, RING_Z)
CODE_COARSE = codes(COARSE_IN, 2, 4, 128, COARSE_Z)
CODE_COARSE_RING = codes(COARSE_OUT, 2, 4, 128, COARSE_RING_Z)
CODE_WIDE_P = codes(rows_wide(1), 4, 8, 256, WIDE_Z)
CODE_RING_P = codes(rows_ring(1), 4, 8, 256, RING_Z)
CODE_256 = np.concatenate([CODE_WIDE, CODE_RING, CODE_WIDE_P, CODE_RING_P], axis=0)
CODE_128 = np.concatenate([CODE_COARSE, CODE_COARSE_RING], axis=0)


def face_pair(outs, ins, width, total):
    single = face_matrix(outs, ins)
    table = np.zeros((len(outs), total), np.float32)
    table[:, : single.shape[1]] = single
    table[:, width : width + single.shape[1]] = single
    return table


FACE_1 = face_pair(rows_ring(1), rows_wide(1), 128, 256)
FACE_2 = face_pair([row for x in range(4) for row in plane_block(x, 0)], rows_ring(1), 64, 128)


def split(value):
    high = value.astype(BF16)
    low = (value - high.astype(F32)).astype(BF16)
    return high, low


def z_shift_sum(product, rows):
    lanes = product.shape[1]
    return (
        product[rows : 2 * rows]
        + pltpu.roll(product[0:rows], 1, 1)
        + pltpu.roll(product[2 * rows : 3 * rows], lanes - 1, 1)
    )


def body(
    rhs_hbm, press_hbm, ids_hbm, visc_hbm, stencil_hbm, windex_hbm, cindex_hbm, findex_hbm,
    code256_hbm, code128_hbm, face1_hbm, face2_hbm,
    out_ref, pout_ref,
    rhs, press, ids, visc, stencil, windex, cindex, findex, code256, code128, face1, face2,
    eta, main, qmain, ypack, qpack, cpack, zpack, rx, ry, rc, rqx, rqy, rz,
    before, coarse, zpack2, xsend, ysend, csend, rx2, ry2, rc2, rz2,
    tables, w, w_coarse, w_fine, wide, wide_p, ring_x, resid, blank,
    in_sem, send_sem, recv_sem,
):
    nx, ny, nz = (lax.axis_size(name) for name in ("gx", "gy", "gz"))
    ix, iy, iz = (lax.axis_index(name) for name in ("gx", "gy", "gz"))
    ends = {
        ("x", -1): ix > 0, ("x", 1): ix < nx - 1,
        ("y", -1): iy > 0, ("y", 1): iy < ny - 1,
        ("z", -1): iz > 0, ("z", 1): iz < nz - 1,
    }

    def present(dx, dy, dz):
        found = None
        for axis, step in (("x", dx), ("y", dy), ("z", dz)):
            if step:
                one = ends[axis, step]
                found = one if found is None else jnp.logical_and(found, one)
        return found

    def device(dx, dy, dz):
        return (ix + dx, iy + dy, iz + dz)

    def load(n, pairs):
        for source, target in pairs:
            pltpu.make_async_copy(source, target, in_sem.at[n]).start()

    def tiles(count):
        return blank.at[pl.ds(0, count)]

    def loaded(n, count):
        pltpu.make_async_copy(tiles(count), tiles(count), in_sem.at[n]).wait()

    visc_load = pltpu.make_async_copy(visc_hbm, visc, in_sem.at[0])
    visc_load.start()
    load(1, [(ids_hbm, ids), (rhs_hbm, rhs), (press_hbm, press)])
    stencil_load = pltpu.make_async_copy(stencil_hbm, stencil, in_sem.at[2])
    stencil_load.start()
    windex_load = pltpu.make_async_copy(windex_hbm, windex, in_sem.at[3])
    windex_load.start()
    rest = [
        (code256_hbm, code256), (code128_hbm, code128), (cindex_hbm, cindex), (findex_hbm, findex),
        (face1_hbm, face1), (face2_hbm, face2),
    ]
    load(4, rest)

    partners = AHEAD + [(dx, dy, 0) for dx, dy in SIDES]
    barrier = pltpu.get_barrier_semaphore()
    expected = 0
    for where in partners:
        there = present(*where)
        expected = expected + there.astype(jnp.int32)

        @pl.when(there)
        def _():
            pl.semaphore_signal(barrier, inc=1, device_id=device(*where), device_id_type=MESH)

    def send(group, source, target, where):
        copy = pltpu.make_async_remote_copy(
            src_ref=source,
            dst_ref=target,
            send_sem=send_sem.at[0],
            recv_sem=recv_sem.at[group],
            device_id=device(*where),
            device_id_type=MESH,
        )
        pl.when(present(*where))(copy.start)

    count_x, count_y, count_z = (
        ends[axis, -1].astype(jnp.int32) + ends[axis, 1].astype(jnp.int32) for axis in "xyz"
    )

    def wait_group(semaphore, choices):
        for there, count in choices:

            @pl.when(there)
            def _():
                pltpu.make_async_copy(tiles(count), tiles(count), semaphore).wait()

    def plane_choices(corner, along_x, along_y):
        return [
            (
                jnp.logical_and(count_x == nx, count_y == ny),
                corner * nx * ny + along_x * nx + along_y * ny,
            )
            for nx in (1, 2)
            for ny in (1, 2)
        ]

    def ahead_choices():
        return [
            (
                jnp.logical_and(jnp.logical_and(count_x == nx, count_y == ny), count_z == nz),
                (nx + 1) * (ny + 1) * nz,
            )
            for nx in (1, 2)
            for ny in (1, 2)
            for nz in (1, 2)
        ]

    def receive(group, choices):
        wait_group(recv_sem.at[group], choices)

    bad = NEVER
    for bit, end in (
        (XLO, ("x", -1)), (XHI, ("x", 1)), (YLO, ("y", -1)), (YHI, ("y", 1)), (ZLO, ("z", -1)), (ZHI, ("z", 1)),
    ):
        bad = bad + bit * (1 - ends[end].astype(jnp.int32))

    lane8 = lax.broadcasted_iota(jnp.int32, (8, 128), 1)
    row8 = lax.broadcasted_iota(jnp.int32, (8, 128), 0)
    low_rows = row8 < 4
    odd_rows = (row8 & 1) == 1

    def inside(code):
        return (code & bad) == 0

    def roll(value, shift):
        return pltpu.roll(value, shift % 128, 1) if shift % 128 else value

    visc_load.wait()
    loaded(1, 20)
    for p in range(4):
        layer = ids[p]
        value = jnp.zeros((8, 128), F32)
        for k in range(8):
            value = value + jnp.where(layer == k, visc[k], 0.0)
        eta[p] = value
        inverse = 1.0 / value
        for j in range(3):
            main[p, j] = rhs[j, p] * inverse
        qmain[p] = press[p] * value

    for s in range(2):
        for p in range(4):
            for j in range(3):
                ypack[s, j, 2 * p : 2 * p + 2, :] = main[p, j, 6 * s : 6 * s + 2, :]
            qpack[s, 2 * p : 2 * p + 2, :] = qmain[p, 6 * s : 6 * s + 2, :]
    for s in range(2):
        for v, (one, two) in enumerate(((ypack[s, 0], ypack[s, 1]), (ypack[s, 2], qpack[s]))):
            two = pltpu.roll(two, 4, 0)
            cpack[0, s, v] = jnp.where(low_rows, one, two)
            cpack[1, s, v] = jnp.where(low_rows, two, one)
    items = []
    for p in range(4):
        items += [main[p, j] for j in range(3)] + [qmain[p]]
    for s in range(2):
        items += [ypack[s, j] for j in range(3)] + [qpack[s]]
    total = jnp.zeros((8, 128), F32)
    for k, value in enumerate(items):
        total = jnp.where(((lane8 + (130 - 4 * k)) & 127) < 4, roll(value, 4 * k), total)
    zpack[...] = total

    pl.semaphore_wait(barrier, expected)

    def send_ahead(group, source, slots):
        for dx, dy, dz in AHEAD:
            send(group, source, slots.at[0 if dz > 0 else 1, 1 - dx, 1 - dy], (dx, dy, dz))

    send_ahead(0, zpack, rz)
    for dx in (-1, 1):
        for dy in (-1, 1):
            send(
                1,
                cpack.at[0 if dx < 0 else 1, 0 if dy < 0 else 1],
                rc.at[0 if dx > 0 else 1, 0 if dy > 0 else 1],
                (dx, dy, 0),
            )
        planes = pl.ds(0 if dx < 0 else 2, 2)
        send(1, main.at[planes], rx.at[0 if dx > 0 else 1], (dx, 0, 0))
    for dy in (-1, 1):
        send(1, ypack.at[0 if dy < 0 else 1], ry.at[0 if dy > 0 else 1], (0, dy, 0))
    for dx in (-1, 1):
        planes = pl.ds(0 if dx < 0 else 2, 2)
        send(2, qmain.at[planes], rqx.at[0 if dx > 0 else 1], (dx, 0, 0))
    for dy in (-1, 1):
        send(2, qpack.at[0 if dy < 0 else 1], rqy.at[0 if dy > 0 else 1], (0, dy, 0))

    stencil_load.wait()
    kc = (stencil[0, 0, 13] + stencil[1, 1, 13] + stencil[2, 2, 13]) / 3.0
    for c in range(3):
        rows = []
        for i in range(3):
            base = jnp.zeros((8, 128), F32)
            for a in range(3):
                for b in range(3):
                    for j in range(3):
                        at = 3 * (3 * a + b) + j
                        base = jnp.where(lane8 == at, stencil[i, j, 9 * a + 3 * b + c], base)
            low = lane8 < 27
            pair_a = base + jnp.where(low, roll(base, -9), 0.0)
            pair_b = base + jnp.where(low, roll(base, -3), 0.0)
            pair_ab = pair_a + jnp.where(low, roll(pair_a, -3), 0.0)
            full = base + roll(pair_a, 32) + roll(pair_b, 64) + roll(pair_ab, 96)
            rows.append(jnp.where(lane8 == ONE, 1.0, full))
        for combo, (one, two) in enumerate(((0, 1), (2, 0), (1, 2))):
            tables[3 * c + combo, 0:8, :] = rows[one]
            tables[3 * c + combo, 8:16, :] = rows[two]

    lane16 = lax.broadcasted_iota(jnp.int32, (16, 128), 1)

    def build(index, section, target, tiles, width, unroll):
        at, count, copies, first = section

        def chunk(t):
            combo = lax.rem(t, 3)
            start = pl.multiple_of(t * 16, 16)
            for tile in range(tiles):
                lanes = slice(128 * tile, 128 * tile + 128)
                picked = index[pl.ds(at + start, 16), lanes]
                for c in range(copies):
                    value = jnp.take_along_axis(
                        tables[3 * c + combo], picked, axis=1, mode="promise_in_bounds"
                    )
                    rows = pl.ds(first + c * count + start, 16)
                    if width is None:
                        high, low = split(value)
                        target[rows, lanes] = high
                        target[rows, 256 + 128 * tile : 384 + 128 * tile] = low
                        target[rows, 512 + 128 * tile : 640 + 128 * tile] = high
                    else:
                        low = value - value.astype(BF16).astype(F32)
                        lane = lane16 + 128 * tile
                        value = jnp.where((lane >= width) & (lane < 2 * width), low, value)
                        target[rows, lanes] = value.astype(BF16)

        def step(t, carry):
            for n in range(unroll):
                chunk(t * unroll + n)
            return carry

        lax.fori_loop(0, count // (16 * unroll), step, 0)

    windex_load.wait()
    for name in ("a", "b", "local"):
        build(windex, WIDE_SECTIONS[name], w, 2, None, 3)
    loaded(4, REST_TILES)
    for name in ("coarse", "keep"):
        build(cindex, COARSE_SECTIONS[name], w_coarse, 4, 144, 1)
    for name in ("fine", "spread"):
        build(findex, FINE_SECTIONS[name], w_fine, 2, 80, 3)

    def along_z(slots, select, ox, oy):
        return jnp.where(select, slots[1, ox + 1, oy + 1], slots[0, ox + 1, oy + 1])

    from_high_1 = (lane8 & 3) < 2
    from_high_2 = ((lane8 < 32) & ((lane8 & 1) == 0)) | ((lane8 >= 64) & (lane8 < 127))

    def wide_blocks(comp, tile):
        comps = 4

        def edge(ox, oy, k):
            return roll(along_z(rz, from_high_1, ox, oy), -4 * k)

        blocks = {}
        for p in range(4):
            own = main[p, comp] if comp < 3 else qmain[p]
            blocks[p] = edge(0, 0, p * comps + comp) if tile else own
        for n in range(2):
            for side, ox, first in ((0, -1, -2), (1, 1, 4)):
                near = rx[side, n, comp] if comp < 3 else rqx[side, n]
                plane = n if ox > 0 else n + 2
                blocks[first + n] = edge(ox, 0, plane * comps + comp) if tile else near
        for s, oy in enumerate((-1, 1)):
            k = 4 * comps + (1 - s) * comps + comp
            if tile:
                blocks["y", s] = edge(0, oy, k)
                blocks["c", s] = jnp.where(low_rows, edge(1, oy, k), edge(-1, oy, k))
                continue
            blocks["y", s] = ry[s, comp] if comp < 3 else rqy[s]
            below, above = rc[0, s, comp // 2], rc[1, s, comp // 2]
            if comp % 2 == 0:
                blocks["c", s] = jnp.where(low_rows, above, below)
            else:
                blocks["c", s] = pltpu.roll(jnp.where(low_rows, below, above), 4, 0)
        return blocks

    def store_wide(target, comps, code_at, tile):
        lanes = slice(128 * tile, 128 * tile + 128)
        for slot, comp in enumerate(comps):
            blocks = wide_blocks(comp, tile)
            order = [-2, -1, 0, 1, 2, ("y", 0), ("y", 1), ("c", 0), ("c", 1), 3, 4, 5]
            for n, key in enumerate(order):
                at = 8 * (n * len(comps) + slot)
                code = code256[code_at + at : code_at + at + 8, lanes]
                target[at : at + 8, lanes] = jnp.where(inside(code), blocks[key], 0.0)

    def ring_of(source, comps):
        def block(n):
            return source[8 * comps * n : 8 * comps * (n + 1), :]

        row = lax.broadcasted_iota(jnp.int32, (8 * comps, source.shape[1]), 0)
        odd, low = (row & 1) == 1, (row & 7) < 4
        level = jnp.where(odd, block(5), block(6))
        corner = jnp.where(odd, block(7), block(8))
        return jnp.concatenate(
            [
                block(1), block(2), block(3), jnp.where(low, level, corner),
                block(4), block(9), block(10), jnp.where(low, corner, level),
            ],
            axis=0,
        )

    def local_of(ring, comps):
        return jnp.concatenate([ring[8 * comps : 24 * comps], ring[32 * comps : 48 * comps]], axis=0)

    def ring_products(tile):
        lanes = slice(128 * tile, 128 * tile + 128)
        parts = []
        for name, start in (("a", 0), ("b", 32)):
            high, low = split(wide[start : start + 256, lanes])
            right = jnp.concatenate([high, high, low], axis=0)
            base = WIDE_SECTIONS[name][3]
            parts.append(jnp.dot(w[base : base + 288, :], right, preferred_element_type=F32))
        return tuple(
            jnp.concatenate([part[96 * c : 96 * c + 96] for part in parts], axis=0) for c in range(3)
        )

    def operator_local(value):
        high, low = split(value)
        gap = jnp.zeros((64, 256), BF16)
        right = jnp.concatenate([high, gap, high, gap, low, gap], axis=0)
        base = WIDE_SECTIONS["local"][3]
        product = jnp.dot(w[base : base + 288, :], right, preferred_element_type=F32)
        return z_shift_sum(product, 96)

    ikc = (jnp.full((8, 256), 1.0, F32) / kc)[0:1, :]
    gain_u = ((1.0 + MOM + WEIGHT * THETA) / THETA) * ikc
    gain_s = (-WEIGHT / THETA) * ikc * ikc

    ring_code = len(CODE_WIDE)
    wide_p_code = ring_code + len(CODE_RING)
    ring_p_code = wide_p_code + len(CODE_WIDE_P)

    def ring_inside():
        return inside(code256[ring_code : ring_code + 192, :])

    receive(1, plane_choices(2, 6, 3))
    store_wide(wide, (0, 1, 2), 0, 0)

    lane192 = lax.broadcasted_iota(jnp.int32, (192, 128), 1)
    at_first, at_last = lane192 == 0, lane192 == 127
    below, level, above = ring_products(0)
    below, above = pltpu.roll(below, 1, 1), pltpu.roll(above, 127, 1)
    gu, gs = gain_u[:, 0:128], gain_s[:, 0:128]
    level = level + jnp.where(at_first, 0.0, below) + jnp.where(at_last, 0.0, above)
    ring_x[:, 0:128] = gu * ring_of(wide[:, 0:128], 3) + gs * level
    ring_x[:, 128:256] = gs * (jnp.where(at_first, below, 0.0) + jnp.where(at_last, above, 0.0))

    receive(0, ahead_choices())
    store_wide(wide, (0, 1, 2), 0, 1)
    below, level, above = ring_products(1)
    below, above = pltpu.roll(below, 1, 1), pltpu.roll(above, 127, 1)
    one = ring_x[:, 0:128] + gs * jnp.where(at_first, below, jnp.where(at_last, above, 0.0))
    two = level + jnp.where(at_last, below, jnp.where(at_first, above, 0.0))
    two = ring_x[:, 128:256] + gu * ring_of(wide[:, 128:256], 3) + gs * two
    x2 = jnp.where(ring_inside(), jnp.concatenate([one, two], axis=1), 0.0)
    ring_x[...] = x2

    applied = operator_local(x2)
    even = (lane8 * 2) & 127

    def row_sum(source, n):
        return source[n, pl.ds(0, 8, 2), :] + source[n, pl.ds(1, 8, 2), :]

    def pair_sum(value, index):
        one = jnp.take_along_axis(value, index, axis=1, mode="promise_in_bounds")
        two = jnp.take_along_axis(value, index + 1, axis=1, mode="promise_in_bounds")
        return one + two

    def local_row(p):
        return 8 * (3 + 3 * p if p < 2 else 6 + 3 * p)

    for big in range(2):
        resid[3, 8 * big : 8 * big + 8, :] = eta[2 * big] + eta[2 * big + 1]
        for j in range(3):
            total = jnp.zeros((8, 128), F32)
            for p in (2 * big, 2 * big + 1):
                n = 8 * (3 * p + j)
                left = main[p, j] - applied[n : n + 8, 0:128]
                resid[4 + j, 8 * p : 8 * p + 8, :] = left
                at = local_row(p) + 8 * j
                value = ring_x[at : at + 8, 0:128] + ((1.0 / THETA) * ikc[:, 0:128]) * left
                before[p, j] = value
                total = total + eta[p] * left
            resid[j, 8 * big : 8 * big + 8, :] = total
    weights = row_sum(resid, 3)
    four_over = 4.0 / pair_sum(weights, even)
    total = jnp.zeros((8, 128), F32)
    for j in range(3):
        value = row_sum(resid, j)
        coarse[j] = pair_sum(value, even) * four_over
        first = (lane8 >= 98 + 4 * j) & (lane8 < 100 + 4 * j)
        last = (lane8 >= 32 + 4 * j) & (lane8 < 34 + 4 * j)
        here = jnp.where(first, 2 * (lane8 - (98 + 4 * j)), jnp.where(last, 2 * (lane8 + 30 - 4 * j), 0))
        packed = pair_sum(value, here) * (4.0 / pair_sum(weights, here))
        total = jnp.where(first | last, packed, total)
        for p in range(4):
            ysend[2 + j, 2 * p : 2 * p + 1, :] = before[p, j, 0:1, :]
            ysend[2 + j, 2 * p + 1 : 2 * p + 2, :] = before[p, j, 7:8, :]
            if p in (0, 3):
                n = 0 if p == 0 else 1
                xsend[n, 2 + j] = before[p, j]
                csend[n, 2, 2 * j : 2 * j + 1, :] = before[p, j, 0:1, :]
                csend[n, 2, 2 * j + 1 : 2 * j + 2, :] = before[p, j, 7:8, :]
    items = [before[p, j] for p in range(4) for j in range(3)] + [ysend[2 + j] for j in range(3)]
    for k, value in enumerate(items):
        total = jnp.where(((lane8 + (129 - 2 * k)) & 127) < 2, roll(value, 2 * k), total)
    zpack2[...] = total
    for n, value in enumerate((jnp.where(lane8 < 64, coarse[0], roll(coarse[1], 64)), coarse[2])):
        ysend[n] = value
        for m in range(2):
            xsend[m, n] = value
            csend[m, n] = value
    send_ahead(3, zpack2, rz2)
    for dx in (-1, 1):
        for dy in (-1, 1):
            send(
                4,
                csend.at[0 if dx < 0 else 1],
                rc2.at[0 if dx > 0 else 1, 0 if dy > 0 else 1],
                (dx, dy, 0),
            )
        send(4, xsend.at[0 if dx < 0 else 1], rx2.at[0 if dx > 0 else 1], (dx, 0, 0))
    for dy in (-1, 1):
        send(4, ysend, ry2.at[0 if dy > 0 else 1], (0, dy, 0))

    receive(2, plane_choices(0, 2, 1))
    store_wide(wide_p, (3,), wide_p_code, 0)
    store_wide(wide_p, (3,), wide_p_code, 1)
    q_ring = ring_of(wide_p, 1)
    high, low = split(wide_p[...])
    gap = jnp.zeros((32, 256), BF16)
    near = jnp.dot(face1[...], jnp.concatenate([high, gap, low, gap], axis=0), preferred_element_type=F32)
    near = near + pltpu.roll(q_ring, 1, 1) + pltpu.roll(q_ring, 255, 1)
    p_ring = (4.0 / 27.0) * q_ring + (1.0 / 81.0) * near
    p_ring = jnp.where(inside(code256[ring_p_code : ring_p_code + 64, :]), p_ring, 0.0)
    high, low = split(p_ring)
    near = jnp.dot(face2[...], jnp.concatenate([high, low], axis=0), preferred_element_type=F32)
    p_in, q_in = local_of(p_ring, 1), local_of(q_ring, 1)
    near = near + pltpu.roll(p_in, 1, 1) + pltpu.roll(p_in, 255, 1)
    p_out = (1.0 / 3.0) * p_in + (1.0 / 9.0) * q_in + (1.0 / 9.0) * near
    for p in range(4):
        pout_ref[p] = p_out[8 * p : 8 * p + 8, 0:128]
    receive(4, plane_choices(3, 5, 5))
    receive(3, ahead_choices())

    def from_side(ox, oy, n):
        if ox and oy:
            return rc2[0 if ox < 0 else 1, 0 if oy < 0 else 1, n]
        return rx2[0 if ox < 0 else 1, n] if ox else ry2[0 if oy < 0 else 1, n]

    def coarse_block(ox, oy, j):
        if (ox, oy) == (0, 0):
            inner = coarse[j]
        else:
            inner = from_side(ox, oy, j // 2)
            inner = roll(inner, 64) if j == 1 else inner
        return jnp.where(lane8 < 64, inner, roll(along_z(rz2, from_high_2, ox, oy), -(34 + 4 * j)))

    blocks = []
    near_high = (row8 & 3) < 2
    for ox in (-1, 0, 1):
        blocks += [coarse_block(ox, 0, j) for j in range(3)]
        blocks += [jnp.where(near_high, coarse_block(ox, 1, j), coarse_block(ox, -1, j)) for j in range(3)]
    value = jnp.where(inside(code128[0:144, :]), jnp.concatenate(blocks, axis=0), 0.0)
    high, low = split(value)
    right = jnp.concatenate([high, high, low, jnp.zeros((80, 128), BF16)], axis=0)
    product = jnp.dot(w_coarse[...], right, preferred_element_type=F32)
    e = gain_u[:, 0:128] * product[240:320] + gain_s[:, 0:128] * z_shift_sum(product, 80)
    e = jnp.where(inside(code128[144:224, :]), e, 0.0)
    lane80 = lax.broadcasted_iota(jnp.int32, (80, 128), 1)
    near_lane = lane80 >> 1
    far_lane = jnp.where(lane80 < 2, 64, jnp.where(lane80 >= 126, 127, 100))
    e = jnp.concatenate(
        [
            jnp.take_along_axis(e, near_lane, axis=1, mode="promise_in_bounds"),
            jnp.take_along_axis(e, far_lane, axis=1, mode="promise_in_bounds"),
        ],
        axis=1,
    )
    high, low = split(e)
    right = jnp.concatenate([high, high, low, jnp.zeros((16, 256), BF16)], axis=0)
    product = jnp.dot(w_fine[...], right, preferred_element_type=F32)

    def ring_block(ox, oy, inner, k):
        return jnp.concatenate([inner, roll(along_z(rz2, from_high_2, ox, oy), -2 * k)], axis=1)

    def layer(ox, j):
        if ox == 0:
            inner = jnp.where(odd_rows, from_side(0, -1, 2 + j), from_side(0, 1, 2 + j))
        else:
            inner = jnp.where(odd_rows, from_side(ox, -1, 2), from_side(ox, 1, 2))
            shift = (-2 * j if ox > 0 else 6 - 2 * j) % 8
            inner = pltpu.roll(inner, shift, 0) if shift else inner
        outer = jnp.where(odd_rows, along_z(rz2, from_high_2, ox, -1), along_z(rz2, from_high_2, ox, 1))
        return jnp.concatenate([inner, roll(outer, -2 * (12 + j))], axis=1)

    low_wide = lax.broadcasted_iota(jnp.int32, (8, 256), 0) < 4
    halves = [[], []]
    for half in range(2):
        for x in ((-1, 0, 1), (2, 3, 4))[half]:
            for j in range(3):
                if x == -1:
                    halves[half].append(ring_block(-1, 0, rx2[0, 2 + j], 9 + j))
                elif x == 4:
                    halves[half].append(ring_block(1, 0, rx2[1, 2 + j], j))
                else:
                    halves[half].append(ring_block(0, 0, before[x, j], 3 * x + j))
    for j in range(3):
        level = layer(0, j)
        halves[0].append(jnp.where(low_wide, level, layer(-1, j)))
        halves[1].append(jnp.where(low_wide, layer(1, j), level))
    start = jnp.concatenate(halves[0] + halves[1], axis=0)

    down = ((1.0 / THETA) * ikc) * z_shift_sum(product, 192)
    x = jnp.where(ring_inside(), start + product[576:768] - down, 0.0)
    applied = operator_local(x)
    x_in, down_in = local_of(x, 3), local_of(down, 3)
    for p in range(4):
        for j in range(3):
            n = 8 * (3 * p + j)
            step = ((1.0 / THETA) * ikc[:, 0:128]) * resid[4 + j, 8 * p : 8 * p + 8, :] - down_in[n : n + 8, 0:128]
            out_ref[j, p] = (
                x_in[n : n + 8, 0:128]
                + MOM * step
                + (WEIGHT * ikc[:, 0:128]) * (main[p, j] - applied[n : n + 8, 0:128])
            )

    totals = [
        (there, 2 * (nx + 1) * (ny + 1) * nz + 5 * nx * ny + 13 * nx + 9 * ny)
        for (there, _), (nx, ny, nz) in zip(
            ahead_choices(), [(nx, ny, nz) for nx in (1, 2) for ny in (1, 2) for nz in (1, 2)]
        )
    ]
    wait_group(send_sem.at[0], totals)


GROUPS = 5
REST_TILES = (
    CODE_256.size + CODE_128.size + COARSE_INDEX.size + FINE_INDEX.size + (FACE_1.size + FACE_2.size) // 2
) // 1024


def scratch():
    vmem = pltpu.VMEM
    return [
        vmem((3, 4, 8, 128), F32),
        vmem((4, 8, 128), F32),
        vmem((4, 8, 128), jnp.int32),
        pltpu.SMEM((8,), F32),
        pltpu.SMEM((3, 3, 27), F32),
        vmem(WIDE_INDEX.shape, jnp.int32),
        vmem(COARSE_INDEX.shape, jnp.int32),
        vmem(FINE_INDEX.shape, jnp.int32),
        vmem(CODE_256.shape, jnp.int32),
        vmem(CODE_128.shape, jnp.int32),
        vmem(FACE_1.shape, BF16),
        vmem(FACE_2.shape, BF16),
        vmem((4, 8, 128), F32),
        vmem((4, 3, 8, 128), F32),
        vmem((4, 8, 128), F32),
        vmem((2, 3, 8, 128), F32),
        vmem((2, 8, 128), F32),
        vmem((2, 2, 2, 8, 128), F32),
        vmem((8, 128), F32),
        vmem((2, 2, 3, 8, 128), F32),
        vmem((2, 3, 8, 128), F32),
        vmem((2, 2, 2, 8, 128), F32),
        vmem((2, 2, 8, 128), F32),
        vmem((2, 8, 128), F32),
        vmem((2, 3, 3, 8, 128), F32),
        vmem((4, 3, 8, 128), F32),
        vmem((3, 8, 128), F32),
        vmem((8, 128), F32),
        vmem((2, 5, 8, 128), F32),
        vmem((5, 8, 128), F32),
        vmem((2, 3, 8, 128), F32),
        vmem((2, 5, 8, 128), F32),
        vmem((2, 5, 8, 128), F32),
        vmem((2, 2, 3, 8, 128), F32),
        vmem((2, 3, 3, 8, 128), F32),
        vmem((9, 16, 128), F32),
        vmem((WIDE_ROWS, 768), BF16),
        vmem((COARSE_ROWS, 512), BF16),
        vmem((FINE_ROWS, 256), BF16),
        vmem((288, 256), F32),
        vmem((96, 256), F32),
        vmem((192, 256), F32),
        vmem((7, 32, 128), F32),
        vmem((REST_TILES, 8, 128), F32),
        pltpu.SemaphoreType.DMA((5,)),
        pltpu.SemaphoreType.DMA((1,)),
        pltpu.SemaphoreType.DMA((GROUPS,)),
    ]


def store_results(velocity, pressure, velocity_out, pressure_out, sem):
    one = pltpu.make_async_copy(velocity, velocity_out, sem.at[0])
    two = pltpu.make_async_copy(pressure, pressure_out, sem.at[1])
    one.start()
    two.start()
    one.wait()
    two.wait()


def on_device(rhs_velocity, rhs_pressure, layer_ids, visc_table, stencil):
    anywhere = pl.BlockSpec(memory_space=pltpu.HBM)
    inside = pl.BlockSpec(memory_space=pltpu.VMEM)
    results = pl.pallas_call(
        body,
        name="stokes",
        out_shape=(
            pltpu.VMEM(rhs_velocity.shape, F32),
            pltpu.VMEM(rhs_pressure.shape, F32),
        ),
        in_specs=[anywhere] * 12,
        out_specs=(inside, inside),
        scratch_shapes=scratch(),
        compiler_params=pltpu.CompilerParams(
            collective_id=0, has_side_effects=True, vmem_limit_bytes=60 * 1024 * 1024
        ),
    )(
        *(
            pltpu.with_memory_space_constraint(value, pltpu.HBM)
            for value in (
                rhs_velocity,
                rhs_pressure,
                layer_ids,
                visc_table,
                stencil.transpose(1, 2, 0),
                jnp.asarray(WIDE_INDEX),
                jnp.asarray(COARSE_INDEX),
                jnp.asarray(FINE_INDEX),
                jnp.asarray(CODE_256),
                jnp.asarray(CODE_128),
                jnp.asarray(FACE_1, BF16),
                jnp.asarray(FACE_2, BF16),
            )
        )
    )
    return pl.pallas_call(
        store_results,
        name="store",
        out_shape=(
            jax.ShapeDtypeStruct(rhs_velocity.shape, F32),
            jax.ShapeDtypeStruct(rhs_pressure.shape, F32),
        ),
        in_specs=[inside] * 2,
        out_specs=(anywhere,) * 2,
        scratch_shapes=[pltpu.SemaphoreType.DMA((2,))],
    )(*(pltpu.with_memory_space_constraint(value, pltpu.VMEM) for value in results))


def solution(mesh):
    placed = (P(None, "gx", "gy", "gz"), P("gx", "gy", "gz"), P("gx", "gy", "gz"), P(), P())
    return jax.shard_map(
        on_device,
        mesh=mesh,
        in_specs=placed,
        out_specs=(P(None, "gx", "gy", "gz"), P("gx", "gy", "gz")),
        check_vma=False,
    )
```

```python
import functools

import numpy as np
import jax
import jax.numpy as jnp
from jax import lax
from jax.experimental import pallas as pl
from jax.experimental.pallas import tpu as pltpu
from jax.sharding import PartitionSpec as P

F32 = jnp.float32
BF16 = jnp.bfloat16
MESH = pl.DeviceIdType.MESH

THETA = (1.8 + 0.2) / 2.0
DELTA = (1.8 - 0.2) / 2.0
SIGMA = THETA / DELTA
RHO0 = 1.0 / SIGMA
RHO1 = 1.0 / (2.0 * SIGMA - RHO0)
MOM = RHO1 * RHO0
WEIGHT = 2.0 * RHO1 / DELTA

XLO, XHI, YLO, YHI, ZLO, ZHI, NEVER = 1, 2, 4, 8, 16, 32, 64

ONE, ZERO = 28, 31

CORNER_X = (4, 5, -2, -1)
SIDES = [(dx, dy) for dx in (-1, 0, 1) for dy in (-1, 0, 1) if (dx, dy) != (0, 0)]
AHEAD = [(dx, dy, dz) for dx in (-1, 1, 0) for dy in (0, -1, 1) for dz in (-1, 1)]


def plane_block(x, j):
    return [(x, r, j) for r in range(8)]


def y_block(s, j):
    return [(r // 2, (-2 if s == 0 else 8) + r % 2, j) for r in range(8)]


def c_block(s, j):
    return [(CORNER_X[r // 2], (-2 if s == 0 else 8) + r % 2, j) for r in range(8)]


def edge_block(i, half):
    rows = []
    for r in range(8):
        y = -1 if r % 2 else 8
        if half == 0:
            x = r // 2 if r < 4 else (-1 if r >= 6 else None)
        else:
            x = r // 2 if r >= 4 else (4 if r < 2 else None)
        rows.append(None if x is None else (x, y, i))
    return rows


def rows_wide(comps):
    rows = []
    for x in (-2, -1, 0, 1, 2):
        for j in range(comps):
            rows += plane_block(x, j)
    for block in (y_block, c_block):
        for s in range(2):
            for j in range(comps):
                rows += block(s, j)
    for x in (3, 4, 5):
        for j in range(comps):
            rows += plane_block(x, j)
    return rows


def rows_half(half, comps):
    rows = []
    for x in ((-1, 0, 1), (2, 3, 4))[half]:
        for i in range(comps):
            rows += plane_block(x, i)
    for i in range(comps):
        rows += edge_block(i, half)
    return rows


def rows_ring(comps):
    return rows_half(0, comps) + rows_half(1, comps)


def rows_coarse_in():
    rows = []
    for dx in (-1, 0, 1):
        for j in range(3):
            rows += [(2 * dx + r // 4, r % 4, j) for r in range(8)]
        for j in range(3):
            rows += [(2 * dx + r // 4, r % 4 + (4 if r % 4 < 2 else -4), j) for r in range(8)]
    return rows


def rows_coarse_out():
    rows = []
    for q in range(3):
        for i in range(3):
            for r in range(8):
                n = 8 * q + r
                rows.append((n // 6 - 1, n % 6 - 1, i))
    return rows + [None] * 8


def index_stencil(outs, ins):
    table = np.full((len(outs), len(ins)), ZERO, np.int32)
    for m, out in enumerate(outs):
        if out is None:
            continue
        for k, source in enumerate(ins):
            if source is None:
                continue
            a, b = source[0] - out[0] + 1, source[1] - out[1] + 1
            if 0 <= a <= 2 and 0 <= b <= 2:
                table[m, k] = 3 * (3 * a + b) + source[2]
    return table


def index_same(outs, ins, scale):
    table = np.full((len(outs), len(ins)), ZERO, np.int32)
    for m, out in enumerate(outs):
        if out is None:
            continue
        for k, source in enumerate(ins):
            if source is not None and (out[0] // scale, out[1] // scale, out[2]) == source:
                table[m, k] = ONE
    return table


def index_refined(outs, ins):
    table = np.full((len(outs), len(ins)), ZERO, np.int32)
    for m, out in enumerate(outs):
        if out is None:
            continue
        for k, source in enumerate(ins):
            if source is None:
                continue
            a = [v for v in range(3) if (out[0] + v - 1) // 2 == source[0]]
            b = [v for v in range(3) if (out[1] + v - 1) // 2 == source[1]]
            if a and b:
                segment = (len(a) - 1) + 2 * (len(b) - 1)
                table[m, k] = 32 * segment + 3 * (3 * a[0] + b[0]) + source[2]
    return table


def codes(rows, x_end, y_end, lanes, z_bits):
    table = np.full((len(rows), lanes), NEVER, np.int32)
    z_row = np.full((lanes,), NEVER, np.int32)
    for lane, bits in z_bits:
        z_row[lane] = bits
    for m, row in enumerate(rows):
        if row is None:
            continue
        bits = (XLO if row[0] < 0 else 0) | (XHI if row[0] >= x_end else 0)
        bits |= (YLO if row[1] < 0 else 0) | (YHI if row[1] >= y_end else 0)
        table[m] = bits | z_row
    return table


def face_matrix(outs, ins):
    table = np.zeros((len(outs), len(ins)), np.float32)
    for m, out in enumerate(outs):
        if out is None:
            continue
        for k, source in enumerate(ins):
            if source is not None and abs(source[0] - out[0]) + abs(source[1] - out[1]) == 1:
                table[m, k] = 1.0
    return table


FINE_LANES = [(z, 0) for z in range(128)]
WIDE_Z = FINE_LANES + [(128, ZHI), (129, ZHI), (254, ZLO), (255, ZLO)]
RING_Z = FINE_LANES + [(128, ZHI), (255, ZLO)]
COARSE_Z = [(z, 0) for z in range(64)] + [(64, ZHI), (65, ZHI), (126, ZLO), (127, ZLO)]
COARSE_RING_Z = [(z, 0) for z in range(64)] + [(64, ZHI), (127, ZLO)]

WIDE = rows_wide(3)
RING = rows_ring(3)
LOCAL = [row for x in range(4) for i in range(3) for row in plane_block(x, i)]
HALF_A = rows_half(0, 3)
HALF_B = rows_half(1, 3)
COARSE_IN = rows_coarse_in()
COARSE_OUT = rows_coarse_out()

def triple(table, width):
    wide = np.full((len(table), width), ZERO, np.int32)
    count = table.shape[1]
    for n in range(3):
        wide[:, n * count : (n + 1) * count] = table
    return wide


def single(table):
    return np.concatenate([table, np.full((len(table), 256 - table.shape[1]), ZERO, np.int32)], axis=1)


def place(sections):
    places, at, row = {}, 0, 0
    for name, table, copies in sections:
        places[name] = (at, len(table), copies, row)
        at += len(table)
        row += len(table) * copies
    return places, np.concatenate([section[1] for section in sections], axis=0), row


WIDE_SECTIONS, WIDE_INDEX, WIDE_ROWS = place(
    [
        ("a", single(index_stencil(HALF_A, WIDE[0:256])), 3),
        ("b", single(index_stencil(HALF_B, WIDE[32:288])), 3),
        ("local", single(index_stencil(LOCAL, RING)), 3),
    ]
)
COARSE_SECTIONS, COARSE_INDEX, COARSE_ROWS = place(
    [
        ("coarse", triple(index_stencil(COARSE_OUT, COARSE_IN), 512), 3),
        ("keep", triple(index_same(COARSE_OUT, COARSE_IN, 1), 512), 1),
    ]
)
FINE_SECTIONS, FINE_INDEX, FINE_ROWS = place(
    [
        ("fine", triple(index_refined(RING, COARSE_OUT), 256), 3),
        ("spread", triple(index_same(RING, COARSE_OUT, 2), 256), 1),
    ]
)

CODE_WIDE = codes(WIDE, 4, 8, 256, WIDE_Z)
CODE_RING = codes(RING, 4, 8, 256, RING_Z)
CODE_COARSE = codes(COARSE_IN, 2, 4, 128, COARSE_Z)
CODE_COARSE_RING = codes(COARSE_OUT, 2, 4, 128, COARSE_RING_Z)
CODE_WIDE_P = codes(rows_wide(1), 4, 8, 256, WIDE_Z)
CODE_RING_P = codes(rows_ring(1), 4, 8, 256, RING_Z)
CODE_256 = np.concatenate([CODE_WIDE, CODE_RING, CODE_WIDE_P, CODE_RING_P], axis=0)
CODE_128 = np.concatenate([CODE_COARSE, CODE_COARSE_RING], axis=0)


def face_pair(outs, ins, width, total):
    single = face_matrix(outs, ins)
    table = np.zeros((len(outs), total), np.float32)
    table[:, : single.shape[1]] = single
    table[:, width : width + single.shape[1]] = single
    return table


FACE_1 = face_pair(rows_ring(1), rows_wide(1), 128, 256)
FACE_2 = face_pair([row for x in range(4) for row in plane_block(x, 0)], rows_ring(1), 64, 128)


def split(value):
    high = value.astype(BF16)
    low = (value - high.astype(F32)).astype(BF16)
    return high, low


def z_shift_sum(product, rows):
    lanes = product.shape[1]
    return (
        product[rows : 2 * rows]
        + pltpu.roll(product[0:rows], 1, 1)
        + pltpu.roll(product[2 * rows : 3 * rows], lanes - 1, 1)
    )


def body(
    rhs_hbm, press_hbm, ids_hbm, visc_hbm, stencil_hbm, windex_hbm, cindex_hbm, findex_hbm,
    code256_hbm, code128_hbm, face1_hbm, face2_hbm,
    out_ref, pout_ref,
    rhs, press, ids, visc, stencil, windex, cindex, findex, code256, code128, face1, face2,
    eta, main, qmain, ypack, qpack, cpack, zpack, rx, ry, rc, rqx, rqy, rz,
    before, coarse, zpack2, xsend, ysend, csend, rx2, ry2, rc2, rz2,
    tables, w, w_coarse, w_fine, wide, wide_p, ring_x, resid, blank,
    in_sem, send_sem, recv_sem,
):
    nx, ny, nz = (lax.axis_size(name) for name in ("gx", "gy", "gz"))
    ix, iy, iz = (lax.axis_index(name) for name in ("gx", "gy", "gz"))
    ends = {
        ("x", -1): ix > 0, ("x", 1): ix < nx - 1,
        ("y", -1): iy > 0, ("y", 1): iy < ny - 1,
        ("z", -1): iz > 0, ("z", 1): iz < nz - 1,
    }

    def present(dx, dy, dz):
        found = None
        for axis, step in (("x", dx), ("y", dy), ("z", dz)):
            if step:
                one = ends[axis, step]
                found = one if found is None else jnp.logical_and(found, one)
        return found

    def device(dx, dy, dz):
        return (ix + dx, iy + dy, iz + dz)

    def load(n, pairs):
        for source, target in pairs:
            pltpu.make_async_copy(source, target, in_sem.at[n]).start()

    def tiles(count):
        return blank.at[pl.ds(0, count)]

    def loaded(n, count):
        pltpu.make_async_copy(tiles(count), tiles(count), in_sem.at[n]).wait()

    visc_load = pltpu.make_async_copy(visc_hbm, visc, in_sem.at[0])
    visc_load.start()
    load(1, [(ids_hbm, ids), (rhs_hbm, rhs), (press_hbm, press)])
    stencil_load = pltpu.make_async_copy(stencil_hbm, stencil, in_sem.at[2])
    stencil_load.start()
    windex_load = pltpu.make_async_copy(windex_hbm, windex, in_sem.at[3])
    windex_load.start()
    rest = [
        (code256_hbm, code256), (code128_hbm, code128), (cindex_hbm, cindex), (findex_hbm, findex),
        (face1_hbm, face1), (face2_hbm, face2),
    ]
    load(4, rest)

    partners = AHEAD + [(dx, dy, 0) for dx, dy in SIDES]
    barrier = pltpu.get_barrier_semaphore()
    expected = 0
    for where in partners:
        there = present(*where)
        expected = expected + there.astype(jnp.int32)

        @pl.when(there)
        def _():
            pl.semaphore_signal(barrier, inc=1, device_id=device(*where), device_id_type=MESH)

    def send(group, source, target, where):
        copy = pltpu.make_async_remote_copy(
            src_ref=source,
            dst_ref=target,
            send_sem=send_sem.at[0],
            recv_sem=recv_sem.at[group],
            device_id=device(*where),
            device_id_type=MESH,
        )
        pl.when(present(*where))(copy.start)

    count_x, count_y, count_z = (
        ends[axis, -1].astype(jnp.int32) + ends[axis, 1].astype(jnp.int32) for axis in "xyz"
    )

    def wait_group(semaphore, choices):
        for there, count in choices:

            @pl.when(there)
            def _():
                pltpu.make_async_copy(tiles(count), tiles(count), semaphore).wait()

    def plane_choices(corner, along_x, along_y):
        return [
            (
                jnp.logical_and(count_x == nx, count_y == ny),
                corner * nx * ny + along_x * nx + along_y * ny,
            )
            for nx in (1, 2)
            for ny in (1, 2)
        ]

    def ahead_choices():
        return [
            (
                jnp.logical_and(jnp.logical_and(count_x == nx, count_y == ny), count_z == nz),
                (nx + 1) * (ny + 1) * nz,
            )
            for nx in (1, 2)
            for ny in (1, 2)
            for nz in (1, 2)
        ]

    def receive(group, choices):
        wait_group(recv_sem.at[group], choices)

    bad = NEVER
    for bit, end in (
        (XLO, ("x", -1)), (XHI, ("x", 1)), (YLO, ("y", -1)), (YHI, ("y", 1)), (ZLO, ("z", -1)), (ZHI, ("z", 1)),
    ):
        bad = bad + bit * (1 - ends[end].astype(jnp.int32))

    lane8 = lax.broadcasted_iota(jnp.int32, (8, 128), 1)
    row8 = lax.broadcasted_iota(jnp.int32, (8, 128), 0)
    low_rows = row8 < 4
    odd_rows = (row8 & 1) == 1

    def inside(code):
        return (code & bad) == 0

    def roll(value, shift):
        return pltpu.roll(value, shift % 128, 1) if shift % 128 else value

    visc_load.wait()
    loaded(1, 20)
    for p in range(4):
        layer = ids[p]
        value = jnp.zeros((8, 128), F32)
        for k in range(8):
            value = value + jnp.where(layer == k, visc[k], 0.0)
        eta[p] = value
        inverse = 1.0 / value
        for j in range(3):
            main[p, j] = rhs[j, p] * inverse
        qmain[p] = press[p] * value

    for s in range(2):
        for p in range(4):
            for j in range(3):
                ypack[s, j, 2 * p : 2 * p + 2, :] = main[p, j, 6 * s : 6 * s + 2, :]
            qpack[s, 2 * p : 2 * p + 2, :] = qmain[p, 6 * s : 6 * s + 2, :]
    for s in range(2):
        for v, (one, two) in enumerate(((ypack[s, 0], ypack[s, 1]), (ypack[s, 2], qpack[s]))):
            two = pltpu.roll(two, 4, 0)
            cpack[0, s, v] = jnp.where(low_rows, one, two)
            cpack[1, s, v] = jnp.where(low_rows, two, one)
    items = []
    for p in range(4):
        items += [main[p, j] for j in range(3)] + [qmain[p]]
    for s in range(2):
        items += [ypack[s, j] for j in range(3)] + [qpack[s]]
    total = jnp.zeros((8, 128), F32)
    for k, value in enumerate(items):
        total = jnp.where(((lane8 + (130 - 4 * k)) & 127) < 4, roll(value, 4 * k), total)
    zpack[...] = total

    pl.semaphore_wait(barrier, expected)

    def send_ahead(group, source, slots):
        for dx, dy, dz in AHEAD:
            send(group, source, slots.at[0 if dz > 0 else 1, 1 - dx, 1 - dy], (dx, dy, dz))

    send_ahead(0, zpack, rz)
    for dx in (-1, 1):
        for dy in (-1, 1):
            send(
                1,
                cpack.at[0 if dx < 0 else 1, 0 if dy < 0 else 1],
                rc.at[0 if dx > 0 else 1, 0 if dy > 0 else 1],
                (dx, dy, 0),
            )
        planes = pl.ds(0 if dx < 0 else 2, 2)
        send(1, main.at[planes], rx.at[0 if dx > 0 else 1], (dx, 0, 0))
    for dy in (-1, 1):
        send(1, ypack.at[0 if dy < 0 else 1], ry.at[0 if dy > 0 else 1], (0, dy, 0))
    for dx in (-1, 1):
        planes = pl.ds(0 if dx < 0 else 2, 2)
        send(2, qmain.at[planes], rqx.at[0 if dx > 0 else 1], (dx, 0, 0))
    for dy in (-1, 1):
        send(2, qpack.at[0 if dy < 0 else 1], rqy.at[0 if dy > 0 else 1], (0, dy, 0))

    stencil_load.wait()
    kc = (stencil[0, 0, 13] + stencil[1, 1, 13] + stencil[2, 2, 13]) / 3.0
    for c in range(3):
        rows = []
        for i in range(3):
            base = jnp.zeros((8, 128), F32)
            for a in range(3):
                for b in range(3):
                    for j in range(3):
                        at = 3 * (3 * a + b) + j
                        base = jnp.where(lane8 == at, stencil[i, j, 9 * a + 3 * b + c], base)
            low = lane8 < 27
            pair_a = base + jnp.where(low, roll(base, -9), 0.0)
            pair_b = base + jnp.where(low, roll(base, -3), 0.0)
            pair_ab = pair_a + jnp.where(low, roll(pair_a, -3), 0.0)
            full = base + roll(pair_a, 32) + roll(pair_b, 64) + roll(pair_ab, 96)
            rows.append(jnp.where(lane8 == ONE, 1.0, full))
        for combo, (one, two) in enumerate(((0, 1), (2, 0), (1, 2))):
            tables[3 * c + combo, 0:8, :] = rows[one]
            tables[3 * c + combo, 8:16, :] = rows[two]

    lane16 = lax.broadcasted_iota(jnp.int32, (16, 128), 1)

    def build(index, section, target, tiles, width, unroll):
        at, count, copies, first = section

        def chunk(t):
            combo = lax.rem(t, 3)
            start = pl.multiple_of(t * 16, 16)
            for tile in range(tiles):
                lanes = slice(128 * tile, 128 * tile + 128)
                picked = index[pl.ds(at + start, 16), lanes]
                for c in range(copies):
                    value = jnp.take_along_axis(
                        tables[3 * c + combo], picked, axis=1, mode="promise_in_bounds"
                    )
                    rows = pl.ds(first + c * count + start, 16)
                    if width is None:
                        high, low = split(value)
                        target[rows, lanes] = high
                        target[rows, 256 + 128 * tile : 384 + 128 * tile] = low
                        target[rows, 512 + 128 * tile : 640 + 128 * tile] = high
                    else:
                        low = value - value.astype(BF16).astype(F32)
                        lane = lane16 + 128 * tile
                        value = jnp.where((lane >= width) & (lane < 2 * width), low, value)
                        target[rows, lanes] = value.astype(BF16)

        def step(t, carry):
            for n in range(unroll):
                chunk(t * unroll + n)
            return carry

        lax.fori_loop(0, count // (16 * unroll), step, 0)

    windex_load.wait()
    for name in ("a", "b", "local"):
        build(windex, WIDE_SECTIONS[name], w, 2, None, 6)
    loaded(4, REST_TILES)

    def along_z(slots, select, ox, oy):
        return jnp.where(select, slots[1, ox + 1, oy + 1], slots[0, ox + 1, oy + 1])

    from_high_1 = (lane8 & 3) < 2
    from_high_2 = ((lane8 < 32) & ((lane8 & 1) == 0)) | ((lane8 >= 64) & (lane8 < 127))

    def wide_blocks(comp, tile):
        comps = 4

        def edge(ox, oy, k):
            return roll(along_z(rz, from_high_1, ox, oy), -4 * k)

        blocks = {}
        for p in range(4):
            own = main[p, comp] if comp < 3 else qmain[p]
            blocks[p] = edge(0, 0, p * comps + comp) if tile else own
        for n in range(2):
            for side, ox, first in ((0, -1, -2), (1, 1, 4)):
                near = rx[side, n, comp] if comp < 3 else rqx[side, n]
                plane = n if ox > 0 else n + 2
                blocks[first + n] = edge(ox, 0, plane * comps + comp) if tile else near
        for s, oy in enumerate((-1, 1)):
            k = 4 * comps + (1 - s) * comps + comp
            if tile:
                blocks["y", s] = edge(0, oy, k)
                blocks["c", s] = jnp.where(low_rows, edge(1, oy, k), edge(-1, oy, k))
                continue
            blocks["y", s] = ry[s, comp] if comp < 3 else rqy[s]
            below, above = rc[0, s, comp // 2], rc[1, s, comp // 2]
            if comp % 2 == 0:
                blocks["c", s] = jnp.where(low_rows, above, below)
            else:
                blocks["c", s] = pltpu.roll(jnp.where(low_rows, below, above), 4, 0)
        return blocks

    def store_wide(target, comps, code_at, tile):
        lanes = slice(128 * tile, 128 * tile + 128)
        for slot, comp in enumerate(comps):
            blocks = wide_blocks(comp, tile)
            order = [-2, -1, 0, 1, 2, ("y", 0), ("y", 1), ("c", 0), ("c", 1), 3, 4, 5]
            for n, key in enumerate(order):
                at = 8 * (n * len(comps) + slot)
                code = code256[code_at + at : code_at + at + 8, lanes]
                target[at : at + 8, lanes] = jnp.where(inside(code), blocks[key], 0.0)

    def ring_of(source, comps):
        def block(n):
            return source[8 * comps * n : 8 * comps * (n + 1), :]

        row = lax.broadcasted_iota(jnp.int32, (8 * comps, source.shape[1]), 0)
        odd, low = (row & 1) == 1, (row & 7) < 4
        level = jnp.where(odd, block(5), block(6))
        corner = jnp.where(odd, block(7), block(8))
        return jnp.concatenate(
            [
                block(1), block(2), block(3), jnp.where(low, level, corner),
                block(4), block(9), block(10), jnp.where(low, corner, level),
            ],
            axis=0,
        )

    def local_of(ring, comps):
        return jnp.concatenate([ring[8 * comps : 24 * comps], ring[32 * comps : 48 * comps]], axis=0)

    def ring_products(tile):
        lanes = slice(128 * tile, 128 * tile + 128)
        parts = []
        for name, start in (("a", 0), ("b", 32)):
            high, low = split(wide[start : start + 256, lanes])
            right = jnp.concatenate([high, high, low], axis=0)
            base = WIDE_SECTIONS[name][3]
            parts.append(jnp.dot(w[base : base + 288, :], right, preferred_element_type=F32))
        return tuple(
            jnp.concatenate([part[96 * c : 96 * c + 96] for part in parts], axis=0) for c in range(3)
        )

    def operator_local(value):
        high, low = split(value)
        gap = jnp.zeros((64, 256), BF16)
        right = jnp.concatenate([high, gap, high, gap, low, gap], axis=0)
        base = WIDE_SECTIONS["local"][3]
        product = jnp.dot(w[base : base + 288, :], right, preferred_element_type=F32)
        return z_shift_sum(product, 96)

    ikc = (jnp.full((8, 256), 1.0, F32) / kc)[0:1, :]
    gain_u = ((1.0 + MOM + WEIGHT * THETA) / THETA) * ikc
    gain_s = (-WEIGHT / THETA) * ikc * ikc

    ring_code = len(CODE_WIDE)
    wide_p_code = ring_code + len(CODE_RING)
    ring_p_code = wide_p_code + len(CODE_WIDE_P)

    def ring_inside():
        return inside(code256[ring_code : ring_code + 192, :])

    receive(1, plane_choices(2, 6, 3))
    store_wide(wide, (0, 1, 2), 0, 0)

    lane192 = lax.broadcasted_iota(jnp.int32, (192, 128), 1)
    at_first, at_last = lane192 == 0, lane192 == 127
    below, level, above = ring_products(0)
    below, above = pltpu.roll(below, 1, 1), pltpu.roll(above, 127, 1)
    gu, gs = gain_u[:, 0:128], gain_s[:, 0:128]
    level = level + jnp.where(at_first, 0.0, below) + jnp.where(at_last, 0.0, above)
    ring_x[:, 0:128] = gu * ring_of(wide[:, 0:128], 3) + gs * level
    ring_x[:, 128:256] = gs * (jnp.where(at_first, below, 0.0) + jnp.where(at_last, above, 0.0))

    receive(0, ahead_choices())
    store_wide(wide, (0, 1, 2), 0, 1)
    below, level, above = ring_products(1)
    below, above = pltpu.roll(below, 1, 1), pltpu.roll(above, 127, 1)
    one = ring_x[:, 0:128] + gs * jnp.where(at_first, below, jnp.where(at_last, above, 0.0))
    two = level + jnp.where(at_last, below, jnp.where(at_first, above, 0.0))
    two = ring_x[:, 128:256] + gu * ring_of(wide[:, 128:256], 3) + gs * two
    x2 = jnp.where(ring_inside(), jnp.concatenate([one, two], axis=1), 0.0)
    ring_x[...] = x2

    applied = operator_local(x2)
    even = (lane8 * 2) & 127

    def row_sum(source, n):
        return source[n, pl.ds(0, 8, 2), :] + source[n, pl.ds(1, 8, 2), :]

    def pair_sum(value, index):
        one = jnp.take_along_axis(value, index, axis=1, mode="promise_in_bounds")
        two = jnp.take_along_axis(value, index + 1, axis=1, mode="promise_in_bounds")
        return one + two

    def local_row(p):
        return 8 * (3 + 3 * p if p < 2 else 6 + 3 * p)

    for big in range(2):
        resid[3, 8 * big : 8 * big + 8, :] = eta[2 * big] + eta[2 * big + 1]
        for j in range(3):
            total = jnp.zeros((8, 128), F32)
            for p in (2 * big, 2 * big + 1):
                n = 8 * (3 * p + j)
                left = main[p, j] - applied[n : n + 8, 0:128]
                resid[4 + j, 8 * p : 8 * p + 8, :] = left
                at = local_row(p) + 8 * j
                value = ring_x[at : at + 8, 0:128] + ((1.0 / THETA) * ikc[:, 0:128]) * left
                before[p, j] = value
                total = total + eta[p] * left
            resid[j, 8 * big : 8 * big + 8, :] = total
    weights = row_sum(resid, 3)
    four_over = 4.0 / pair_sum(weights, even)
    total = jnp.zeros((8, 128), F32)
    for j in range(3):
        value = row_sum(resid, j)
        coarse[j] = pair_sum(value, even) * four_over
        first = (lane8 >= 98 + 4 * j) & (lane8 < 100 + 4 * j)
        last = (lane8 >= 32 + 4 * j) & (lane8 < 34 + 4 * j)
        here = jnp.where(first, 2 * (lane8 - (98 + 4 * j)), jnp.where(last, 2 * (lane8 + 30 - 4 * j), 0))
        packed = pair_sum(value, here) * (4.0 / pair_sum(weights, here))
        total = jnp.where(first | last, packed, total)
        for p in range(4):
            ysend[2 + j, 2 * p : 2 * p + 1, :] = before[p, j, 0:1, :]
            ysend[2 + j, 2 * p + 1 : 2 * p + 2, :] = before[p, j, 7:8, :]
            if p in (0, 3):
                n = 0 if p == 0 else 1
                xsend[n, 2 + j] = before[p, j]
                csend[n, 2, 2 * j : 2 * j + 1, :] = before[p, j, 0:1, :]
                csend[n, 2, 2 * j + 1 : 2 * j + 2, :] = before[p, j, 7:8, :]
    items = [before[p, j] for p in range(4) for j in range(3)] + [ysend[2 + j] for j in range(3)]
    for k, value in enumerate(items):
        total = jnp.where(((lane8 + (129 - 2 * k)) & 127) < 2, roll(value, 2 * k), total)
    zpack2[...] = total
    for n, value in enumerate((jnp.where(lane8 < 64, coarse[0], roll(coarse[1], 64)), coarse[2])):
        ysend[n] = value
        for m in range(2):
            xsend[m, n] = value
            csend[m, n] = value
    send_ahead(3, zpack2, rz2)
    for dx in (-1, 1):
        for dy in (-1, 1):
            send(
                4,
                csend.at[0 if dx < 0 else 1],
                rc2.at[0 if dx > 0 else 1, 0 if dy > 0 else 1],
                (dx, dy, 0),
            )
        send(4, xsend.at[0 if dx < 0 else 1], rx2.at[0 if dx > 0 else 1], (dx, 0, 0))
    for dy in (-1, 1):
        send(4, ysend, ry2.at[0 if dy > 0 else 1], (0, dy, 0))

    receive(2, plane_choices(0, 2, 1))
    store_wide(wide_p, (3,), wide_p_code, 0)
    store_wide(wide_p, (3,), wide_p_code, 1)
    q_ring = ring_of(wide_p, 1)
    high, low = split(wide_p[...])
    gap = jnp.zeros((32, 256), BF16)
    near = jnp.dot(face1[...], jnp.concatenate([high, gap, low, gap], axis=0), preferred_element_type=F32)
    near = near + pltpu.roll(q_ring, 1, 1) + pltpu.roll(q_ring, 255, 1)
    p_ring = (4.0 / 27.0) * q_ring + (1.0 / 81.0) * near
    p_ring = jnp.where(inside(code256[ring_p_code : ring_p_code + 64, :]), p_ring, 0.0)
    high, low = split(p_ring)
    near = jnp.dot(face2[...], jnp.concatenate([high, low], axis=0), preferred_element_type=F32)
    p_in, q_in = local_of(p_ring, 1), local_of(q_ring, 1)
    near = near + pltpu.roll(p_in, 1, 1) + pltpu.roll(p_in, 255, 1)
    p_out = (1.0 / 3.0) * p_in + (1.0 / 9.0) * q_in + (1.0 / 9.0) * near
    for p in range(4):
        pout_ref[p] = p_out[8 * p : 8 * p + 8, 0:128]
    for name in ("coarse", "keep"):
        build(cindex, COARSE_SECTIONS[name], w_coarse, 4, 144, 5)
    for name in ("fine", "spread"):
        build(findex, FINE_SECTIONS[name], w_fine, 2, 80, 6)
    receive(4, plane_choices(3, 5, 5))
    receive(3, ahead_choices())

    def from_side(ox, oy, n):
        if ox and oy:
            return rc2[0 if ox < 0 else 1, 0 if oy < 0 else 1, n]
        return rx2[0 if ox < 0 else 1, n] if ox else ry2[0 if oy < 0 else 1, n]

    def coarse_block(ox, oy, j):
        if (ox, oy) == (0, 0):
            inner = coarse[j]
        else:
            inner = from_side(ox, oy, j // 2)
            inner = roll(inner, 64) if j == 1 else inner
        return jnp.where(lane8 < 64, inner, roll(along_z(rz2, from_high_2, ox, oy), -(34 + 4 * j)))

    blocks = []
    near_high = (row8 & 3) < 2
    for ox in (-1, 0, 1):
        blocks += [coarse_block(ox, 0, j) for j in range(3)]
        blocks += [jnp.where(near_high, coarse_block(ox, 1, j), coarse_block(ox, -1, j)) for j in range(3)]
    value = jnp.where(inside(code128[0:144, :]), jnp.concatenate(blocks, axis=0), 0.0)
    high, low = split(value)
    right = jnp.concatenate([high, high, low, jnp.zeros((80, 128), BF16)], axis=0)
    product = jnp.dot(w_coarse[...], right, preferred_element_type=F32)
    e = gain_u[:, 0:128] * product[240:320] + gain_s[:, 0:128] * z_shift_sum(product, 80)
    e = jnp.where(inside(code128[144:224, :]), e, 0.0)
    lane80 = lax.broadcasted_iota(jnp.int32, (80, 128), 1)
    near_lane = lane80 >> 1
    far_lane = jnp.where(lane80 < 2, 64, jnp.where(lane80 >= 126, 127, 100))
    e = jnp.concatenate(
        [
            jnp.take_along_axis(e, near_lane, axis=1, mode="promise_in_bounds"),
            jnp.take_along_axis(e, far_lane, axis=1, mode="promise_in_bounds"),
        ],
        axis=1,
    )
    high, low = split(e)
    right = jnp.concatenate([high, high, low, jnp.zeros((16, 256), BF16)], axis=0)
    product = jnp.dot(w_fine[...], right, preferred_element_type=F32)

    def ring_block(ox, oy, inner, k):
        return jnp.concatenate([inner, roll(along_z(rz2, from_high_2, ox, oy), -2 * k)], axis=1)

    def layer(ox, j):
        if ox == 0:
            inner = jnp.where(odd_rows, from_side(0, -1, 2 + j), from_side(0, 1, 2 + j))
        else:
            inner = jnp.where(odd_rows, from_side(ox, -1, 2), from_side(ox, 1, 2))
            shift = (-2 * j if ox > 0 else 6 - 2 * j) % 8
            inner = pltpu.roll(inner, shift, 0) if shift else inner
        outer = jnp.where(odd_rows, along_z(rz2, from_high_2, ox, -1), along_z(rz2, from_high_2, ox, 1))
        return jnp.concatenate([inner, roll(outer, -2 * (12 + j))], axis=1)

    low_wide = lax.broadcasted_iota(jnp.int32, (8, 256), 0) < 4
    halves = [[], []]
    for half in range(2):
        for x in ((-1, 0, 1), (2, 3, 4))[half]:
            for j in range(3):
                if x == -1:
                    halves[half].append(ring_block(-1, 0, rx2[0, 2 + j], 9 + j))
                elif x == 4:
                    halves[half].append(ring_block(1, 0, rx2[1, 2 + j], j))
                else:
                    halves[half].append(ring_block(0, 0, before[x, j], 3 * x + j))
    for j in range(3):
        level = layer(0, j)
        halves[0].append(jnp.where(low_wide, level, layer(-1, j)))
        halves[1].append(jnp.where(low_wide, layer(1, j), level))
    start = jnp.concatenate(halves[0] + halves[1], axis=0)

    down = ((1.0 / THETA) * ikc) * z_shift_sum(product, 192)
    x = jnp.where(ring_inside(), start + product[576:768] - down, 0.0)
    applied = operator_local(x)
    x_in, down_in = local_of(x, 3), local_of(down, 3)
    for p in range(4):
        for j in range(3):
            n = 8 * (3 * p + j)
            step = ((1.0 / THETA) * ikc[:, 0:128]) * resid[4 + j, 8 * p : 8 * p + 8, :] - down_in[n : n + 8, 0:128]
            out_ref[j, p] = (
                x_in[n : n + 8, 0:128]
                + MOM * step
                + (WEIGHT * ikc[:, 0:128]) * (main[p, j] - applied[n : n + 8, 0:128])
            )

    totals = [
        (there, 2 * (nx + 1) * (ny + 1) * nz + 5 * nx * ny + 13 * nx + 9 * ny)
        for (there, _), (nx, ny, nz) in zip(
            ahead_choices(), [(nx, ny, nz) for nx in (1, 2) for ny in (1, 2) for nz in (1, 2)]
        )
    ]
    wait_group(send_sem.at[0], totals)


GROUPS = 5
REST_TILES = (
    CODE_256.size + CODE_128.size + COARSE_INDEX.size + FINE_INDEX.size + (FACE_1.size + FACE_2.size) // 2
) // 1024


def scratch():
    vmem = pltpu.VMEM
    return [
        vmem((3, 4, 8, 128), F32),
        vmem((4, 8, 128), F32),
        vmem((4, 8, 128), jnp.int32),
        pltpu.SMEM((8,), F32),
        pltpu.SMEM((3, 3, 27), F32),
        vmem(WIDE_INDEX.shape, jnp.int32),
        vmem(COARSE_INDEX.shape, jnp.int32),
        vmem(FINE_INDEX.shape, jnp.int32),
        vmem(CODE_256.shape, jnp.int32),
        vmem(CODE_128.shape, jnp.int32),
        vmem(FACE_1.shape, BF16),
        vmem(FACE_2.shape, BF16),
        vmem((4, 8, 128), F32),
        vmem((4, 3, 8, 128), F32),
        vmem((4, 8, 128), F32),
        vmem((2, 3, 8, 128), F32),
        vmem((2, 8, 128), F32),
        vmem((2, 2, 2, 8, 128), F32),
        vmem((8, 128), F32),
        vmem((2, 2, 3, 8, 128), F32),
        vmem((2, 3, 8, 128), F32),
        vmem((2, 2, 2, 8, 128), F32),
        vmem((2, 2, 8, 128), F32),
        vmem((2, 8, 128), F32),
        vmem((2, 3, 3, 8, 128), F32),
        vmem((4, 3, 8, 128), F32),
        vmem((3, 8, 128), F32),
        vmem((8, 128), F32),
        vmem((2, 5, 8, 128), F32),
        vmem((5, 8, 128), F32),
        vmem((2, 3, 8, 128), F32),
        vmem((2, 5, 8, 128), F32),
        vmem((2, 5, 8, 128), F32),
        vmem((2, 2, 3, 8, 128), F32),
        vmem((2, 3, 3, 8, 128), F32),
        vmem((9, 16, 128), F32),
        vmem((WIDE_ROWS, 768), BF16),
        vmem((COARSE_ROWS, 512), BF16),
        vmem((FINE_ROWS, 256), BF16),
        vmem((288, 256), F32),
        vmem((96, 256), F32),
        vmem((192, 256), F32),
        vmem((7, 32, 128), F32),
        vmem((REST_TILES, 8, 128), F32),
        pltpu.SemaphoreType.DMA((5,)),
        pltpu.SemaphoreType.DMA((1,)),
        pltpu.SemaphoreType.DMA((GROUPS,)),
    ]


def store_results(velocity, pressure, velocity_out, pressure_out, sem):
    one = pltpu.make_async_copy(velocity, velocity_out, sem.at[0])
    two = pltpu.make_async_copy(pressure, pressure_out, sem.at[1])
    one.start()
    two.start()
    one.wait()
    two.wait()


def on_device(rhs_velocity, rhs_pressure, layer_ids, visc_table, stencil):
    anywhere = pl.BlockSpec(memory_space=pltpu.HBM)
    inside = pl.BlockSpec(memory_space=pltpu.VMEM)
    results = pl.pallas_call(
        body,
        name="stokes",
        out_shape=(
            pltpu.VMEM(rhs_velocity.shape, F32),
            pltpu.VMEM(rhs_pressure.shape, F32),
        ),
        in_specs=[anywhere] * 12,
        out_specs=(inside, inside),
        scratch_shapes=scratch(),
        compiler_params=pltpu.CompilerParams(
            collective_id=0, has_side_effects=True, vmem_limit_bytes=60 * 1024 * 1024
        ),
    )(
        *(
            pltpu.with_memory_space_constraint(value, pltpu.HBM)
            for value in (
                rhs_velocity,
                rhs_pressure,
                layer_ids,
                visc_table,
                stencil.transpose(1, 2, 0),
                jnp.asarray(WIDE_INDEX),
                jnp.asarray(COARSE_INDEX),
                jnp.asarray(FINE_INDEX),
                jnp.asarray(CODE_256),
                jnp.asarray(CODE_128),
                jnp.asarray(FACE_1, BF16),
                jnp.asarray(FACE_2, BF16),
            )
        )
    )
    return pl.pallas_call(
        store_results,
        name="store",
        out_shape=(
            jax.ShapeDtypeStruct(rhs_velocity.shape, F32),
            jax.ShapeDtypeStruct(rhs_pressure.shape, F32),
        ),
        in_specs=[inside] * 2,
        out_specs=(anywhere,) * 2,
        scratch_shapes=[pltpu.SemaphoreType.DMA((2,))],
    )(*(pltpu.with_memory_space_constraint(value, pltpu.VMEM) for value in results))


def solution(mesh):
    placed = (P(None, "gx", "gy", "gz"), P("gx", "gy", "gz"), P("gx", "gy", "gz"), P(), P())
    return jax.shard_map(
        on_device,
        mesh=mesh,
        in_specs=placed,
        out_specs=(P(None, "gx", "gy", "gz"), P("gx", "gy", "gz")),
        check_vma=False,
    )
```

```python
import functools

import numpy as np
import jax
import jax.numpy as jnp
from jax import lax
from jax.experimental import pallas as pl
from jax.experimental.pallas import tpu as pltpu
from jax.sharding import PartitionSpec as P

F32 = jnp.float32
BF16 = jnp.bfloat16
MESH = pl.DeviceIdType.MESH

THETA = (1.8 + 0.2) / 2.0
DELTA = (1.8 - 0.2) / 2.0
SIGMA = THETA / DELTA
RHO0 = 1.0 / SIGMA
RHO1 = 1.0 / (2.0 * SIGMA - RHO0)
MOM = RHO1 * RHO0
WEIGHT = 2.0 * RHO1 / DELTA

XLO, XHI, YLO, YHI, ZLO, ZHI, NEVER = 1, 2, 4, 8, 16, 32, 64

ONE, ZERO = 28, 31

CORNER_X = (4, 5, -2, -1)
SIDES = [(dx, dy) for dx in (-1, 0, 1) for dy in (-1, 0, 1) if (dx, dy) != (0, 0)]
AHEAD = [(dx, dy, dz) for dx in (-1, 1, 0) for dy in (0, -1, 1) for dz in (-1, 1)]


def plane_block(x, j):
    return [(x, r, j) for r in range(8)]


def y_block(s, j):
    return [(r // 2, (-2 if s == 0 else 8) + r % 2, j) for r in range(8)]


def c_block(s, j):
    return [(CORNER_X[r // 2], (-2 if s == 0 else 8) + r % 2, j) for r in range(8)]


def edge_block(i, half):
    rows = []
    for r in range(8):
        y = -1 if r % 2 else 8
        if half == 0:
            x = r // 2 if r < 4 else (-1 if r >= 6 else None)
        else:
            x = r // 2 if r >= 4 else (4 if r < 2 else None)
        rows.append(None if x is None else (x, y, i))
    return rows


def rows_wide(comps):
    rows = []
    for x in (-2, -1, 0, 1, 2):
        for j in range(comps):
            rows += plane_block(x, j)
    for block in (y_block, c_block):
        for s in range(2):
            for j in range(comps):
                rows += block(s, j)
    for x in (3, 4, 5):
        for j in range(comps):
            rows += plane_block(x, j)
    return rows


def rows_half(half, comps):
    rows = []
    for x in ((-1, 0, 1), (2, 3, 4))[half]:
        for i in range(comps):
            rows += plane_block(x, i)
    for i in range(comps):
        rows += edge_block(i, half)
    return rows


def rows_ring(comps):
    return rows_half(0, comps) + rows_half(1, comps)


def rows_coarse_in():
    rows = []
    for dx in (-1, 0, 1):
        for j in range(3):
            rows += [(2 * dx + r // 4, r % 4, j) for r in range(8)]
        for j in range(3):
            rows += [(2 * dx + r // 4, r % 4 + (4 if r % 4 < 2 else -4), j) for r in range(8)]
    return rows


def rows_coarse_out():
    rows = []
    for q in range(3):
        for i in range(3):
            for r in range(8):
                n = 8 * q + r
                rows.append((n // 6 - 1, n % 6 - 1, i))
    return rows + [None] * 8


def index_stencil(outs, ins):
    table = np.full((len(outs), len(ins)), ZERO, np.int32)
    for m, out in enumerate(outs):
        if out is None:
            continue
        for k, source in enumerate(ins):
            if source is None:
                continue
            a, b = source[0] - out[0] + 1, source[1] - out[1] + 1
            if 0 <= a <= 2 and 0 <= b <= 2:
                table[m, k] = 3 * (3 * a + b) + source[2]
    return table


def index_same(outs, ins, scale):
    table = np.full((len(outs), len(ins)), ZERO, np.int32)
    for m, out in enumerate(outs):
        if out is None:
            continue
        for k, source in enumerate(ins):
            if source is not None and (out[0] // scale, out[1] // scale, out[2]) == source:
                table[m, k] = ONE
    return table


def index_refined(outs, ins):
    table = np.full((len(outs), len(ins)), ZERO, np.int32)
    for m, out in enumerate(outs):
        if out is None:
            continue
        for k, source in enumerate(ins):
            if source is None:
                continue
            a = [v for v in range(3) if (out[0] + v - 1) // 2 == source[0]]
            b = [v for v in range(3) if (out[1] + v - 1) // 2 == source[1]]
            if a and b:
                segment = (len(a) - 1) + 2 * (len(b) - 1)
                table[m, k] = 32 * segment + 3 * (3 * a[0] + b[0]) + source[2]
    return table


def codes(rows, x_end, y_end, lanes, z_bits):
    table = np.full((len(rows), lanes), NEVER, np.int32)
    z_row = np.full((lanes,), NEVER, np.int32)
    for lane, bits in z_bits:
        z_row[lane] = bits
    for m, row in enumerate(rows):
        if row is None:
            continue
        bits = (XLO if row[0] < 0 else 0) | (XHI if row[0] >= x_end else 0)
        bits |= (YLO if row[1] < 0 else 0) | (YHI if row[1] >= y_end else 0)
        table[m] = bits | z_row
    return table


def face_matrix(outs, ins):
    table = np.zeros((len(outs), len(ins)), np.float32)
    for m, out in enumerate(outs):
        if out is None:
            continue
        for k, source in enumerate(ins):
            if source is not None and abs(source[0] - out[0]) + abs(source[1] - out[1]) == 1:
                table[m, k] = 1.0
    return table


FINE_LANES = [(z, 0) for z in range(128)]
WIDE_Z = FINE_LANES + [(128, ZHI), (129, ZHI), (254, ZLO), (255, ZLO)]
RING_Z = FINE_LANES + [(128, ZHI), (255, ZLO)]
COARSE_Z = [(z, 0) for z in range(64)] + [(64, ZHI), (65, ZHI), (126, ZLO), (127, ZLO)]
COARSE_RING_Z = [(z, 0) for z in range(64)] + [(64, ZHI), (127, ZLO)]

WIDE = rows_wide(3)
RING = rows_ring(3)
LOCAL = [row for x in range(4) for i in range(3) for row in plane_block(x, i)]
HALF_A = rows_half(0, 3)
HALF_B = rows_half(1, 3)
COARSE_IN = rows_coarse_in()
COARSE_OUT = rows_coarse_out()

def triple(table, width):
    wide = np.full((len(table), width), ZERO, np.int32)
    count = table.shape[1]
    for n in range(3):
        wide[:, n * count : (n + 1) * count] = table
    return wide


def single(table):
    return np.concatenate([table, np.full((len(table), 256 - table.shape[1]), ZERO, np.int32)], axis=1)


def place(sections):
    places, at, row = {}, 0, 0
    for name, table, copies in sections:
        places[name] = (at, len(table), copies, row)
        at += len(table)
        row += len(table) * copies
    return places, np.concatenate([section[1] for section in sections], axis=0), row


WIDE_SECTIONS, WIDE_INDEX, WIDE_ROWS = place(
    [
        ("a", single(index_stencil(HALF_A, WIDE[0:256])), 3),
        ("b", single(index_stencil(HALF_B, WIDE[32:288])), 3),
        ("local", single(index_stencil(LOCAL, RING)), 3),
    ]
)
COARSE_SECTIONS, COARSE_INDEX, COARSE_ROWS = place(
    [
        ("coarse", triple(index_stencil(COARSE_OUT, COARSE_IN), 512), 3),
        ("keep", triple(index_same(COARSE_OUT, COARSE_IN, 1), 512), 1),
    ]
)
FINE_SECTIONS, FINE_INDEX, FINE_ROWS = place(
    [
        ("fine", triple(index_refined(RING, COARSE_OUT), 256), 3),
        ("spread", triple(index_same(RING, COARSE_OUT, 2), 256), 1),
    ]
)

CODE_WIDE = codes(WIDE, 4, 8, 256, WIDE_Z)
CODE_RING = codes(RING, 4, 8, 256, RING_Z)
CODE_COARSE = codes(COARSE_IN, 2, 4, 128, COARSE_Z)
CODE_COARSE_RING = codes(COARSE_OUT, 2, 4, 128, COARSE_RING_Z)
CODE_WIDE_P = codes(rows_wide(1), 4, 8, 256, WIDE_Z)
CODE_RING_P = codes(rows_ring(1), 4, 8, 256, RING_Z)
CODE_256 = np.concatenate([CODE_WIDE, CODE_RING, CODE_WIDE_P, CODE_RING_P], axis=0)
CODE_128 = np.concatenate([CODE_COARSE, CODE_COARSE_RING], axis=0)


def face_pair(outs, ins, width, total):
    single = face_matrix(outs, ins)
    table = np.zeros((len(outs), total), np.float32)
    table[:, : single.shape[1]] = single
    table[:, width : width + single.shape[1]] = single
    return table


FACE_1 = face_pair(rows_ring(1), rows_wide(1), 128, 256)
FACE_2 = face_pair([row for x in range(4) for row in plane_block(x, 0)], rows_ring(1), 64, 128)


def split(value):
    high = value.astype(BF16)
    low = (value - high.astype(F32)).astype(BF16)
    return high, low


def z_shift_sum(product, rows):
    lanes = product.shape[1]
    return (
        product[rows : 2 * rows]
        + pltpu.roll(product[0:rows], 1, 1)
        + pltpu.roll(product[2 * rows : 3 * rows], lanes - 1, 1)
    )


def body(
    rhs_hbm, press_hbm, ids_hbm, visc_hbm, stencil_hbm, windex_hbm, cindex_hbm, findex_hbm,
    code256_hbm, code128_hbm, face1_hbm, face2_hbm,
    out_ref, pout_ref,
    rhs, press, ids, visc, stencil, windex, cindex, findex, code256, code128, face1, face2,
    eta, main, qmain, ypack, qpack, cpack, zpack, rx, ry, rc, rqx, rqy, rz,
    before, coarse, zpack2, xsend, ysend, csend, rx2, ry2, rc2, rz2,
    tables, w, w_coarse, w_fine, wide, wide_p, ring_x, resid, blank,
    in_sem, send_sem, recv_sem,
):
    nx, ny, nz = (lax.axis_size(name) for name in ("gx", "gy", "gz"))
    ix, iy, iz = (lax.axis_index(name) for name in ("gx", "gy", "gz"))
    ends = {
        ("x", -1): ix > 0, ("x", 1): ix < nx - 1,
        ("y", -1): iy > 0, ("y", 1): iy < ny - 1,
        ("z", -1): iz > 0, ("z", 1): iz < nz - 1,
    }

    def present(dx, dy, dz):
        found = None
        for axis, step in (("x", dx), ("y", dy), ("z", dz)):
            if step:
                one = ends[axis, step]
                found = one if found is None else jnp.logical_and(found, one)
        return found

    def device(dx, dy, dz):
        return (ix + dx, iy + dy, iz + dz)

    def load(n, pairs):
        for source, target in pairs:
            pltpu.make_async_copy(source, target, in_sem.at[n]).start()

    def tiles(count):
        return blank.at[pl.ds(0, count)]

    def loaded(n, count):
        pltpu.make_async_copy(tiles(count), tiles(count), in_sem.at[n]).wait()

    visc_load = pltpu.make_async_copy(visc_hbm, visc, in_sem.at[0])
    visc_load.start()
    load(1, [(ids_hbm, ids), (rhs_hbm, rhs), (press_hbm, press)])
    stencil_load = pltpu.make_async_copy(stencil_hbm, stencil, in_sem.at[2])
    stencil_load.start()
    windex_load = pltpu.make_async_copy(windex_hbm, windex, in_sem.at[3])
    windex_load.start()
    rest = [
        (code256_hbm, code256), (code128_hbm, code128), (cindex_hbm, cindex), (findex_hbm, findex),
        (face1_hbm, face1), (face2_hbm, face2),
    ]
    load(4, rest)

    partners = AHEAD + [(dx, dy, 0) for dx, dy in SIDES]
    barrier = pltpu.get_barrier_semaphore()
    expected = 0
    for where in partners:
        there = present(*where)
        expected = expected + there.astype(jnp.int32)

        @pl.when(there)
        def _():
            pl.semaphore_signal(barrier, inc=1, device_id=device(*where), device_id_type=MESH)

    def send(group, source, target, where):
        copy = pltpu.make_async_remote_copy(
            src_ref=source,
            dst_ref=target,
            send_sem=send_sem.at[0],
            recv_sem=recv_sem.at[group],
            device_id=device(*where),
            device_id_type=MESH,
        )
        pl.when(present(*where))(copy.start)

    count_x, count_y, count_z = (
        ends[axis, -1].astype(jnp.int32) + ends[axis, 1].astype(jnp.int32) for axis in "xyz"
    )

    def wait_group(semaphore, choices):
        for there, count in choices:

            @pl.when(there)
            def _():
                pltpu.make_async_copy(tiles(count), tiles(count), semaphore).wait()

    def plane_choices(corner, along_x, along_y):
        return [
            (
                jnp.logical_and(count_x == nx, count_y == ny),
                corner * nx * ny + along_x * nx + along_y * ny,
            )
            for nx in (1, 2)
            for ny in (1, 2)
        ]

    def ahead_choices():
        return [
            (
                jnp.logical_and(jnp.logical_and(count_x == nx, count_y == ny), count_z == nz),
                (nx + 1) * (ny + 1) * nz,
            )
            for nx in (1, 2)
            for ny in (1, 2)
            for nz in (1, 2)
        ]

    def receive(group, choices):
        wait_group(recv_sem.at[group], choices)

    bad = NEVER
    for bit, end in (
        (XLO, ("x", -1)), (XHI, ("x", 1)), (YLO, ("y", -1)), (YHI, ("y", 1)), (ZLO, ("z", -1)), (ZHI, ("z", 1)),
    ):
        bad = bad + bit * (1 - ends[end].astype(jnp.int32))

    lane8 = lax.broadcasted_iota(jnp.int32, (8, 128), 1)
    row8 = lax.broadcasted_iota(jnp.int32, (8, 128), 0)
    low_rows = row8 < 4
    odd_rows = (row8 & 1) == 1

    def inside(code):
        return (code & bad) == 0

    def roll(value, shift):
        return pltpu.roll(value, shift % 128, 1) if shift % 128 else value

    visc_load.wait()
    loaded(1, 20)
    for p in range(4):
        layer = ids[p]
        value = jnp.zeros((8, 128), F32)
        for k in range(8):
            value = value + jnp.where(layer == k, visc[k], 0.0)
        eta[p] = value
        inverse = 1.0 / value
        for j in range(3):
            main[p, j] = rhs[j, p] * inverse
        qmain[p] = press[p] * value

    for s in range(2):
        for p in range(4):
            for j in range(3):
                ypack[s, j, 2 * p : 2 * p + 2, :] = main[p, j, 6 * s : 6 * s + 2, :]
            qpack[s, 2 * p : 2 * p + 2, :] = qmain[p, 6 * s : 6 * s + 2, :]
    for s in range(2):
        for v, (one, two) in enumerate(((ypack[s, 0], ypack[s, 1]), (ypack[s, 2], qpack[s]))):
            two = pltpu.roll(two, 4, 0)
            cpack[0, s, v] = jnp.where(low_rows, one, two)
            cpack[1, s, v] = jnp.where(low_rows, two, one)
    items = []
    for p in range(4):
        items += [main[p, j] for j in range(3)] + [qmain[p]]
    for s in range(2):
        items += [ypack[s, j] for j in range(3)] + [qpack[s]]
    total = jnp.zeros((8, 128), F32)
    for k, value in enumerate(items):
        total = jnp.where(((lane8 + (130 - 4 * k)) & 127) < 4, roll(value, 4 * k), total)
    zpack[...] = total

    pl.semaphore_wait(barrier, expected)

    def send_ahead(group, source, slots):
        for dx, dy, dz in AHEAD:
            send(group, source, slots.at[0 if dz > 0 else 1, 1 - dx, 1 - dy], (dx, dy, dz))

    send_ahead(0, zpack, rz)
    for dx in (-1, 1):
        for dy in (-1, 1):
            send(
                1,
                cpack.at[0 if dx < 0 else 1, 0 if dy < 0 else 1],
                rc.at[0 if dx > 0 else 1, 0 if dy > 0 else 1],
                (dx, dy, 0),
            )
        planes = pl.ds(0 if dx < 0 else 2, 2)
        send(1, main.at[planes], rx.at[0 if dx > 0 else 1], (dx, 0, 0))
    for dy in (-1, 1):
        send(1, ypack.at[0 if dy < 0 else 1], ry.at[0 if dy > 0 else 1], (0, dy, 0))
    for dx in (-1, 1):
        planes = pl.ds(0 if dx < 0 else 2, 2)
        send(2, qmain.at[planes], rqx.at[0 if dx > 0 else 1], (dx, 0, 0))
    for dy in (-1, 1):
        send(2, qpack.at[0 if dy < 0 else 1], rqy.at[0 if dy > 0 else 1], (0, dy, 0))

    stencil_load.wait()
    kc = (stencil[0, 0, 13] + stencil[1, 1, 13] + stencil[2, 2, 13]) / 3.0
    for c in range(3):
        rows = []
        for i in range(3):
            base = jnp.zeros((8, 128), F32)
            for a in range(3):
                for b in range(3):
                    for j in range(3):
                        at = 3 * (3 * a + b) + j
                        base = jnp.where(lane8 == at, stencil[i, j, 9 * a + 3 * b + c], base)
            low = lane8 < 27
            pair_a = base + jnp.where(low, roll(base, -9), 0.0)
            pair_b = base + jnp.where(low, roll(base, -3), 0.0)
            pair_ab = pair_a + jnp.where(low, roll(pair_a, -3), 0.0)
            full = base + roll(pair_a, 32) + roll(pair_b, 64) + roll(pair_ab, 96)
            rows.append(jnp.where(lane8 == ONE, 1.0, full))
        for combo, (one, two) in enumerate(((0, 1), (2, 0), (1, 2))):
            tables[3 * c + combo, 0:8, :] = rows[one]
            tables[3 * c + combo, 8:16, :] = rows[two]

    lane16 = lax.broadcasted_iota(jnp.int32, (16, 128), 1)

    def build(index, section, target, tiles, width, unroll):
        at, count, copies, first = section

        def chunk(t):
            combo = lax.rem(t, 3)
            start = pl.multiple_of(t * 16, 16)
            for tile in range(tiles):
                lanes = slice(128 * tile, 128 * tile + 128)
                picked = index[pl.ds(at + start, 16), lanes]
                for c in range(copies):
                    value = jnp.take_along_axis(
                        tables[3 * c + combo], picked, axis=1, mode="promise_in_bounds"
                    )
                    rows = pl.ds(first + c * count + start, 16)
                    if width is None:
                        high, low = split(value)
                        target[rows, lanes] = high
                        target[rows, 256 + 128 * tile : 384 + 128 * tile] = low
                        target[rows, 512 + 128 * tile : 640 + 128 * tile] = high
                    else:
                        low = value - value.astype(BF16).astype(F32)
                        lane = lane16 + 128 * tile
                        value = jnp.where((lane >= width) & (lane < 2 * width), low, value)
                        target[rows, lanes] = value.astype(BF16)

        def step(t, carry):
            for n in range(unroll):
                chunk(t * unroll + n)
            return carry

        lax.fori_loop(0, count // (16 * unroll), step, 0)

    windex_load.wait()
    for name in ("a", "b", "local"):
        build(windex, WIDE_SECTIONS[name], w, 2, None, 6)
    loaded(4, REST_TILES)

    def along_z(slots, select, ox, oy):
        return jnp.where(select, slots[1, ox + 1, oy + 1], slots[0, ox + 1, oy + 1])

    from_high_1 = (lane8 & 3) < 2
    from_high_2 = ((lane8 < 32) & ((lane8 & 1) == 0)) | ((lane8 >= 64) & (lane8 < 127))

    def wide_blocks(comp, tile):
        comps = 4

        def edge(ox, oy, k):
            return roll(along_z(rz, from_high_1, ox, oy), -4 * k)

        blocks = {}
        for p in range(4):
            own = main[p, comp] if comp < 3 else qmain[p]
            blocks[p] = edge(0, 0, p * comps + comp) if tile else own
        for n in range(2):
            for side, ox, first in ((0, -1, -2), (1, 1, 4)):
                near = rx[side, n, comp] if comp < 3 else rqx[side, n]
                plane = n if ox > 0 else n + 2
                blocks[first + n] = edge(ox, 0, plane * comps + comp) if tile else near
        for s, oy in enumerate((-1, 1)):
            k = 4 * comps + (1 - s) * comps + comp
            if tile:
                blocks["y", s] = edge(0, oy, k)
                blocks["c", s] = jnp.where(low_rows, edge(1, oy, k), edge(-1, oy, k))
                continue
            blocks["y", s] = ry[s, comp] if comp < 3 else rqy[s]
            below, above = rc[0, s, comp // 2], rc[1, s, comp // 2]
            if comp % 2 == 0:
                blocks["c", s] = jnp.where(low_rows, above, below)
            else:
                blocks["c", s] = pltpu.roll(jnp.where(low_rows, below, above), 4, 0)
        return blocks

    def store_wide(target, comps, code_at, tile):
        lanes = slice(128 * tile, 128 * tile + 128)
        for slot, comp in enumerate(comps):
            blocks = wide_blocks(comp, tile)
            order = [-2, -1, 0, 1, 2, ("y", 0), ("y", 1), ("c", 0), ("c", 1), 3, 4, 5]
            for n, key in enumerate(order):
                at = 8 * (n * len(comps) + slot)
                code = code256[code_at + at : code_at + at + 8, lanes]
                target[at : at + 8, lanes] = jnp.where(inside(code), blocks[key], 0.0)

    def ring_of(source, comps):
        def block(n):
            return source[8 * comps * n : 8 * comps * (n + 1), :]

        row = lax.broadcasted_iota(jnp.int32, (8 * comps, source.shape[1]), 0)
        odd, low = (row & 1) == 1, (row & 7) < 4
        level = jnp.where(odd, block(5), block(6))
        corner = jnp.where(odd, block(7), block(8))
        return jnp.concatenate(
            [
                block(1), block(2), block(3), jnp.where(low, level, corner),
                block(4), block(9), block(10), jnp.where(low, corner, level),
            ],
            axis=0,
        )

    def local_of(ring, comps):
        return jnp.concatenate([ring[8 * comps : 24 * comps], ring[32 * comps : 48 * comps]], axis=0)

    def operator_ring():
        parts = []
        for name, start in (("a", 0), ("b", 32)):
            high, low = split(wide[start : start + 256, :])
            right = jnp.concatenate([high, high, low], axis=0)
            base = WIDE_SECTIONS[name][3]
            product = jnp.dot(w[base : base + 288, :], right, preferred_element_type=F32)
            parts.append(z_shift_sum(product, 96))
        return jnp.concatenate(parts, axis=0)

    def operator_local(value):
        high, low = split(value)
        gap = jnp.zeros((64, 256), BF16)
        right = jnp.concatenate([high, gap, high, gap, low, gap], axis=0)
        base = WIDE_SECTIONS["local"][3]
        product = jnp.dot(w[base : base + 288, :], right, preferred_element_type=F32)
        return z_shift_sum(product, 96)

    ikc = (jnp.full((8, 256), 1.0, F32) / kc)[0:1, :]
    gain_u = ((1.0 + MOM + WEIGHT * THETA) / THETA) * ikc
    gain_s = (-WEIGHT / THETA) * ikc * ikc

    ring_code = len(CODE_WIDE)
    wide_p_code = ring_code + len(CODE_RING)
    ring_p_code = wide_p_code + len(CODE_WIDE_P)

    def ring_inside():
        return inside(code256[ring_code : ring_code + 192, :])

    receive(1, plane_choices(2, 6, 3))
    store_wide(wide, (0, 1, 2), 0, 0)

    receive(0, ahead_choices())

    store_wide(wide, (0, 1, 2), 0, 1)
    x2 = jnp.where(ring_inside(), gain_u * ring_of(wide, 3) + gain_s * operator_ring(), 0.0)
    ring_x[...] = x2

    applied = operator_local(x2)
    even = (lane8 * 2) & 127

    def row_sum(source, n):
        return source[n, pl.ds(0, 8, 2), :] + source[n, pl.ds(1, 8, 2), :]

    def pair_sum(value, index):
        one = jnp.take_along_axis(value, index, axis=1, mode="promise_in_bounds")
        two = jnp.take_along_axis(value, index + 1, axis=1, mode="promise_in_bounds")
        return one + two

    def local_row(p):
        return 8 * (3 + 3 * p if p < 2 else 6 + 3 * p)

    for big in range(2):
        resid[3, 8 * big : 8 * big + 8, :] = eta[2 * big] + eta[2 * big + 1]
        for j in range(3):
            total = jnp.zeros((8, 128), F32)
            for p in (2 * big, 2 * big + 1):
                n = 8 * (3 * p + j)
                left = main[p, j] - applied[n : n + 8, 0:128]
                resid[4 + j, 8 * p : 8 * p + 8, :] = left
                at = local_row(p) + 8 * j
                value = ring_x[at : at + 8, 0:128] + ((1.0 / THETA) * ikc[:, 0:128]) * left
                before[p, j] = value
                total = total + eta[p] * left
            resid[j, 8 * big : 8 * big + 8, :] = total
    weights = row_sum(resid, 3)
    four_over = 4.0 / pair_sum(weights, even)
    total = jnp.zeros((8, 128), F32)
    for j in range(3):
        value = row_sum(resid, j)
        coarse[j] = pair_sum(value, even) * four_over
        first = (lane8 >= 98 + 4 * j) & (lane8 < 100 + 4 * j)
        last = (lane8 >= 32 + 4 * j) & (lane8 < 34 + 4 * j)
        here = jnp.where(first, 2 * (lane8 - (98 + 4 * j)), jnp.where(last, 2 * (lane8 + 30 - 4 * j), 0))
        packed = pair_sum(value, here) * (4.0 / pair_sum(weights, here))
        total = jnp.where(first | last, packed, total)
        for p in range(4):
            ysend[2 + j, 2 * p : 2 * p + 1, :] = before[p, j, 0:1, :]
            ysend[2 + j, 2 * p + 1 : 2 * p + 2, :] = before[p, j, 7:8, :]
            if p in (0, 3):
                n = 0 if p == 0 else 1
                xsend[n, 2 + j] = before[p, j]
                csend[n, 2, 2 * j : 2 * j + 1, :] = before[p, j, 0:1, :]
                csend[n, 2, 2 * j + 1 : 2 * j + 2, :] = before[p, j, 7:8, :]
    items = [before[p, j] for p in range(4) for j in range(3)] + [ysend[2 + j] for j in range(3)]
    for k, value in enumerate(items):
        total = jnp.where(((lane8 + (129 - 2 * k)) & 127) < 2, roll(value, 2 * k), total)
    zpack2[...] = total
    for n, value in enumerate((jnp.where(lane8 < 64, coarse[0], roll(coarse[1], 64)), coarse[2])):
        ysend[n] = value
        for m in range(2):
            xsend[m, n] = value
            csend[m, n] = value
    send_ahead(3, zpack2, rz2)
    for dx in (-1, 1):
        for dy in (-1, 1):
            send(
                4,
                csend.at[0 if dx < 0 else 1],
                rc2.at[0 if dx > 0 else 1, 0 if dy > 0 else 1],
                (dx, dy, 0),
            )
        send(4, xsend.at[0 if dx < 0 else 1], rx2.at[0 if dx > 0 else 1], (dx, 0, 0))
    for dy in (-1, 1):
        send(4, ysend, ry2.at[0 if dy > 0 else 1], (0, dy, 0))

    receive(2, plane_choices(0, 2, 1))
    store_wide(wide_p, (3,), wide_p_code, 0)
    store_wide(wide_p, (3,), wide_p_code, 1)
    q_ring = ring_of(wide_p, 1)
    high, low = split(wide_p[...])
    gap = jnp.zeros((32, 256), BF16)
    near = jnp.dot(face1[...], jnp.concatenate([high, gap, low, gap], axis=0), preferred_element_type=F32)
    near = near + pltpu.roll(q_ring, 1, 1) + pltpu.roll(q_ring, 255, 1)
    p_ring = (4.0 / 27.0) * q_ring + (1.0 / 81.0) * near
    p_ring = jnp.where(inside(code256[ring_p_code : ring_p_code + 64, :]), p_ring, 0.0)
    high, low = split(p_ring)
    near = jnp.dot(face2[...], jnp.concatenate([high, low], axis=0), preferred_element_type=F32)
    p_in, q_in = local_of(p_ring, 1), local_of(q_ring, 1)
    near = near + pltpu.roll(p_in, 1, 1) + pltpu.roll(p_in, 255, 1)
    p_out = (1.0 / 3.0) * p_in + (1.0 / 9.0) * q_in + (1.0 / 9.0) * near
    for p in range(4):
        pout_ref[p] = p_out[8 * p : 8 * p + 8, 0:128]
    for name in ("coarse", "keep"):
        build(cindex, COARSE_SECTIONS[name], w_coarse, 4, 144, 5)
    for name in ("fine", "spread"):
        build(findex, FINE_SECTIONS[name], w_fine, 2, 80, 6)
    receive(4, plane_choices(3, 5, 5))
    receive(3, ahead_choices())

    def from_side(ox, oy, n):
        if ox and oy:
            return rc2[0 if ox < 0 else 1, 0 if oy < 0 else 1, n]
        return rx2[0 if ox < 0 else 1, n] if ox else ry2[0 if oy < 0 else 1, n]

    def coarse_block(ox, oy, j):
        if (ox, oy) == (0, 0):
            inner = coarse[j]
        else:
            inner = from_side(ox, oy, j // 2)
            inner = roll(inner, 64) if j == 1 else inner
        return jnp.where(lane8 < 64, inner, roll(along_z(rz2, from_high_2, ox, oy), -(34 + 4 * j)))

    blocks = []
    near_high = (row8 & 3) < 2
    for ox in (-1, 0, 1):
        blocks += [coarse_block(ox, 0, j) for j in range(3)]
        blocks += [jnp.where(near_high, coarse_block(ox, 1, j), coarse_block(ox, -1, j)) for j in range(3)]
    value = jnp.where(inside(code128[0:144, :]), jnp.concatenate(blocks, axis=0), 0.0)
    high, low = split(value)
    right = jnp.concatenate([high, high, low, jnp.zeros((80, 128), BF16)], axis=0)
    product = jnp.dot(w_coarse[...], right, preferred_element_type=F32)
    e = gain_u[:, 0:128] * product[240:320] + gain_s[:, 0:128] * z_shift_sum(product, 80)
    e = jnp.where(inside(code128[144:224, :]), e, 0.0)
    lane80 = lax.broadcasted_iota(jnp.int32, (80, 128), 1)
    near_lane = lane80 >> 1
    far_lane = jnp.where(lane80 < 2, 64, jnp.where(lane80 >= 126, 127, 100))
    e = jnp.concatenate(
        [
            jnp.take_along_axis(e, near_lane, axis=1, mode="promise_in_bounds"),
            jnp.take_along_axis(e, far_lane, axis=1, mode="promise_in_bounds"),
        ],
        axis=1,
    )
    high, low = split(e)
    right = jnp.concatenate([high, high, low, jnp.zeros((16, 256), BF16)], axis=0)
    product = jnp.dot(w_fine[...], right, preferred_element_type=F32)

    def ring_block(ox, oy, inner, k):
        return jnp.concatenate([inner, roll(along_z(rz2, from_high_2, ox, oy), -2 * k)], axis=1)

    def layer(ox, j):
        if ox == 0:
            inner = jnp.where(odd_rows, from_side(0, -1, 2 + j), from_side(0, 1, 2 + j))
        else:
            inner = jnp.where(odd_rows, from_side(ox, -1, 2), from_side(ox, 1, 2))
            shift = (-2 * j if ox > 0 else 6 - 2 * j) % 8
            inner = pltpu.roll(inner, shift, 0) if shift else inner
        outer = jnp.where(odd_rows, along_z(rz2, from_high_2, ox, -1), along_z(rz2, from_high_2, ox, 1))
        return jnp.concatenate([inner, roll(outer, -2 * (12 + j))], axis=1)

    low_wide = lax.broadcasted_iota(jnp.int32, (8, 256), 0) < 4
    halves = [[], []]
    for half in range(2):
        for x in ((-1, 0, 1), (2, 3, 4))[half]:
            for j in range(3):
                if x == -1:
                    halves[half].append(ring_block(-1, 0, rx2[0, 2 + j], 9 + j))
                elif x == 4:
                    halves[half].append(ring_block(1, 0, rx2[1, 2 + j], j))
                else:
                    halves[half].append(ring_block(0, 0, before[x, j], 3 * x + j))
    for j in range(3):
        level = layer(0, j)
        halves[0].append(jnp.where(low_wide, level, layer(-1, j)))
        halves[1].append(jnp.where(low_wide, layer(1, j), level))
    start = jnp.concatenate(halves[0] + halves[1], axis=0)

    down = ((1.0 / THETA) * ikc) * z_shift_sum(product, 192)
    x = jnp.where(ring_inside(), start + product[576:768] - down, 0.0)
    applied = operator_local(x)
    x_in, down_in = local_of(x, 3), local_of(down, 3)
    for p in range(4):
        for j in range(3):
            n = 8 * (3 * p + j)
            step = ((1.0 / THETA) * ikc[:, 0:128]) * resid[4 + j, 8 * p : 8 * p + 8, :] - down_in[n : n + 8, 0:128]
            out_ref[j, p] = (
                x_in[n : n + 8, 0:128]
                + MOM * step
                + (WEIGHT * ikc[:, 0:128]) * (main[p, j] - applied[n : n + 8, 0:128])
            )

    totals = [
        (there, 2 * (nx + 1) * (ny + 1) * nz + 5 * nx * ny + 13 * nx + 9 * ny)
        for (there, _), (nx, ny, nz) in zip(
            ahead_choices(), [(nx, ny, nz) for nx in (1, 2) for ny in (1, 2) for nz in (1, 2)]
        )
    ]
    wait_group(send_sem.at[0], totals)


GROUPS = 5
REST_TILES = (
    CODE_256.size + CODE_128.size + COARSE_INDEX.size + FINE_INDEX.size + (FACE_1.size + FACE_2.size) // 2
) // 1024


def scratch():
    vmem = pltpu.VMEM
    return [
        vmem((3, 4, 8, 128), F32),
        vmem((4, 8, 128), F32),
        vmem((4, 8, 128), jnp.int32),
        pltpu.SMEM((8,), F32),
        pltpu.SMEM((3, 3, 27), F32),
        vmem(WIDE_INDEX.shape, jnp.int32),
        vmem(COARSE_INDEX.shape, jnp.int32),
        vmem(FINE_INDEX.shape, jnp.int32),
        vmem(CODE_256.shape, jnp.int32),
        vmem(CODE_128.shape, jnp.int32),
        vmem(FACE_1.shape, BF16),
        vmem(FACE_2.shape, BF16),
        vmem((4, 8, 128), F32),
        vmem((4, 3, 8, 128), F32),
        vmem((4, 8, 128), F32),
        vmem((2, 3, 8, 128), F32),
        vmem((2, 8, 128), F32),
        vmem((2, 2, 2, 8, 128), F32),
        vmem((8, 128), F32),
        vmem((2, 2, 3, 8, 128), F32),
        vmem((2, 3, 8, 128), F32),
        vmem((2, 2, 2, 8, 128), F32),
        vmem((2, 2, 8, 128), F32),
        vmem((2, 8, 128), F32),
        vmem((2, 3, 3, 8, 128), F32),
        vmem((4, 3, 8, 128), F32),
        vmem((3, 8, 128), F32),
        vmem((8, 128), F32),
        vmem((2, 5, 8, 128), F32),
        vmem((5, 8, 128), F32),
        vmem((2, 3, 8, 128), F32),
        vmem((2, 5, 8, 128), F32),
        vmem((2, 5, 8, 128), F32),
        vmem((2, 2, 3, 8, 128), F32),
        vmem((2, 3, 3, 8, 128), F32),
        vmem((9, 16, 128), F32),
        vmem((WIDE_ROWS, 768), BF16),
        vmem((COARSE_ROWS, 512), BF16),
        vmem((FINE_ROWS, 256), BF16),
        vmem((288, 256), F32),
        vmem((96, 256), F32),
        vmem((192, 256), F32),
        vmem((7, 32, 128), F32),
        vmem((REST_TILES, 8, 128), F32),
        pltpu.SemaphoreType.DMA((5,)),
        pltpu.SemaphoreType.DMA((1,)),
        pltpu.SemaphoreType.DMA((GROUPS,)),
    ]


def store_results(velocity, pressure, velocity_out, pressure_out, sem):
    one = pltpu.make_async_copy(velocity, velocity_out, sem.at[0])
    two = pltpu.make_async_copy(pressure, pressure_out, sem.at[1])
    one.start()
    two.start()
    one.wait()
    two.wait()


def on_device(rhs_velocity, rhs_pressure, layer_ids, visc_table, stencil):
    anywhere = pl.BlockSpec(memory_space=pltpu.HBM)
    inside = pl.BlockSpec(memory_space=pltpu.VMEM)
    results = pl.pallas_call(
        body,
        name="stokes",
        out_shape=(
            pltpu.VMEM(rhs_velocity.shape, F32),
            pltpu.VMEM(rhs_pressure.shape, F32),
        ),
        in_specs=[anywhere] * 12,
        out_specs=(inside, inside),
        scratch_shapes=scratch(),
        compiler_params=pltpu.CompilerParams(
            collective_id=0, has_side_effects=True, vmem_limit_bytes=60 * 1024 * 1024
        ),
    )(
        *(
            pltpu.with_memory_space_constraint(value, pltpu.HBM)
            for value in (
                rhs_velocity,
                rhs_pressure,
                layer_ids,
                visc_table,
                stencil.transpose(1, 2, 0),
                jnp.asarray(WIDE_INDEX),
                jnp.asarray(COARSE_INDEX),
                jnp.asarray(FINE_INDEX),
                jnp.asarray(CODE_256),
                jnp.asarray(CODE_128),
                jnp.asarray(FACE_1, BF16),
                jnp.asarray(FACE_2, BF16),
            )
        )
    )
    return pl.pallas_call(
        store_results,
        name="store",
        out_shape=(
            jax.ShapeDtypeStruct(rhs_velocity.shape, F32),
            jax.ShapeDtypeStruct(rhs_pressure.shape, F32),
        ),
        in_specs=[inside] * 2,
        out_specs=(anywhere,) * 2,
        scratch_shapes=[pltpu.SemaphoreType.DMA((2,))],
    )(*(pltpu.with_memory_space_constraint(value, pltpu.VMEM) for value in results))


def solution(mesh):
    placed = (P(None, "gx", "gy", "gz"), P("gx", "gy", "gz"), P("gx", "gy", "gz"), P(), P())
    return jax.shard_map(
        on_device,
        mesh=mesh,
        in_specs=placed,
        out_specs=(P(None, "gx", "gy", "gz"), P("gx", "gy", "gz")),
        check_vma=False,
    )
```

```python
import functools

import numpy as np
import jax
import jax.numpy as jnp
from jax import lax
from jax.experimental import pallas as pl
from jax.experimental.pallas import tpu as pltpu
from jax.sharding import PartitionSpec as P

F32 = jnp.float32
BF16 = jnp.bfloat16
MESH = pl.DeviceIdType.MESH

THETA = (1.8 + 0.2) / 2.0
DELTA = (1.8 - 0.2) / 2.0
SIGMA = THETA / DELTA
RHO0 = 1.0 / SIGMA
RHO1 = 1.0 / (2.0 * SIGMA - RHO0)
MOM = RHO1 * RHO0
WEIGHT = 2.0 * RHO1 / DELTA

XLO, XHI, YLO, YHI, ZLO, ZHI, NEVER = 1, 2, 4, 8, 16, 32, 64

ONE, ZERO = 28, 31

CORNER_X = (4, 5, -2, -1)
SIDES = [(dx, dy) for dx in (-1, 0, 1) for dy in (-1, 0, 1) if (dx, dy) != (0, 0)]
AHEAD = [(dx, dy, dz) for dx in (-1, 1, 0) for dy in (0, -1, 1) for dz in (-1, 1)]


def plane_block(x, j):
    return [(x, r, j) for r in range(8)]


def y_block(s, j):
    return [(r // 2, (-2 if s == 0 else 8) + r % 2, j) for r in range(8)]


def c_block(s, j):
    return [(CORNER_X[r // 2], (-2 if s == 0 else 8) + r % 2, j) for r in range(8)]


def edge_block(i, half):
    rows = []
    for r in range(8):
        y = -1 if r % 2 else 8
        if half == 0:
            x = r // 2 if r < 4 else (-1 if r >= 6 else None)
        else:
            x = r // 2 if r >= 4 else (4 if r < 2 else None)
        rows.append(None if x is None else (x, y, i))
    return rows


def rows_wide(comps):
    rows = []
    for x in (-2, -1, 0, 1, 2):
        for j in range(comps):
            rows += plane_block(x, j)
    for block in (y_block, c_block):
        for s in range(2):
            for j in range(comps):
                rows += block(s, j)
    for x in (3, 4, 5):
        for j in range(comps):
            rows += plane_block(x, j)
    return rows


def rows_half(half, comps):
    rows = []
    for x in ((-1, 0, 1), (2, 3, 4))[half]:
        for i in range(comps):
            rows += plane_block(x, i)
    for i in range(comps):
        rows += edge_block(i, half)
    return rows


def rows_ring(comps):
    return rows_half(0, comps) + rows_half(1, comps)


def rows_coarse_in():
    rows = []
    for dx in (-1, 0, 1):
        for j in range(3):
            rows += [(2 * dx + r // 4, r % 4, j) for r in range(8)]
        for j in range(3):
            rows += [(2 * dx + r // 4, r % 4 + (4 if r % 4 < 2 else -4), j) for r in range(8)]
    return rows


def rows_coarse_out():
    rows = []
    for q in range(3):
        for i in range(3):
            for r in range(8):
                n = 8 * q + r
                rows.append((n // 6 - 1, n % 6 - 1, i))
    return rows + [None] * 8


def index_stencil(outs, ins):
    table = np.full((len(outs), len(ins)), ZERO, np.int32)
    for m, out in enumerate(outs):
        if out is None:
            continue
        for k, source in enumerate(ins):
            if source is None:
                continue
            a, b = source[0] - out[0] + 1, source[1] - out[1] + 1
            if 0 <= a <= 2 and 0 <= b <= 2:
                table[m, k] = 3 * (3 * a + b) + source[2]
    return table


def index_same(outs, ins, scale):
    table = np.full((len(outs), len(ins)), ZERO, np.int32)
    for m, out in enumerate(outs):
        if out is None:
            continue
        for k, source in enumerate(ins):
            if source is not None and (out[0] // scale, out[1] // scale, out[2]) == source:
                table[m, k] = ONE
    return table


def index_refined(outs, ins):
    table = np.full((len(outs), len(ins)), ZERO, np.int32)
    for m, out in enumerate(outs):
        if out is None:
            continue
        for k, source in enumerate(ins):
            if source is None:
                continue
            a = [v for v in range(3) if (out[0] + v - 1) // 2 == source[0]]
            b = [v for v in range(3) if (out[1] + v - 1) // 2 == source[1]]
            if a and b:
                segment = (len(a) - 1) + 2 * (len(b) - 1)
                table[m, k] = 32 * segment + 3 * (3 * a[0] + b[0]) + source[2]
    return table


def codes(rows, x_end, y_end, lanes, z_bits):
    table = np.full((len(rows), lanes), NEVER, np.int32)
    z_row = np.full((lanes,), NEVER, np.int32)
    for lane, bits in z_bits:
        z_row[lane] = bits
    for m, row in enumerate(rows):
        if row is None:
            continue
        bits = (XLO if row[0] < 0 else 0) | (XHI if row[0] >= x_end else 0)
        bits |= (YLO if row[1] < 0 else 0) | (YHI if row[1] >= y_end else 0)
        table[m] = bits | z_row
    return table


def face_matrix(outs, ins):
    table = np.zeros((len(outs), len(ins)), np.float32)
    for m, out in enumerate(outs):
        if out is None:
            continue
        for k, source in enumerate(ins):
            if source is not None and abs(source[0] - out[0]) + abs(source[1] - out[1]) == 1:
                table[m, k] = 1.0
    return table


FINE_LANES = [(z, 0) for z in range(128)]
WIDE_Z = FINE_LANES + [(128, ZHI), (129, ZHI), (254, ZLO), (255, ZLO)]
RING_Z = FINE_LANES + [(128, ZHI), (255, ZLO)]
COARSE_Z = [(z, 0) for z in range(64)] + [(64, ZHI), (65, ZHI), (126, ZLO), (127, ZLO)]
COARSE_RING_Z = [(z, 0) for z in range(64)] + [(64, ZHI), (127, ZLO)]

WIDE = rows_wide(3)
RING = rows_ring(3)
LOCAL = [row for x in range(4) for i in range(3) for row in plane_block(x, i)]
HALF_A = rows_half(0, 3)
HALF_B = rows_half(1, 3)
COARSE_IN = rows_coarse_in()
COARSE_OUT = rows_coarse_out()

def triple(table, width):
    wide = np.full((len(table), width), ZERO, np.int32)
    count = table.shape[1]
    for n in range(3):
        wide[:, n * count : (n + 1) * count] = table
    return wide


def single(table):
    return np.concatenate([table, np.full((len(table), 256 - table.shape[1]), ZERO, np.int32)], axis=1)


def place(sections):
    places, at, row = {}, 0, 0
    for name, table, copies in sections:
        places[name] = (at, len(table), copies, row)
        at += len(table)
        row += len(table) * copies
    return places, np.concatenate([section[1] for section in sections], axis=0), row


WIDE_SECTIONS, WIDE_INDEX, WIDE_ROWS = place(
    [
        ("a", single(index_stencil(HALF_A, WIDE[0:256])), 3),
        ("b", single(index_stencil(HALF_B, WIDE[32:288])), 3),
        ("local", single(index_stencil(LOCAL, RING)), 3),
    ]
)
COARSE_SECTIONS, COARSE_INDEX, COARSE_ROWS = place(
    [
        ("coarse", triple(index_stencil(COARSE_OUT, COARSE_IN), 512), 3),
        ("keep", triple(index_same(COARSE_OUT, COARSE_IN, 1), 512), 1),
    ]
)
FINE_SECTIONS, FINE_INDEX, FINE_ROWS = place(
    [
        ("fine", triple(index_refined(RING, COARSE_OUT), 256), 3),
        ("spread", triple(index_same(RING, COARSE_OUT, 2), 256), 1),
    ]
)

CODE_WIDE = codes(WIDE, 4, 8, 256, WIDE_Z)
CODE_RING = codes(RING, 4, 8, 256, RING_Z)
CODE_COARSE = codes(COARSE_IN, 2, 4, 128, COARSE_Z)
CODE_COARSE_RING = codes(COARSE_OUT, 2, 4, 128, COARSE_RING_Z)
CODE_WIDE_P = codes(rows_wide(1), 4, 8, 256, WIDE_Z)
CODE_RING_P = codes(rows_ring(1), 4, 8, 256, RING_Z)
CODE_256 = np.concatenate([CODE_WIDE, CODE_RING, CODE_WIDE_P, CODE_RING_P], axis=0)
CODE_128 = np.concatenate([CODE_COARSE, CODE_COARSE_RING], axis=0)


def face_pair(outs, ins, width, total):
    single = face_matrix(outs, ins)
    table = np.zeros((len(outs), total), np.float32)
    table[:, : single.shape[1]] = single
    table[:, width : width + single.shape[1]] = single
    return table


FACE_1 = face_pair(rows_ring(1), rows_wide(1), 128, 256)
FACE_2 = face_pair([row for x in range(4) for row in plane_block(x, 0)], rows_ring(1), 64, 128)


def split(value):
    high = value.astype(BF16)
    low = (value - high.astype(F32)).astype(BF16)
    return high, low


def z_shift_sum(product, rows):
    lanes = product.shape[1]
    return (
        product[rows : 2 * rows]
        + pltpu.roll(product[0:rows], 1, 1)
        + pltpu.roll(product[2 * rows : 3 * rows], lanes - 1, 1)
    )


def body(
    rhs_hbm, press_hbm, ids_hbm, visc_hbm, stencil_hbm, windex_hbm, cindex_hbm, findex_hbm,
    code256_hbm, code128_hbm, face1_hbm, face2_hbm,
    out_ref, pout_ref,
    rhs, press, ids, visc, stencil, windex, cindex, findex, code256, code128, face1, face2,
    eta, main, qmain, ypack, qpack, cpack, zpack, rx, ry, rc, rqx, rqy, rz,
    before, coarse, zpack2, xsend, ysend, csend, rx2, ry2, rc2, rz2,
    tables, w, w_coarse, w_fine, wide, wide_p, ring_x, resid, blank,
    in_sem, send_sem, recv_sem,
):
    nx, ny, nz = (lax.axis_size(name) for name in ("gx", "gy", "gz"))
    ix, iy, iz = (lax.axis_index(name) for name in ("gx", "gy", "gz"))
    ends = {
        ("x", -1): ix > 0, ("x", 1): ix < nx - 1,
        ("y", -1): iy > 0, ("y", 1): iy < ny - 1,
        ("z", -1): iz > 0, ("z", 1): iz < nz - 1,
    }

    def present(dx, dy, dz):
        found = None
        for axis, step in (("x", dx), ("y", dy), ("z", dz)):
            if step:
                one = ends[axis, step]
                found = one if found is None else jnp.logical_and(found, one)
        return found

    def device(dx, dy, dz):
        return (ix + dx, iy + dy, iz + dz)

    def load(n, pairs):
        for source, target in pairs:
            pltpu.make_async_copy(source, target, in_sem.at[n]).start()

    def tiles(count):
        return blank.at[pl.ds(0, count)]

    def loaded(n, count):
        pltpu.make_async_copy(tiles(count), tiles(count), in_sem.at[n]).wait()

    visc_load = pltpu.make_async_copy(visc_hbm, visc, in_sem.at[0])
    visc_load.start()
    load(1, [(ids_hbm, ids), (rhs_hbm, rhs), (press_hbm, press)])
    stencil_load = pltpu.make_async_copy(stencil_hbm, stencil, in_sem.at[2])
    stencil_load.start()
    windex_load = pltpu.make_async_copy(windex_hbm, windex, in_sem.at[3])
    windex_load.start()
    rest = [
        (code256_hbm, code256), (code128_hbm, code128), (cindex_hbm, cindex), (findex_hbm, findex),
        (face1_hbm, face1), (face2_hbm, face2),
    ]
    load(4, rest)

    partners = AHEAD + [(dx, dy, 0) for dx, dy in SIDES]
    barrier = pltpu.get_barrier_semaphore()
    expected = 0
    for where in partners:
        there = present(*where)
        expected = expected + there.astype(jnp.int32)

        @pl.when(there)
        def _():
            pl.semaphore_signal(barrier, inc=1, device_id=device(*where), device_id_type=MESH)

    def send(group, source, target, where):
        copy = pltpu.make_async_remote_copy(
            src_ref=source,
            dst_ref=target,
            send_sem=send_sem.at[0],
            recv_sem=recv_sem.at[group],
            device_id=device(*where),
            device_id_type=MESH,
        )
        pl.when(present(*where))(copy.start)

    count_x, count_y, count_z = (
        ends[axis, -1].astype(jnp.int32) + ends[axis, 1].astype(jnp.int32) for axis in "xyz"
    )

    def wait_group(semaphore, choices):
        for there, count in choices:

            @pl.when(there)
            def _():
                pltpu.make_async_copy(tiles(count), tiles(count), semaphore).wait()

    def plane_choices(corner, along_x, along_y):
        return [
            (
                jnp.logical_and(count_x == nx, count_y == ny),
                2 * (corner * nx * ny + along_x * nx + along_y * ny),
            )
            for nx in (1, 2)
            for ny in (1, 2)
        ]

    def ahead_choices(corner):
        return [
            (
                jnp.logical_and(jnp.logical_and(count_x == nx, count_y == ny), count_z == nz),
                (2 + 2 * nx + 2 * ny + corner * nx * ny) * nz,
            )
            for nx in (1, 2)
            for ny in (1, 2)
            for nz in (1, 2)
        ]

    def receive(group, choices):
        wait_group(recv_sem.at[group], choices)

    bad = NEVER
    for bit, end in (
        (XLO, ("x", -1)), (XHI, ("x", 1)), (YLO, ("y", -1)), (YHI, ("y", 1)), (ZLO, ("z", -1)), (ZHI, ("z", 1)),
    ):
        bad = bad + bit * (1 - ends[end].astype(jnp.int32))

    lane8 = lax.broadcasted_iota(jnp.int32, (8, 128), 1)
    row8 = lax.broadcasted_iota(jnp.int32, (8, 128), 0)
    low_rows = row8 < 4
    odd_rows = (row8 & 1) == 1

    def inside(code):
        return (code & bad) == 0

    def roll(value, shift):
        return pltpu.roll(value, shift % 128, 1) if shift % 128 else value

    visc_load.wait()
    loaded(1, 40)
    for p in range(4):
        layer = ids[p]
        value = jnp.zeros((8, 128), F32)
        for k in range(8):
            value = value + jnp.where(layer == k, visc[k], 0.0)
        eta[p] = value
        inverse = 1.0 / value
        for j in range(3):
            main[p, j] = rhs[j, p] * inverse
        qmain[p] = press[p] * value

    for s in range(2):
        for p in range(4):
            for j in range(3):
                ypack[s, j, 2 * p : 2 * p + 2, :] = main[p, j, 6 * s : 6 * s + 2, :]
            qpack[s, 2 * p : 2 * p + 2, :] = qmain[p, 6 * s : 6 * s + 2, :]
    for s in range(2):
        for v, (one, two) in enumerate(((ypack[s, 0], ypack[s, 1]), (ypack[s, 2], qpack[s]))):
            two = pltpu.roll(two, 4, 0)
            cpack[0, s, v] = jnp.where(low_rows, one, two)
            cpack[1, s, v] = jnp.where(low_rows, two, one)
    items = []
    for p in range(4):
        items += [main[p, j] for j in range(3)] + [qmain[p]]
    for s in range(2):
        items += [ypack[s, j] for j in range(3)] + [qpack[s]]
    total = jnp.zeros((8, 128), F32)
    for k, value in enumerate(items):
        total = jnp.where(((lane8 + (130 - 4 * k)) & 127) < 4, roll(value, 4 * k), total)
    zpack[...] = total

    pl.semaphore_wait(barrier, expected)

    def send_ahead(group, source, slots):
        for dx, dy, dz in AHEAD:
            slot = slots.at[0 if dz > 0 else 1, 1 - dx, 1 - dy]
            if group == 0 and dx and dy:
                half = pl.ds(0 if dx < 0 else 4, 4)
                send(group, source.at[half], slot.at[half], (dx, dy, dz))
            else:
                send(group, source, slot, (dx, dy, dz))

    send_ahead(0, zpack, rz)
    for dx in (-1, 1):
        for dy in (-1, 1):
            send(
                1,
                cpack.at[0 if dx < 0 else 1, 0 if dy < 0 else 1],
                rc.at[0 if dx > 0 else 1, 0 if dy > 0 else 1],
                (dx, dy, 0),
            )
        planes = pl.ds(0 if dx < 0 else 2, 2)
        send(1, main.at[planes], rx.at[0 if dx > 0 else 1], (dx, 0, 0))
    for dy in (-1, 1):
        send(1, ypack.at[0 if dy < 0 else 1], ry.at[0 if dy > 0 else 1], (0, dy, 0))
    for dx in (-1, 1):
        planes = pl.ds(0 if dx < 0 else 2, 2)
        send(2, qmain.at[planes], rqx.at[0 if dx > 0 else 1], (dx, 0, 0))
    for dy in (-1, 1):
        send(2, qpack.at[0 if dy < 0 else 1], rqy.at[0 if dy > 0 else 1], (0, dy, 0))

    stencil_load.wait()
    kc = (stencil[0, 0, 13] + stencil[1, 1, 13] + stencil[2, 2, 13]) / 3.0
    for c in range(3):
        rows = []
        for i in range(3):
            base = jnp.zeros((8, 128), F32)
            for a in range(3):
                for b in range(3):
                    for j in range(3):
                        at = 3 * (3 * a + b) + j
                        base = jnp.where(lane8 == at, stencil[i, j, 9 * a + 3 * b + c], base)
            low = lane8 < 27
            pair_a = base + jnp.where(low, roll(base, -9), 0.0)
            pair_b = base + jnp.where(low, roll(base, -3), 0.0)
            pair_ab = pair_a + jnp.where(low, roll(pair_a, -3), 0.0)
            full = base + roll(pair_a, 32) + roll(pair_b, 64) + roll(pair_ab, 96)
            rows.append(jnp.where(lane8 == ONE, 1.0, full))
        for combo, (one, two) in enumerate(((0, 1), (2, 0), (1, 2))):
            tables[3 * c + combo, 0:8, :] = rows[one]
            tables[3 * c + combo, 8:16, :] = rows[two]

    lane16 = lax.broadcasted_iota(jnp.int32, (16, 128), 1)

    def build(index, section, target, tiles, width, unroll):
        at, count, copies, first = section

        def chunk(t):
            combo = lax.rem(t, 3)
            start = pl.multiple_of(t * 16, 16)
            for tile in range(tiles):
                lanes = slice(128 * tile, 128 * tile + 128)
                picked = index[pl.ds(at + start, 16), lanes]
                for c in range(copies):
                    value = jnp.take_along_axis(
                        tables[3 * c + combo], picked, axis=1, mode="promise_in_bounds"
                    )
                    rows = pl.ds(first + c * count + start, 16)
                    if width is None:
                        high, low = split(value)
                        target[rows, lanes] = high
                        target[rows, 256 + 128 * tile : 384 + 128 * tile] = low
                        target[rows, 512 + 128 * tile : 640 + 128 * tile] = high
                    else:
                        low = value - value.astype(BF16).astype(F32)
                        lane = lane16 + 128 * tile
                        value = jnp.where((lane >= width) & (lane < 2 * width), low, value)
                        target[rows, lanes] = value.astype(BF16)

        def step(t, carry):
            for n in range(unroll):
                chunk(t * unroll + n)
            return carry

        lax.fori_loop(0, count // (16 * unroll), step, 0)

    windex_load.wait()
    for name in ("a", "b", "local"):
        build(windex, WIDE_SECTIONS[name], w, 2, None, 6)
    loaded(4, 2 * REST_TILES)

    def along_z(slots, select, ox, oy):
        return jnp.where(select, slots[1, ox + 1, oy + 1], slots[0, ox + 1, oy + 1])

    from_high_1 = (lane8 & 3) < 2
    from_high_2 = ((lane8 < 32) & ((lane8 & 1) == 0)) | ((lane8 >= 64) & (lane8 < 127))

    def wide_blocks(comp, tile):
        comps = 4

        def edge(ox, oy, k):
            return roll(along_z(rz, from_high_1, ox, oy), -4 * k)

        blocks = {}
        for p in range(4):
            own = main[p, comp] if comp < 3 else qmain[p]
            blocks[p] = edge(0, 0, p * comps + comp) if tile else own
        for n in range(2):
            for side, ox, first in ((0, -1, -2), (1, 1, 4)):
                near = rx[side, n, comp] if comp < 3 else rqx[side, n]
                plane = n if ox > 0 else n + 2
                blocks[first + n] = edge(ox, 0, plane * comps + comp) if tile else near
        for s, oy in enumerate((-1, 1)):
            k = 4 * comps + (1 - s) * comps + comp
            if tile:
                blocks["y", s] = edge(0, oy, k)
                blocks["c", s] = jnp.where(low_rows, edge(1, oy, k), edge(-1, oy, k))
                continue
            blocks["y", s] = ry[s, comp] if comp < 3 else rqy[s]
            below, above = rc[0, s, comp // 2], rc[1, s, comp // 2]
            if comp % 2 == 0:
                blocks["c", s] = jnp.where(low_rows, above, below)
            else:
                blocks["c", s] = pltpu.roll(jnp.where(low_rows, below, above), 4, 0)
        return blocks

    def store_wide(target, comps, code_at, tile):
        lanes = slice(128 * tile, 128 * tile + 128)
        for slot, comp in enumerate(comps):
            blocks = wide_blocks(comp, tile)
            order = [-2, -1, 0, 1, 2, ("y", 0), ("y", 1), ("c", 0), ("c", 1), 3, 4, 5]
            for n, key in enumerate(order):
                at = 8 * (n * len(comps) + slot)
                code = code256[code_at + at : code_at + at + 8, lanes]
                target[at : at + 8, lanes] = jnp.where(inside(code), blocks[key], 0.0)

    def ring_of(source, comps):
        def block(n):
            return source[8 * comps * n : 8 * comps * (n + 1), :]

        row = lax.broadcasted_iota(jnp.int32, (8 * comps, source.shape[1]), 0)
        odd, low = (row & 1) == 1, (row & 7) < 4
        level = jnp.where(odd, block(5), block(6))
        corner = jnp.where(odd, block(7), block(8))
        return jnp.concatenate(
            [
                block(1), block(2), block(3), jnp.where(low, level, corner),
                block(4), block(9), block(10), jnp.where(low, corner, level),
            ],
            axis=0,
        )

    def local_of(ring, comps):
        return jnp.concatenate([ring[8 * comps : 24 * comps], ring[32 * comps : 48 * comps]], axis=0)

    def operator_ring():
        parts = []
        for name, start in (("a", 0), ("b", 32)):
            high, low = split(wide[start : start + 256, :])
            right = jnp.concatenate([high, high, low], axis=0)
            base = WIDE_SECTIONS[name][3]
            product = jnp.dot(w[base : base + 288, :], right, preferred_element_type=F32)
            parts.append(z_shift_sum(product, 96))
        return jnp.concatenate(parts, axis=0)

    def operator_local(value):
        high, low = split(value)
        gap = jnp.zeros((64, 256), BF16)
        right = jnp.concatenate([high, gap, high, gap, low, gap], axis=0)
        base = WIDE_SECTIONS["local"][3]
        product = jnp.dot(w[base : base + 288, :], right, preferred_element_type=F32)
        return z_shift_sum(product, 96)

    ikc = (jnp.full((8, 256), 1.0, F32) / kc)[0:1, :]
    gain_u = ((1.0 + MOM + WEIGHT * THETA) / THETA) * ikc
    gain_s = (-WEIGHT / THETA) * ikc * ikc

    ring_code = len(CODE_WIDE)
    wide_p_code = ring_code + len(CODE_RING)
    ring_p_code = wide_p_code + len(CODE_WIDE_P)

    def ring_inside():
        return inside(code256[ring_code : ring_code + 192, :])

    receive(1, plane_choices(2, 6, 3))
    store_wide(wide, (0, 1, 2), 0, 0)

    receive(0, ahead_choices(1))

    store_wide(wide, (0, 1, 2), 0, 1)
    x2 = jnp.where(ring_inside(), gain_u * ring_of(wide, 3) + gain_s * operator_ring(), 0.0)
    ring_x[...] = x2

    applied = operator_local(x2)
    even = (lane8 * 2) & 127

    def row_sum(source, n):
        return source[n, pl.ds(0, 8, 2), :] + source[n, pl.ds(1, 8, 2), :]

    def pair_sum(value, index):
        one = jnp.take_along_axis(value, index, axis=1, mode="promise_in_bounds")
        two = jnp.take_along_axis(value, index + 1, axis=1, mode="promise_in_bounds")
        return one + two

    def local_row(p):
        return 8 * (3 + 3 * p if p < 2 else 6 + 3 * p)

    for big in range(2):
        resid[3, 8 * big : 8 * big + 8, :] = eta[2 * big] + eta[2 * big + 1]
        for j in range(3):
            total = jnp.zeros((8, 128), F32)
            for p in (2 * big, 2 * big + 1):
                n = 8 * (3 * p + j)
                left = main[p, j] - applied[n : n + 8, 0:128]
                resid[4 + j, 8 * p : 8 * p + 8, :] = left
                at = local_row(p) + 8 * j
                value = ring_x[at : at + 8, 0:128] + ((1.0 / THETA) * ikc[:, 0:128]) * left
                before[p, j] = value
                total = total + eta[p] * left
            resid[j, 8 * big : 8 * big + 8, :] = total
    weights = row_sum(resid, 3)
    four_over = 4.0 / pair_sum(weights, even)
    total = jnp.zeros((8, 128), F32)
    for j in range(3):
        value = row_sum(resid, j)
        coarse[j] = pair_sum(value, even) * four_over
        first = (lane8 >= 98 + 4 * j) & (lane8 < 100 + 4 * j)
        last = (lane8 >= 32 + 4 * j) & (lane8 < 34 + 4 * j)
        here = jnp.where(first, 2 * (lane8 - (98 + 4 * j)), jnp.where(last, 2 * (lane8 + 30 - 4 * j), 0))
        packed = pair_sum(value, here) * (4.0 / pair_sum(weights, here))
        total = jnp.where(first | last, packed, total)
        for p in range(4):
            ysend[2 + j, 2 * p : 2 * p + 1, :] = before[p, j, 0:1, :]
            ysend[2 + j, 2 * p + 1 : 2 * p + 2, :] = before[p, j, 7:8, :]
            if p in (0, 3):
                n = 0 if p == 0 else 1
                xsend[n, 2 + j] = before[p, j]
                csend[n, 2, 2 * j : 2 * j + 1, :] = before[p, j, 0:1, :]
                csend[n, 2, 2 * j + 1 : 2 * j + 2, :] = before[p, j, 7:8, :]
    items = [before[p, j] for p in range(4) for j in range(3)] + [ysend[2 + j] for j in range(3)]
    for k, value in enumerate(items):
        total = jnp.where(((lane8 + (129 - 2 * k)) & 127) < 2, roll(value, 2 * k), total)
    zpack2[...] = total
    for n, value in enumerate((jnp.where(lane8 < 64, coarse[0], roll(coarse[1], 64)), coarse[2])):
        ysend[n] = value
        for m in range(2):
            xsend[m, n] = value
            csend[m, n] = value
    send_ahead(3, zpack2, rz2)
    for dx in (-1, 1):
        for dy in (-1, 1):
            send(
                4,
                csend.at[0 if dx < 0 else 1],
                rc2.at[0 if dx > 0 else 1, 0 if dy > 0 else 1],
                (dx, dy, 0),
            )
        send(4, xsend.at[0 if dx < 0 else 1], rx2.at[0 if dx > 0 else 1], (dx, 0, 0))
    for dy in (-1, 1):
        send(4, ysend, ry2.at[0 if dy > 0 else 1], (0, dy, 0))

    receive(2, plane_choices(0, 2, 1))
    store_wide(wide_p, (3,), wide_p_code, 0)
    store_wide(wide_p, (3,), wide_p_code, 1)
    q_ring = ring_of(wide_p, 1)
    high, low = split(wide_p[...])
    gap = jnp.zeros((32, 256), BF16)
    near = jnp.dot(face1[...], jnp.concatenate([high, gap, low, gap], axis=0), preferred_element_type=F32)
    near = near + pltpu.roll(q_ring, 1, 1) + pltpu.roll(q_ring, 255, 1)
    p_ring = (4.0 / 27.0) * q_ring + (1.0 / 81.0) * near
    p_ring = jnp.where(inside(code256[ring_p_code : ring_p_code + 64, :]), p_ring, 0.0)
    high, low = split(p_ring)
    near = jnp.dot(face2[...], jnp.concatenate([high, low], axis=0), preferred_element_type=F32)
    p_in, q_in = local_of(p_ring, 1), local_of(q_ring, 1)
    near = near + pltpu.roll(p_in, 1, 1) + pltpu.roll(p_in, 255, 1)
    p_out = (1.0 / 3.0) * p_in + (1.0 / 9.0) * q_in + (1.0 / 9.0) * near
    for p in range(4):
        pout_ref[p] = p_out[8 * p : 8 * p + 8, 0:128]
    for name in ("coarse", "keep"):
        build(cindex, COARSE_SECTIONS[name], w_coarse, 4, 144, 5)
    for name in ("fine", "spread"):
        build(findex, FINE_SECTIONS[name], w_fine, 2, 80, 6)
    receive(4, plane_choices(3, 5, 5))
    receive(3, ahead_choices(2))

    def from_side(ox, oy, n):
        if ox and oy:
            return rc2[0 if ox < 0 else 1, 0 if oy < 0 else 1, n]
        return rx2[0 if ox < 0 else 1, n] if ox else ry2[0 if oy < 0 else 1, n]

    def coarse_block(ox, oy, j):
        if (ox, oy) == (0, 0):
            inner = coarse[j]
        else:
            inner = from_side(ox, oy, j // 2)
            inner = roll(inner, 64) if j == 1 else inner
        return jnp.where(lane8 < 64, inner, roll(along_z(rz2, from_high_2, ox, oy), -(34 + 4 * j)))

    blocks = []
    near_high = (row8 & 3) < 2
    for ox in (-1, 0, 1):
        blocks += [coarse_block(ox, 0, j) for j in range(3)]
        blocks += [jnp.where(near_high, coarse_block(ox, 1, j), coarse_block(ox, -1, j)) for j in range(3)]
    value = jnp.where(inside(code128[0:144, :]), jnp.concatenate(blocks, axis=0), 0.0)
    high, low = split(value)
    right = jnp.concatenate([high, high, low, jnp.zeros((80, 128), BF16)], axis=0)
    product = jnp.dot(w_coarse[...], right, preferred_element_type=F32)
    e = gain_u[:, 0:128] * product[240:320] + gain_s[:, 0:128] * z_shift_sum(product, 80)
    e = jnp.where(inside(code128[144:224, :]), e, 0.0)
    lane80 = lax.broadcasted_iota(jnp.int32, (80, 128), 1)
    near_lane = lane80 >> 1
    far_lane = jnp.where(lane80 < 2, 64, jnp.where(lane80 >= 126, 127, 100))
    e = jnp.concatenate(
        [
            jnp.take_along_axis(e, near_lane, axis=1, mode="promise_in_bounds"),
            jnp.take_along_axis(e, far_lane, axis=1, mode="promise_in_bounds"),
        ],
        axis=1,
    )
    high, low = split(e)
    right = jnp.concatenate([high, high, low, jnp.zeros((16, 256), BF16)], axis=0)
    product = jnp.dot(w_fine[...], right, preferred_element_type=F32)

    def ring_block(ox, oy, inner, k):
        return jnp.concatenate([inner, roll(along_z(rz2, from_high_2, ox, oy), -2 * k)], axis=1)

    def layer(ox, j):
        if ox == 0:
            inner = jnp.where(odd_rows, from_side(0, -1, 2 + j), from_side(0, 1, 2 + j))
        else:
            inner = jnp.where(odd_rows, from_side(ox, -1, 2), from_side(ox, 1, 2))
            shift = (-2 * j if ox > 0 else 6 - 2 * j) % 8
            inner = pltpu.roll(inner, shift, 0) if shift else inner
        outer = jnp.where(odd_rows, along_z(rz2, from_high_2, ox, -1), along_z(rz2, from_high_2, ox, 1))
        return jnp.concatenate([inner, roll(outer, -2 * (12 + j))], axis=1)

    low_wide = lax.broadcasted_iota(jnp.int32, (8, 256), 0) < 4
    halves = [[], []]
    for half in range(2):
        for x in ((-1, 0, 1), (2, 3, 4))[half]:
            for j in range(3):
                if x == -1:
                    halves[half].append(ring_block(-1, 0, rx2[0, 2 + j], 9 + j))
                elif x == 4:
                    halves[half].append(ring_block(1, 0, rx2[1, 2 + j], j))
                else:
                    halves[half].append(ring_block(0, 0, before[x, j], 3 * x + j))
    for j in range(3):
        level = layer(0, j)
        halves[0].append(jnp.where(low_wide, level, layer(-1, j)))
        halves[1].append(jnp.where(low_wide, layer(1, j), level))
    start = jnp.concatenate(halves[0] + halves[1], axis=0)

    down = ((1.0 / THETA) * ikc) * z_shift_sum(product, 192)
    x = jnp.where(ring_inside(), start + product[576:768] - down, 0.0)
    applied = operator_local(x)
    x_in, down_in = local_of(x, 3), local_of(down, 3)
    for p in range(4):
        for j in range(3):
            n = 8 * (3 * p + j)
            step = ((1.0 / THETA) * ikc[:, 0:128]) * resid[4 + j, 8 * p : 8 * p + 8, :] - down_in[n : n + 8, 0:128]
            out_ref[j, p] = (
                x_in[n : n + 8, 0:128]
                + MOM * step
                + (WEIGHT * ikc[:, 0:128]) * (main[p, j] - applied[n : n + 8, 0:128])
            )

    totals = [
        (there, (4 + 4 * nx + 4 * ny + 3 * nx * ny) * nz + 2 * (5 * nx * ny + 13 * nx + 9 * ny))
        for (there, _), (nx, ny, nz) in zip(
            ahead_choices(2), [(nx, ny, nz) for nx in (1, 2) for ny in (1, 2) for nz in (1, 2)]
        )
    ]
    wait_group(send_sem.at[0], totals)


GROUPS = 5
REST_TILES = (
    CODE_256.size + CODE_128.size + COARSE_INDEX.size + FINE_INDEX.size + (FACE_1.size + FACE_2.size) // 2
) // 1024


def scratch():
    vmem = pltpu.VMEM
    return [
        vmem((3, 4, 8, 128), F32),
        vmem((4, 8, 128), F32),
        vmem((4, 8, 128), jnp.int32),
        pltpu.SMEM((8,), F32),
        pltpu.SMEM((3, 3, 27), F32),
        vmem(WIDE_INDEX.shape, jnp.int32),
        vmem(COARSE_INDEX.shape, jnp.int32),
        vmem(FINE_INDEX.shape, jnp.int32),
        vmem(CODE_256.shape, jnp.int32),
        vmem(CODE_128.shape, jnp.int32),
        vmem(FACE_1.shape, BF16),
        vmem(FACE_2.shape, BF16),
        vmem((4, 8, 128), F32),
        vmem((4, 3, 8, 128), F32),
        vmem((4, 8, 128), F32),
        vmem((2, 3, 8, 128), F32),
        vmem((2, 8, 128), F32),
        vmem((2, 2, 2, 8, 128), F32),
        vmem((8, 128), F32),
        vmem((2, 2, 3, 8, 128), F32),
        vmem((2, 3, 8, 128), F32),
        vmem((2, 2, 2, 8, 128), F32),
        vmem((2, 2, 8, 128), F32),
        vmem((2, 8, 128), F32),
        vmem((2, 3, 3, 8, 128), F32),
        vmem((4, 3, 8, 128), F32),
        vmem((3, 8, 128), F32),
        vmem((8, 128), F32),
        vmem((2, 5, 8, 128), F32),
        vmem((5, 8, 128), F32),
        vmem((2, 3, 8, 128), F32),
        vmem((2, 5, 8, 128), F32),
        vmem((2, 5, 8, 128), F32),
        vmem((2, 2, 3, 8, 128), F32),
        vmem((2, 3, 3, 8, 128), F32),
        vmem((9, 16, 128), F32),
        vmem((WIDE_ROWS, 768), BF16),
        vmem((COARSE_ROWS, 512), BF16),
        vmem((FINE_ROWS, 256), BF16),
        vmem((288, 256), F32),
        vmem((96, 256), F32),
        vmem((192, 256), F32),
        vmem((7, 32, 128), F32),
        vmem((2 * REST_TILES, 4, 128), F32),
        pltpu.SemaphoreType.DMA((5,)),
        pltpu.SemaphoreType.DMA((1,)),
        pltpu.SemaphoreType.DMA((GROUPS,)),
    ]


def store_results(velocity, pressure, velocity_out, pressure_out, sem):
    one = pltpu.make_async_copy(velocity, velocity_out, sem.at[0])
    two = pltpu.make_async_copy(pressure, pressure_out, sem.at[1])
    one.start()
    two.start()
    one.wait()
    two.wait()


def on_device(rhs_velocity, rhs_pressure, layer_ids, visc_table, stencil):
    anywhere = pl.BlockSpec(memory_space=pltpu.HBM)
    inside = pl.BlockSpec(memory_space=pltpu.VMEM)
    results = pl.pallas_call(
        body,
        name="stokes",
        out_shape=(
            pltpu.VMEM(rhs_velocity.shape, F32),
            pltpu.VMEM(rhs_pressure.shape, F32),
        ),
        in_specs=[anywhere] * 12,
        out_specs=(inside, inside),
        scratch_shapes=scratch(),
        compiler_params=pltpu.CompilerParams(
            collective_id=0, has_side_effects=True, vmem_limit_bytes=60 * 1024 * 1024
        ),
    )(
        *(
            pltpu.with_memory_space_constraint(value, pltpu.HBM)
            for value in (
                rhs_velocity,
                rhs_pressure,
                layer_ids,
                visc_table,
                stencil.transpose(1, 2, 0),
                jnp.asarray(WIDE_INDEX),
                jnp.asarray(COARSE_INDEX),
                jnp.asarray(FINE_INDEX),
                jnp.asarray(CODE_256),
                jnp.asarray(CODE_128),
                jnp.asarray(FACE_1, BF16),
                jnp.asarray(FACE_2, BF16),
            )
        )
    )
    return pl.pallas_call(
        store_results,
        name="store",
        out_shape=(
            jax.ShapeDtypeStruct(rhs_velocity.shape, F32),
            jax.ShapeDtypeStruct(rhs_pressure.shape, F32),
        ),
        in_specs=[inside] * 2,
        out_specs=(anywhere,) * 2,
        scratch_shapes=[pltpu.SemaphoreType.DMA((2,))],
    )(*(pltpu.with_memory_space_constraint(value, pltpu.VMEM) for value in results))


def solution(mesh):
    placed = (P(None, "gx", "gy", "gz"), P("gx", "gy", "gz"), P("gx", "gy", "gz"), P(), P())
    return jax.shard_map(
        on_device,
        mesh=mesh,
        in_specs=placed,
        out_specs=(P(None, "gx", "gy", "gz"), P("gx", "gy", "gz")),
        check_vma=False,
    )
```
